32 devices in a mesh: comp: 2 (over core), lat: 4 (over z), lon: 4 (over y, x).
Axes of the slice: x: 2, y: 2, z: 4, core: 2. Of those that a mesh axis runs over, the one named last changes fastest.
Arguments:
- fields: float32 [2, 7, 2048, 256], P('comp', None, ('lat', 'lon')), may hold values from -4 to 4, as said below
- block_owner: int32 [2048], P(('lat', 'lon')), may hold values from 0 to 2047, as said below
- ice_covered: int32 [2048], P(('lat', 'lon')), may hold values 0 or 1
- land_mask: int32 [2048, 256], P(('lat', 'lon')), may hold values 0 or 1
Outputs:
- coupled_out: float32 [2, 2, 2048, 256], P('comp', None, ('lat', 'lon'))
The draws below stay inside these ranges and needn't reach their ends.
Inputs may be any that keep to these rules, and one draw needn't show every extreme that they name: `block_owner`: every block id appears once. Slot d of lat+lon index o holds a block of the ice tile of index d, that is an id from d * 128 to d * 128 + 127. `fields`: ocean channels: winds within 4, currents within 1.5, tilts within 1, air density 0.9 to 1.3; ice channels: velocities within 1.5, mass 0.5 to 4, concentration 0.05 to 1, stresses within 1.5.
All inputs are finite; a program needn't handle non-finite values.
Results may differ from the reference program's by a relative error of at most 0.00002.
Values sent between devices are 32-bit elements.
No kernel may reach another device: no remote copies, remote signals or barrier semaphores. Data moves between devices by JAX's collectives and lax.ppermute only.
A program may use at most 64 MiB of HBM per device.

```python
import jax
import jax.numpy as jnp

KB = 128
GX = 1
BY = 2
BX = 128
NSUB = 4
NBALL = 2048
CELLS = 256
N_LAT = 4
N_LON = 4


def clipped_normal(subkey, scale, limit):
    return jnp.clip(scale * jax.random.normal(subkey, (NBALL, CELLS), jnp.float32), -limit, limit)


def uniform_draw(subkey, low, high):
    return jax.random.uniform(subkey, (NBALL, CELLS), jnp.float32, low, high)


def draw_fields(key, part):
    subkeys = jax.random.split(jax.random.fold_in(key, 11), 14)
    wind = [clipped_normal(subkeys[0], 1.5, 4.0), clipped_normal(subkeys[1], 1.5, 4.0)]
    current = [clipped_normal(subkeys[2], 0.5, 1.5), clipped_normal(subkeys[3], 0.5, 1.5)]
    tilt = [clipped_normal(subkeys[4], 0.3, 1.0), clipped_normal(subkeys[5], 0.3, 1.0)]
    drift = [clipped_normal(subkeys[7], 0.5, 1.5), clipped_normal(subkeys[8], 0.5, 1.5)]
    concentration = uniform_draw(subkeys[10], 0.05, 1.0)
    stresses = [clipped_normal(subkeys[11], 0.5, 1.5), clipped_normal(subkeys[12], 0.5, 1.5), clipped_normal(subkeys[13], 0.5, 1.5)]
    density = uniform_draw(subkeys[6], 0.9, 1.3)
    ice_mass = jnp.exp(uniform_draw(subkeys[9], jnp.log(0.5), jnp.log(4.0)))
    ocean = jnp.stack(wind + current + tilt + [density])
    sea_ice = jnp.stack(drift + [ice_mass, concentration] + stresses)
    return jnp.stack([ocean, sea_ice]).astype(jnp.float32)


def draw_block_owner(key, part):
    devices = N_LAT * N_LON
    per_peer = KB // devices
    subkeys = jax.random.split(jax.random.fold_in(key, 5), devices)
    orders = jax.vmap(lambda subkey: jax.random.permutation(subkey, KB))(subkeys)
    ids = orders.astype(jnp.int32) + (jnp.arange(devices, dtype=jnp.int32) * KB)[:, None]
    ids = ids.reshape(devices, devices, per_peer).transpose(1, 0, 2)
    return ids.reshape(devices * KB).astype(jnp.int32)


def plant(array, key, smallest, largest):
    extent = array.shape
    place = [jax.random.randint(jax.random.fold_in(key, axis), (), 0, extent[axis]) for axis in range(len(extent))]
    array = array.at[tuple(place)].set(smallest)
    longest = extent.index(max(extent))
    place[longest] = (place[longest] + 1) % extent[longest]
    return array.at[tuple(place)].set(largest)


def setup_inputs(seed: int = 0) -> dict:
    streams_of = jax.random.split(jax.random.key(seed), 5)
    fields = draw_fields(jax.random.fold_in(streams_of[4], 71), 0)
    block_owner = draw_block_owner(jax.random.fold_in(streams_of[4], 71), 0)
    ice_covered = plant((jax.random.randint(streams_of[2], (NBALL,), 0, 4) < 3).astype(jnp.int32), jax.random.fold_in(streams_of[2], 1), 0, 1)
    land_mask = plant((jax.random.randint(streams_of[3], (NBALL, CELLS), 0, 8) < 1).astype(jnp.int32), jax.random.fold_in(streams_of[3], 1), 0, 1)
    return dict(fields=fields, block_owner=block_owner, ice_covered=ice_covered, land_mask=land_mask)


CD_ICE = 0.1
CW = 1.5
CSTAR = 2.0
ECC2 = 4.0
DMIN2 = 0.25
RELAX = 0.5
DTE = 0.5
CORIO = 0.3
MASS_FLOOR = 0.5
DRAG_FLOOR = 0.1

def air_stress(ocean):
    wind_x, wind_y, current_x, current_y, tilt_x, tilt_y, density = ocean
    speed_ice = jnp.sqrt(wind_x * wind_x + wind_y * wind_y + 1.0)
    scale_ice = density * CD_ICE * speed_ice
    rel_x = wind_x - current_x
    rel_y = wind_y - current_y
    speed_open = jnp.sqrt(rel_x * rel_x + rel_y * rel_y + 1.0)
    scale_open = density * (0.1 + 0.05 * speed_open) * speed_open
    outbound = jnp.stack([scale_ice * wind_x, scale_ice * wind_y, current_x, current_y, tilt_x, tilt_y])
    open_stress = jnp.stack([scale_open * rel_x, scale_open * rel_y])
    return (outbound, open_stress)

def prepare(ice_tile, forcing, active):
    ice_mass = ice_tile[2]
    concentration = ice_tile[3]
    strength = ice_mass * jnp.exp(CSTAR * (concentration - 1.0)) * active
    drag_base = CW * concentration * active
    push_x = active * (concentration * forcing[0] - ice_mass * forcing[4])
    push_y = active * (concentration * forcing[1] - ice_mass * forcing[5])
    return jnp.stack([strength, ice_mass, drag_base, push_x, push_y, forcing[2], forcing[3], active])

def subcycle(ice_state, statics):
    east_vel, north_vel, stress_one, stress_two, stress_three = ice_state
    strength = statics[0]
    east_base = east_vel[:-1, :-1]
    north_base = north_vel[:-1, :-1]
    strain_xx = east_vel[:-1, 1:] - east_base
    strain_yy = north_vel[1:, :-1] - north_base
    shear = east_vel[1:, :-1] - east_base + (north_vel[:-1, 1:] - north_base)
    divergence = strain_xx + strain_yy
    tension = strain_xx - strain_yy
    delta_norm = jnp.sqrt(divergence * divergence + (tension * tension + shear * shear) / ECC2 + DMIN2)
    viscosity = strength[:-1, :-1] / delta_norm
    stress_sum = (stress_one[:-1, :-1] + RELAX * viscosity * (divergence - delta_norm)) / (1.0 + RELAX)
    stress_diff = (stress_two[:-1, :-1] + RELAX * viscosity * tension / ECC2) / (1.0 + RELAX)
    stress_shear = (stress_three[:-1, :-1] + RELAX * viscosity * shear / (2.0 * ECC2)) / (1.0 + RELAX)
    stress_xx = 0.5 * (stress_sum + stress_diff)
    stress_yy = 0.5 * (stress_sum - stress_diff)
    force_x = stress_xx[1:, 1:] - stress_xx[1:, :-1] + (stress_shear[1:, 1:] - stress_shear[:-1, 1:])
    force_y = stress_shear[1:, 1:] - stress_shear[1:, :-1] + (stress_yy[1:, 1:] - stress_yy[:-1, 1:])
    trimmed = statics[:, 1:-1, 1:-1]
    strength, ice_mass, drag_base, push_x, push_y, current_x, current_y, active = trimmed
    east_old = east_vel[1:-1, 1:-1]
    north_old = north_vel[1:-1, 1:-1]
    diff_x = current_x - east_old
    diff_y = current_y - north_old
    drag_coef = drag_base * jnp.sqrt(diff_x * diff_x + diff_y * diff_y + DRAG_FLOOR)
    denominator = jnp.maximum(ice_mass, MASS_FLOOR) / DTE + drag_coef
    east_new = active * (ice_mass / DTE * east_old + force_x + push_x + drag_coef * current_x + CORIO * ice_mass * north_old) / denominator
    north_new = active * (ice_mass / DTE * north_old + force_y + push_y + drag_coef * current_y - CORIO * ice_mass * east_old) / denominator
    new_state = jnp.stack([east_new, north_new, stress_sum[1:, 1:], stress_diff[1:, 1:], stress_shear[1:, 1:]])
    return (new_state, trimmed)

def give_back(ice_state, statics):
    east_vel = ice_state[0]
    north_vel = ice_state[1]
    drag_base = statics[2]
    current_x = statics[5]
    current_y = statics[6]
    diff_x = east_vel - current_x
    diff_y = north_vel - current_y
    factor = drag_base * jnp.sqrt(diff_x * diff_x + diff_y * diff_y + DRAG_FLOOR)
    return jnp.stack([factor * diff_x, factor * diff_y, drag_base / CW])

def to_grid(blocks):
    channels = blocks.shape[0]
    arranged = blocks.reshape(channels, N_LAT, N_LON, KB // GX, GX, BY, BX)
    arranged = arranged.transpose(0, 1, 3, 5, 2, 4, 6)
    return arranged.reshape(channels, N_LAT * (KB // GX) * BY, N_LON * GX * BX)

def from_grid(values):
    channels = values.shape[0]
    arranged = values.reshape(channels, N_LAT, KB // GX, BY, N_LON, GX, BX)
    arranged = arranged.transpose(0, 1, 4, 2, 5, 3, 6)
    return arranged.reshape(channels, N_LAT * N_LON * KB, BY * BX)

def extend_grid(values, width):
    values = jnp.concatenate([values[..., -width:], values, values[..., :width]], axis=-1)
    return jnp.pad(values, ((0, 0), (width, width), (0, 0)))

def reference(fields, block_owner, ice_covered, land_mask):
    outbound, open_stress = air_stress(fields[0])
    geographic = jnp.zeros_like(outbound).at[:, block_owner].set(outbound)
    forcing = to_grid(geographic)
    ice_tile = to_grid(fields[1])
    covered = ice_covered.astype(jnp.float32)[:, None] * (1 - land_mask).astype(jnp.float32)
    active = to_grid(covered[None])[0]
    statics = prepare(ice_tile, forcing, active)
    ice_state = jnp.stack([ice_tile[0], ice_tile[1], ice_tile[4], ice_tile[5], ice_tile[6]])
    ice_state = extend_grid(ice_state, NSUB)
    statics = extend_grid(statics, NSUB)
    for repeat in range(NSUB):
        ice_state, statics = subcycle(ice_state, statics)
    returned = from_grid(give_back(ice_state, statics))
    received_back = returned[:, block_owner]
    ocean_out = received_back[:2] + (1.0 - received_back[2]) * open_stress
    ice_out = from_grid(ice_state[:2])
    return jnp.stack([ocean_out, ice_out])
```

```python
import functools

import jax
import jax.numpy as jnp
from jax import lax
from jax.experimental import pallas as pl
from jax.experimental.pallas import tpu as pltpu
from jax.sharding import PartitionSpec as P

BX = 128
NSUB = 4
FRONT = 8
STEP = 16

CD_ICE = 0.1
CW = 1.5
CSTAR = 2.0
CORIO = 0.3
DRAG_FLOOR = 0.1

VMEM = pl.BlockSpec(memory_space=pltpu.VMEM)
SMEM = pl.BlockSpec(memory_space=pltpu.SMEM)


def f32(*shape):
    return jax.ShapeDtypeStruct(shape, jnp.float32)


def lanes(rows):
    return lax.broadcasted_iota(jnp.int32, (rows, BX), 1)


def roll(x, by):
    return pltpu.roll(x, by % BX, 1)


def at_end(q, west, east):
    return jnp.where(q, west, east)


def pack_kernel(nlat, nlon, per, count, raw, idb, pay, edge, rim):
    n = nlat * nlon
    lane = lanes(per)
    group = lane // 8
    lat_base = 13 * per

    def tile(t, _):
        def half(ch, y):
            return raw[ch, t, :, y * BX : (y + 1) * BX]

        planes = [None] * 12
        for y in range(2):
            wx, wy, rho = half(0, y), half(1, y), half(6, y)
            scale = rho * CD_ICE * jnp.sqrt(wx * wx + wy * wy + 1.0)
            planes[y] = scale * wx
            planes[2 + y] = scale * wy
            for ch in range(2, 6):
                planes[2 * ch + y] = half(ch, y)
        ends = jnp.zeros((per, BX), jnp.float32)
        for p in range(12):
            pay[t, pl.ds(p, per, stride=12), :] = planes[p]
            ends = jnp.where(group == p, roll(planes[p], 8 * p + 4), ends)
        edge[t] = ends
        ids = idb[t]

        def pick(block, value):
            return jnp.sum(jnp.where(ids == block, value, 0.0), axis=0, keepdims=True)

        rows = [pick(0, x) for x in planes] + [pick(1, x) for x in planes[0::2]]
        rows += [pick(count - 1, x) for x in planes]
        rows += [pick(count - 2, x) for x in planes[1::2]]
        rows += [pick(b, ends) for b in (0, 1, count - 1, count - 2)]
        for k, row in enumerate(rows):
            rim[t, k : k + 1, :] = row
        return 0

    lax.fori_loop(0, n, tile, 0)

    def dest(d, _):
        i, j = d // nlon, d % nlon
        jw, je = (j + nlon - 1) % nlon, (j + 1) % nlon
        q8 = (lane % 8) < 4
        pay[d, 12 * per : 13 * per, :] = at_end(q8, edge[i * nlon + jw], edge[i * nlon + je])
        for ii, ok, lo, c in (
            (jnp.minimum(i + 1, nlat - 1), i + 1 < nlat, 0, 36),
            (jnp.maximum(i - 1, 0), i > 0, 18, 38),
        ):
            scale = jnp.where(ok, 1.0, 0.0)
            pay[d, lat_base + lo : lat_base + lo + 18, :] = rim[ii * nlon + j, lo : lo + 18, :] * scale
            q2 = (lanes(2) % 8) < 4
            corner = at_end(q2, rim[ii * nlon + jw, c : c + 2, :], rim[ii * nlon + je, c : c + 2, :])
            pay[d, lat_base + c : lat_base + c + 2, :] = corner * scale
        return 0

    lax.fori_loop(0, n, dest, 0)


def pack(raw, idb, nlat, nlon):
    _, n, per, _ = raw.shape
    rows = 13 * per + 40
    return pl.pallas_call(
        functools.partial(pack_kernel, nlat, nlon, per, n * per),
        out_shape=f32(n, rows, BX),
        in_specs=[VMEM, VMEM],
        out_specs=VMEM,
        scratch_shapes=[pltpu.VMEM((n, per, BX), jnp.float32), pltpu.VMEM((n, 40, BX), jnp.float32)],
        name="pack",
    )(raw, idb)


def ends_kernel(ice, covered, land, active, ends):
    count = covered.shape[0]
    lane = lanes(count)
    group = lane // 8
    total = jnp.zeros((count, BX), jnp.float32)
    for y in range(2):
        cells = slice(y * BX, (y + 1) * BX)
        act = covered[...].astype(jnp.float32) * (1 - land[:, cells]).astype(jnp.float32)
        active[:, cells] = act
        for ch in range(8):
            x = act if ch == 7 else ice[ch, :, cells]
            p = 2 * ch + y
            total = jnp.where(group == p, roll(x, 8 * p + 4), total)
    ends[...] = total


def ice_ends(ice, covered, land):
    count = covered.shape[0]
    return pl.pallas_call(
        ends_kernel,
        out_shape=[f32(count, 2 * BX), f32(count, BX)],
        in_specs=[VMEM] * 3,
        out_specs=[VMEM] * 2,
        name="ice_ends",
    )(ice, covered, land)


def rows_kernel(ice, active, west, east, sides, north, south):
    count = active.shape[0]
    q = (lanes(count) % 8) < 4
    sides[...] = jnp.where(q, west[...], east[...])
    for out, lo in ((north, count - 2), (south, 0)):
        for y in range(2):
            cells = slice(y * BX, (y + 1) * BX)
            for ch in range(8):
                p = 2 * ch + y
                x = active[lo : lo + 2, cells] if ch == 7 else ice[ch, lo : lo + 2, cells]
                out[2 * p : 2 * p + 2, :] = x
        out[32:34, :] = sides[lo : lo + 2, :]


def ice_rows(ice, active, west, east):
    count = active.shape[0]
    return pl.pallas_call(
        rows_kernel,
        out_shape=[f32(count, BX), f32(34, BX), f32(34, BX)],
        in_specs=[VMEM] * 4,
        out_specs=[VMEM] * 3,
        name="ice_rows",
    )(ice, active, west, east)


def east_of(first, second, last):
    a, b = roll(first, -1), roll(second, -1)
    return jnp.where(last, b, a), jnp.where(last, a, b)


def west_of(first, second, start):
    a, b = roll(first, 1), roll(second, 1)
    return jnp.where(start, b, a), jnp.where(start, a, b)


def ice_kernel(n, per, count, ids, recv, ice, active, sides, below, above, back, moved,
               spot, hw, he, grid, state, fixed, cross, out8):
    tiles = (count + 4 + 7) // 8
    height = tiles * 8
    blank = jnp.zeros((8, BX), jnp.float32)
    for k in range(count + 4, height):
        spot[k * STEP : k * STEP + 8, :] = blank
        spot[k * STEP + 8 : k * STEP + 16, :] = blank
    for k in (0, height - 8):
        hw[k : k + 8, :] = blank
        he[k : k + 8, :] = blank
    spot[0:8, :] = blank
    spot[8:16, :] = blank
    end = (count + 3) * STEP
    spot[end : end + 8, :] = blank
    spot[end + 8 : end + 16, :] = blank

    def place(o, acc):
        for j in range(per):
            b = pl.multiple_of((ids[o, j] + 2) * STEP, STEP)
            spot[pl.ds(b, 12), :] = recv[o, 12 * j : 12 * j + 12, :]
            row = recv[o, 12 * per + j : 12 * per + j + 1, :]
            hw[pl.ds(ids[o, per + j] + 2, 1), :] = row
            he[pl.ds(ids[o, 2 * per + j] + 2, 1), :] = row
        return acc + recv[o, 13 * per : 13 * per + 40, :]

    rim = lax.fori_loop(0, n, place, jnp.zeros((40, BX), jnp.float32))
    up, down = (count + 2) * STEP, STEP
    spot[up : up + 12, :] = rim[0:12]
    spot[down : down + 12, :] = rim[18:30]
    for ch in range(6):
        k = up + STEP + 2 * ch
        spot[k : k + 1, :] = rim[12 + ch : 13 + ch]
        k = 2 * ch + 1
        spot[k : k + 1, :] = rim[30 + ch : 31 + ch]
    for ref in (hw, he):
        ref[count + 2 : count + 4, :] = rim[36:38]
        ref[1:2, :] = rim[38:39]
        ref[0:1, :] = rim[39:40]

    q = (lanes(8) % 8) < 4
    for ch in range(8):
        for y in range(2):
            p = 2 * ch + y
            cells = slice(y * BX, (y + 1) * BX)
            shift = -(8 * p + 4)
            grid[ch, y, 0, 2 : 2 + count, :] = active[:, cells] if ch == 7 else ice[ch, :, cells]
            grid[ch, y, 1, 2 : 2 + count, :] = roll(sides[...], shift)
            for lo, msg in ((0, below), (count + 2, above)):
                grid[ch, y, 0, lo : lo + 2, :] = msg[2 * p : 2 * p + 2, :]
                grid[ch, y, 1, lo : lo + 2, :] = roll(msg[32:34, :], shift)
            grid[ch, y, 0, count + 4 :, :] = jnp.zeros((height - count - 4, BX), jnp.float32)
            grid[ch, y, 1, count + 4 :, :] = jnp.zeros((height - count - 4, BX), jnp.float32)

    for r in range(tiles):
        at = slice(8 * r, 8 * r + 8)
        to = slice(FRONT + 8 * r, FRONT + 8 * r + 8)
        ends = jnp.where(q, hw[at, :], he[at, :])
        for y in range(2):
            for w in range(2):
                if w == 0:
                    f = [spot[pl.ds(8 * r * STEP + 2 * ch + y, 8, stride=STEP), :] for ch in range(6)]
                else:
                    f = [roll(ends, -(8 * (2 * ch + y) + 4)) for ch in range(6)]
                u, v, mass, conc, s1, s2, s12, act = [grid[ch, y, w, at, :] for ch in range(8)]
                state[0, y, w, to, :] = u
                state[1, y, w, to, :] = v
                state[2, y, w, to, :] = s1
                state[3, y, w, to, :] = s2
                state[4, y, w, to, :] = s12
                fixed[0, y, w, at, :] = mass * jnp.exp(CSTAR * (conc - 1.0)) * act * (1.0 / 3.0)
                fixed[1, y, w, at, :] = mass
                fixed[2, y, w, at, :] = CW * conc * act
                fixed[3, y, w, at, :] = act * (conc * f[0] - mass * f[4])
                fixed[4, y, w, at, :] = act * (conc * f[1] - mass * f[5])
                fixed[5, y, w, at, :] = f[2]
                fixed[6, y, w, at, :] = f[3]
                fixed[7, y, w, at, :] = act

    tail = FRONT + height
    for k in range(2):
        for y in range(2):
            for w in range(2):
                state[k, y, w, tail : tail + 8, :] = blank
    for w in range(2):
        state[4, 1, w, 0:8, :] = blank
        cross[w, 0:8, :] = blank

    lane = lanes(8)
    last, start = lane == BX - 1, lane == 0
    both = [(y, w) for y in range(2) for w in range(2)]

    def subcycle(_, carry):
        for r in range(tiles):
            at = slice(8 * r, 8 * r + 8)
            lo = FRONT + 8 * r
            to, up1, down1 = slice(lo, lo + 8), slice(lo + 1, lo + 9), slice(lo - 1, lo + 7)
            u = {k: state[0, k[0], k[1], to, :] for k in both}
            v = {k: state[1, k[0], k[1], to, :] for k in both}
            un = {(0, w): u[1, w] for w in range(2)} | {(1, w): state[0, 0, w, up1, :] for w in range(2)}
            vn = {(0, w): v[1, w] for w in range(2)} | {(1, w): state[1, 0, w, up1, :] for w in range(2)}
            a, c, s12 = {}, {}, {}
            for y in range(2):
                ue = east_of(u[y, 0], u[y, 1], last)
                ve = east_of(v[y, 0], v[y, 1], last)
                for w in range(2):
                    k = y, w
                    sxx = ue[w] - u[k]
                    syy = vn[k] - v[k]
                    shear = (un[k] - u[k]) + (ve[w] - v[k])
                    div, ten = sxx + syy, sxx - syy
                    x = div * div + ((ten * ten + shear * shear) * 0.25 + 0.25)
                    inv = lax.rsqrt(x)
                    kr = fixed[0, y, w, at, :] * inv
                    t1 = state[2, y, w, to, :] * (2.0 / 3.0) + kr * (div - x * inv)
                    t2 = state[3, y, w, to, :] * (2.0 / 3.0) + kr * (ten * 0.25)
                    t3 = state[4, y, w, to, :] * (2.0 / 3.0) + kr * (shear * 0.125)
                    state[2, y, w, to, :] = t1
                    state[3, y, w, to, :] = t2
                    state[4, y, w, to, :] = t3
                    s12[k] = t3
                    a[k] = 0.5 * (t1 + t2)
                    c[k] = 0.5 * (t1 - t2)
            for w in range(2):
                cross[w, to, :] = c[1, w]
            for y in range(2):
                aw = west_of(a[y, 0], a[y, 1], start)
                sw = west_of(s12[y, 0], s12[y, 1], start)
                for w in range(2):
                    k = y, w
                    if y == 1:
                        s12s, cs = s12[0, w], c[0, w]
                    else:
                        s12s, cs = state[4, 1, w, down1, :], cross[w, down1, :]
                    fx = (a[k] - aw[w]) + (s12[k] - s12s)
                    fy = (s12[k] - sw[w]) + (c[k] - cs)
                    mass, base = fixed[1, y, w, at, :], fixed[2, y, w, at, :]
                    cx, cy = fixed[5, y, w, at, :], fixed[6, y, w, at, :]
                    dx, dy = cx - u[k], cy - v[k]
                    drag = base * jnp.sqrt(dx * dx + dy * dy + DRAG_FLOOR)
                    m2 = mass * 2.0
                    part = fixed[7, y, w, at, :] / (jnp.maximum(m2, 1.0) + drag)
                    mc = CORIO * mass
                    state[0, y, w, to, :] = part * (m2 * u[k] + fx + fixed[3, y, w, at, :] + drag * cx + mc * v[k])
                    state[1, y, w, to, :] = part * (m2 * v[k] + fy + fixed[4, y, w, at, :] + drag * cy - mc * u[k])
        return carry

    lax.fori_loop(0, NSUB, subcycle, 0)

    for r in range(tiles):
        at = slice(8 * r, 8 * r + 8)
        to = slice(FRONT + 8 * r, FRONT + 8 * r + 8)
        for y in range(2):
            base = fixed[2, y, 0, at, :]
            dx = state[0, y, 0, to, :] - fixed[5, y, 0, at, :]
            dy = state[1, y, 0, to, :] - fixed[6, y, 0, at, :]
            factor = base * jnp.sqrt(dx * dx + dy * dy + DRAG_FLOOR)
            for k, x in enumerate((factor * dx, factor * dy, base * (1.0 / CW))):
                out8[pl.ds(64 * r + 2 * k + y, 8, stride=8), :] = x
    for y in range(2):
        for k in range(2):
            moved[k, :, y * BX : (y + 1) * BX] = state[k, y, 0, FRONT + 2 : FRONT + 2 + count, :]

    def answer(o, _):
        for j in range(per):
            b = pl.multiple_of((ids[o, j] + 2) * 8, 8)
            back[o, 6 * j : 6 * j + 6, :] = out8[pl.ds(b, 6), :]
        return 0

    lax.fori_loop(0, n, answer, 0)


def ice_step(ids, recv, ice, active, sides, below, above):
    n, per = ids.shape[0], ids.shape[1] // 3
    count = n * per
    height = (count + 4 + 7) // 8 * 8
    tall = height + 2 * FRONT
    scratch = [
        (height * STEP, BX), (height, BX), (height, BX), (8, 2, 2, height, BX),
        (5, 2, 2, tall, BX), (8, 2, 2, height, BX), (2, tall, BX), (height * 8, BX),
    ]
    return pl.pallas_call(
        functools.partial(ice_kernel, n, per, count),
        out_shape=[f32(n, 6 * per, BX), f32(2, count, 2 * BX)],
        in_specs=[SMEM] + [VMEM] * 6,
        out_specs=[VMEM] * 2,
        scratch_shapes=[pltpu.VMEM(s, jnp.float32) for s in scratch],
        name="ice_step",
    )(ids, recv, ice, active, sides, below, above)


def final_kernel(n, per, flag, got, raw, moved, out):
    @pl.when(flag[0] == 0)
    def _():
        def tile(t, _):
            for y in range(2):
                cells = slice(y * BX, (y + 1) * BX)
                wx, wy, cx, cy, rho = [raw[ch, t, :, cells] for ch in (0, 1, 2, 3, 6)]
                rx, ry = wx - cx, wy - cy
                speed = jnp.sqrt(rx * rx + ry * ry + 1.0)
                scale = rho * (0.1 + 0.05 * speed) * speed
                gx, gy, gc = [got[t, pl.ds(2 * k + y, per, stride=6), :] for k in range(3)]
                rest = (1.0 - gc) * scale
                out[0, t, :, cells] = gx + rest * rx
                out[1, t, :, cells] = gy + rest * ry
            return 0

        lax.fori_loop(0, n, tile, 0)

    @pl.when(flag[0] != 0)
    def _():
        out[...] = moved[...]


def final(flag, got, raw, moved):
    _, n, per, cells = raw.shape
    return pl.pallas_call(
        functools.partial(final_kernel, n, per),
        out_shape=f32(2, n, per, cells),
        in_specs=[SMEM] + [VMEM] * 3,
        out_specs=VMEM,
        name="final",
    )(flag, got, raw, moved)


def per_device(fields, block_owner, ice_covered, land_mask):
    nlat, nlon = lax.axis_size("lat"), lax.axis_size("lon")
    n = nlat * nlon
    count = block_owner.shape[0]
    per = count // n
    side = lax.axis_index("comp")
    fields = fields[0]
    local = (block_owner % count).reshape(nlat, nlon, per)
    idb = jnp.broadcast_to(local.reshape(n, per, 1), (n, per, BX))
    ids = jnp.concatenate([local, jnp.roll(local, 1, 1), jnp.roll(local, -1, 1)], 2).reshape(n, 3 * per)
    split = fields.reshape(7, n, per, 2 * BX)
    raw = lax.ppermute(split, "comp", [(0, 1)])
    pay = pack(raw, idb, nlat, nlon)
    active, ends = ice_ends(fields, ice_covered.reshape(count, 1), land_mask)

    def exchange(pay, ids, active, ends):
        recv = lax.all_to_all(pay, ("lat", "lon"), split_axis=0, concat_axis=0, tiled=True)
        owner = lax.all_to_all(ids, ("lat", "lon"), split_axis=0, concat_axis=0, tiled=True)
        ring = [(i, (i + 1) % nlon) for i in range(nlon)]
        west = lax.ppermute(ends, "lon", ring)
        east = lax.ppermute(ends, "lon", [(j, i) for i, j in ring])
        sides, north, south = ice_rows(fields, active, west, east)
        line = [(i, i + 1) for i in range(nlat - 1)]
        below = lax.ppermute(north, "lat", line)
        above = lax.ppermute(south, "lat", [(j, i) for i, j in line])
        return recv, owner, sides, below, above

    def stay(pay, ids, active, ends):
        row = jnp.zeros((34, BX), jnp.float32)
        return pay, ids, ends, row, row

    recv, owner, sides, below, above = lax.cond(side == 1, exchange, stay, pay, ids, active, ends)
    back, moved = ice_step(owner, recv, fields, active, sides, below, above)

    def send(back):
        return lax.all_to_all(back, ("lat", "lon"), split_axis=0, concat_axis=0, tiled=True)

    back = lax.cond(side == 1, send, lambda x: x, back)
    got = lax.ppermute(back, "comp", [(1, 0)])
    out = final(side.reshape(1), got, split, moved.reshape(2, n, per, 2 * BX))
    return out.reshape(1, 2, count, 2 * BX)


def solution(mesh):
    placed = (
        P("comp", None, ("lat", "lon"), None),
        P(("lat", "lon")),
        P(("lat", "lon")),
        P(("lat", "lon"), None),
    )
    return jax.shard_map(
        per_device,
        mesh=mesh,
        in_specs=placed,
        out_specs=P("comp", None, ("lat", "lon"), None),
        check_vma=False,
    )
```

```python
import functools

import jax
import jax.numpy as jnp
from jax import lax
from jax.experimental import pallas as pl
from jax.experimental.pallas import tpu as pltpu
from jax.sharding import PartitionSpec as P

BX = 128
NSUB = 4
FRONT = 8
STEP = 16

CD_ICE = 0.1
CW = 1.5
CSTAR = 2.0
CORIO = 0.3
DRAG_FLOOR = 0.1

VMEM = pl.BlockSpec(memory_space=pltpu.VMEM)
SMEM = pl.BlockSpec(memory_space=pltpu.SMEM)


def params(mib):
    return pltpu.CompilerParams(vmem_limit_bytes=mib * 1024 * 1024)


def f32(*shape):
    return jax.ShapeDtypeStruct(shape, jnp.float32)


def lanes(rows):
    return lax.broadcasted_iota(jnp.int32, (rows, BX), 1)


def roll(x, by):
    return pltpu.roll(x, by % BX, 1)


def at_end(q, west, east):
    return jnp.where(q, west, east)


def pack_body(nlat, nlon, per, count, raw, idb, pay, opened, edge, rim):
    n = nlat * nlon
    lane = lanes(per)
    group = lane // 8
    lat_base = 13 * per

    def tile(t, _):
        def half(ch, y):
            return raw[ch, t, :, y * BX : (y + 1) * BX]

        planes = [None] * 12
        for y in range(2):
            wx, wy, rho = half(0, y), half(1, y), half(6, y)
            scale = rho * CD_ICE * jnp.sqrt(wx * wx + wy * wy + 1.0)
            planes[y] = scale * wx
            planes[2 + y] = scale * wy
            for ch in range(2, 6):
                planes[2 * ch + y] = half(ch, y)
            rx, ry = wx - planes[4 + y], wy - planes[6 + y]
            speed = jnp.sqrt(rx * rx + ry * ry + 1.0)
            rate = rho * (0.1 + 0.05 * speed) * speed
            opened[t, 2 * y] = rate * rx
            opened[t, 2 * y + 1] = rate * ry
        ends = jnp.zeros((per, BX), jnp.float32)
        for p in range(12):
            pay[t, pl.ds(p, per, stride=12), :] = planes[p]
            ends = jnp.where(group == p, roll(planes[p], 8 * p + 4), ends)
        edge[t] = ends
        ids = idb[t]

        def pick(block, value):
            return jnp.sum(jnp.where(ids == block, value, 0.0), axis=0, keepdims=True)

        rows = [pick(0, x) for x in planes] + [pick(1, x) for x in planes[0::2]]
        rows += [pick(count - 1, x) for x in planes]
        rows += [pick(count - 2, x) for x in planes[1::2]]
        rows += [pick(b, ends) for b in (0, 1, count - 1, count - 2)]
        for k, row in enumerate(rows):
            rim[t, k : k + 1, :] = row
        return 0

    lax.fori_loop(0, n, tile, 0)

    def dest(d, _):
        i, j = d // nlon, d % nlon
        jw, je = (j + nlon - 1) % nlon, (j + 1) % nlon
        q8 = (lane % 8) < 4
        pay[d, 12 * per : 13 * per, :] = at_end(q8, edge[i * nlon + jw], edge[i * nlon + je])
        for ii, ok, lo, c in (
            (jnp.minimum(i + 1, nlat - 1), i + 1 < nlat, 0, 36),
            (jnp.maximum(i - 1, 0), i > 0, 18, 38),
        ):
            scale = jnp.where(ok, 1.0, 0.0)
            pay[d, lat_base + lo : lat_base + lo + 18, :] = rim[ii * nlon + j, lo : lo + 18, :] * scale
            q2 = (lanes(2) % 8) < 4
            corner = at_end(q2, rim[ii * nlon + jw, c : c + 2, :], rim[ii * nlon + je, c : c + 2, :])
            pay[d, lat_base + c : lat_base + c + 2, :] = corner * scale
        return 0

    lax.fori_loop(0, n, dest, 0)


def ends_body(ice, covered, land, active, ends):
    count = covered.shape[0]
    lane = lanes(count)
    group = lane // 8
    total = jnp.zeros((count, BX), jnp.float32)
    for y in range(2):
        cells = slice(y * BX, (y + 1) * BX)
        act = covered[...].astype(jnp.float32) * (1 - land[:, cells]).astype(jnp.float32)
        active[:, cells] = act
        for ch in range(8):
            x = act if ch == 7 else ice[ch, :, :, cells].reshape(count, BX)
            p = 2 * ch + y
            total = jnp.where(group == p, roll(x, 8 * p + 4), total)
    ends[...] = total


def first_kernel(nlat, nlon, per, flag, raw, idb, covered, land, pay, opened, active, ends, edge, rim):
    @pl.when(flag[0] == 0)
    def _():
        pack_body(nlat, nlon, per, nlat * nlon * per, raw, idb, pay, opened, edge, rim)

    @pl.when(flag[0] != 0)
    def _():
        ends_body(raw, covered, land, active, ends)


def first(flag, raw, idb, covered, land, nlat, nlon):
    _, n, per, _ = raw.shape
    count = n * per
    return pl.pallas_call(
        functools.partial(first_kernel, nlat, nlon, per),
        out_shape=[f32(n, 13 * per + 40, BX), f32(n, 4, per, BX), f32(count, 2 * BX), f32(count, BX)],
        in_specs=[SMEM] + [VMEM] * 4,
        out_specs=[VMEM] * 4,
        scratch_shapes=[pltpu.VMEM((n, per, BX), jnp.float32), pltpu.VMEM((n, 40, BX), jnp.float32)],
        compiler_params=params(12),
        name="first",
    )(flag, raw, idb, covered, land)


def rows_kernel(ice, active, west, east, sides, north, south):
    count = active.shape[0]
    q = (lanes(count) % 8) < 4
    sides[...] = jnp.where(q, west[...], east[...])
    for out, lo in ((north, count - 2), (south, 0)):
        for y in range(2):
            cells = slice(y * BX, (y + 1) * BX)
            for ch in range(8):
                p = 2 * ch + y
                x = active[lo : lo + 2, cells] if ch == 7 else ice[ch, lo : lo + 2, cells]
                out[2 * p : 2 * p + 2, :] = x
        out[32:34, :] = sides[lo : lo + 2, :]


def ice_rows(ice, active, west, east):
    count = active.shape[0]
    return pl.pallas_call(
        rows_kernel,
        out_shape=[f32(count, BX), f32(34, BX), f32(34, BX)],
        in_specs=[VMEM] * 4,
        out_specs=[VMEM] * 3,
        compiler_params=params(8),
        name="ice_rows",
    )(ice, active, west, east)


def east_of(first, second, last):
    a, b = roll(first, -1), roll(second, -1)
    return jnp.where(last, b, a), jnp.where(last, a, b)


def west_of(first, second, start):
    a, b = roll(first, 1), roll(second, 1)
    return jnp.where(start, b, a), jnp.where(start, a, b)


def prep_kernel(count, height, ice, active, sides, below, above, begin, still, grid):
    for ch in range(8):
        for y in range(2):
            p = 2 * ch + y
            cells = slice(y * BX, (y + 1) * BX)
            shift = -(8 * p + 4)
            grid[ch, y, 0, 2 : 2 + count, :] = active[:, cells] if ch == 7 else ice[ch, :, cells]
            grid[ch, y, 1, 2 : 2 + count, :] = roll(sides[...], shift)
            for lo, msg in ((0, below), (count + 2, above)):
                grid[ch, y, 0, lo : lo + 2, :] = msg[2 * p : 2 * p + 2, :]
                grid[ch, y, 1, lo : lo + 2, :] = roll(msg[32:34, :], shift)
            grid[ch, y, 0, count + 4 :, :] = jnp.zeros((height - count - 4, BX), jnp.float32)
            grid[ch, y, 1, count + 4 :, :] = jnp.zeros((height - count - 4, BX), jnp.float32)

    for r in range(height // 8):
        at = slice(8 * r, 8 * r + 8)
        for y in range(2):
            for w in range(2):
                u, v, mass, conc, s1, s2, s12, act = [grid[ch, y, w, at, :] for ch in range(8)]
                for k, x in enumerate((u, v, s1, s2, s12)):
                    begin[k, y, w, at, :] = x
                still[0, y, w, at, :] = mass * jnp.exp(CSTAR * (conc - 1.0)) * act * (1.0 / 3.0)
                still[1, y, w, at, :] = mass
                still[2, y, w, at, :] = CW * conc * act
                still[3, y, w, at, :] = act
                still[4, y, w, at, :] = conc


def prep(ice, active, sides, below, above):
    count = active.shape[0]
    height = (count + 4 + 7) // 8 * 8
    return pl.pallas_call(
        functools.partial(prep_kernel, count, height),
        out_shape=[f32(5, 2, 2, height, BX)] * 2,
        in_specs=[VMEM] * 5,
        out_specs=[VMEM] * 2,
        scratch_shapes=[pltpu.VMEM((8, 2, 2, height, BX), jnp.float32)],
        compiler_params=params(12),
        name="prep",
    )(ice, active, sides, below, above)


def ice_kernel(n, per, count, ids, recv, begin, still, back, moved,
               spot, hw, he, state, forced, cross, out8):
    tiles = (count + 4 + 7) // 8
    height = tiles * 8
    blank = jnp.zeros((8, BX), jnp.float32)
    for k in range(count + 4, height):
        spot[k * STEP : k * STEP + 8, :] = blank
        spot[k * STEP + 8 : k * STEP + 16, :] = blank
    for k in (0, height - 8):
        hw[k : k + 8, :] = blank
        he[k : k + 8, :] = blank
    spot[0:8, :] = blank
    spot[8:16, :] = blank
    end = (count + 3) * STEP
    spot[end : end + 8, :] = blank
    spot[end + 8 : end + 16, :] = blank

    def place(o, acc):
        for j in range(per):
            b = pl.multiple_of((ids[o, j] + 2) * STEP, STEP)
            spot[pl.ds(b, 12), :] = recv[o, 12 * j : 12 * j + 12, :]
            row = recv[o, 12 * per + j : 12 * per + j + 1, :]
            hw[pl.ds(ids[o, per + j] + 2, 1), :] = row
            he[pl.ds(ids[o, 2 * per + j] + 2, 1), :] = row
        return acc + recv[o, 13 * per : 13 * per + 40, :]

    rim = lax.fori_loop(0, n, place, jnp.zeros((40, BX), jnp.float32))
    up, down = (count + 2) * STEP, STEP
    spot[up : up + 12, :] = rim[0:12]
    spot[down : down + 12, :] = rim[18:30]
    for ch in range(6):
        k = up + STEP + 2 * ch
        spot[k : k + 1, :] = rim[12 + ch : 13 + ch]
        k = 2 * ch + 1
        spot[k : k + 1, :] = rim[30 + ch : 31 + ch]
    for ref in (hw, he):
        ref[count + 2 : count + 4, :] = rim[36:38]
        ref[1:2, :] = rim[38:39]
        ref[0:1, :] = rim[39:40]

    q = (lanes(8) % 8) < 4
    for r in range(tiles):
        at = slice(8 * r, 8 * r + 8)
        to = slice(FRONT + 8 * r, FRONT + 8 * r + 8)
        ends = jnp.where(q, hw[at, :], he[at, :])
        for y in range(2):
            for w in range(2):
                if w == 0:
                    f = [spot[pl.ds(8 * r * STEP + 2 * ch + y, 8, stride=STEP), :] for ch in range(6)]
                else:
                    f = [roll(ends, -(8 * (2 * ch + y) + 4)) for ch in range(6)]
                for k in range(5):
                    state[k, y, w, to, :] = begin[k, y, w, at, :]
                mass, act, conc = [still[k, y, w, at, :] for k in (1, 3, 4)]
                forced[0, y, w, at, :] = act * (conc * f[0] - mass * f[4])
                forced[1, y, w, at, :] = act * (conc * f[1] - mass * f[5])
                forced[2, y, w, at, :] = f[2]
                forced[3, y, w, at, :] = f[3]

    tail = FRONT + height
    for k in range(2):
        for y in range(2):
            for w in range(2):
                state[k, y, w, tail : tail + 8, :] = blank
    for w in range(2):
        state[4, 1, w, 0:8, :] = blank
        cross[w, 0:8, :] = blank

    lane = lanes(8)
    last, start = lane == BX - 1, lane == 0
    both = [(y, w) for y in range(2) for w in range(2)]

    def subcycle(_, carry):
        for r in range(tiles):
            at = slice(8 * r, 8 * r + 8)
            lo = FRONT + 8 * r
            to, up1, down1 = slice(lo, lo + 8), slice(lo + 1, lo + 9), slice(lo - 1, lo + 7)
            u = {k: state[0, k[0], k[1], to, :] for k in both}
            v = {k: state[1, k[0], k[1], to, :] for k in both}
            un = {(0, w): u[1, w] for w in range(2)} | {(1, w): state[0, 0, w, up1, :] for w in range(2)}
            vn = {(0, w): v[1, w] for w in range(2)} | {(1, w): state[1, 0, w, up1, :] for w in range(2)}
            a, c, s12 = {}, {}, {}
            for y in range(2):
                ue = east_of(u[y, 0], u[y, 1], last)
                ve = east_of(v[y, 0], v[y, 1], last)
                for w in range(2):
                    k = y, w
                    sxx = ue[w] - u[k]
                    syy = vn[k] - v[k]
                    shear = (un[k] - u[k]) + (ve[w] - v[k])
                    div, ten = sxx + syy, sxx - syy
                    x = div * div + ((ten * ten + shear * shear) * 0.25 + 0.25)
                    inv = lax.rsqrt(x)
                    kr = still[0, y, w, at, :] * inv
                    t1 = state[2, y, w, to, :] * (2.0 / 3.0) + kr * (div - x * inv)
                    t2 = state[3, y, w, to, :] * (2.0 / 3.0) + kr * (ten * 0.25)
                    t3 = state[4, y, w, to, :] * (2.0 / 3.0) + kr * (shear * 0.125)
                    state[2, y, w, to, :] = t1
                    state[3, y, w, to, :] = t2
                    state[4, y, w, to, :] = t3
                    s12[k] = t3
                    a[k] = 0.5 * (t1 + t2)
                    c[k] = 0.5 * (t1 - t2)
            for w in range(2):
                cross[w, to, :] = c[1, w]
            for y in range(2):
                aw = west_of(a[y, 0], a[y, 1], start)
                sw = west_of(s12[y, 0], s12[y, 1], start)
                for w in range(2):
                    k = y, w
                    if y == 1:
                        s12s, cs = s12[0, w], c[0, w]
                    else:
                        s12s, cs = state[4, 1, w, down1, :], cross[w, down1, :]
                    fx = (a[k] - aw[w]) + (s12[k] - s12s)
                    fy = (s12[k] - sw[w]) + (c[k] - cs)
                    mass, base = still[1, y, w, at, :], still[2, y, w, at, :]
                    cx, cy = forced[2, y, w, at, :], forced[3, y, w, at, :]
                    dx, dy = cx - u[k], cy - v[k]
                    y2 = dx * dx + dy * dy + DRAG_FLOOR
                    drag = base * (y2 * lax.rsqrt(y2))
                    m2 = mass * 2.0
                    part = still[3, y, w, at, :] / (jnp.maximum(m2, 1.0) + drag)
                    mc = CORIO * mass
                    state[0, y, w, to, :] = part * (m2 * u[k] + fx + forced[0, y, w, at, :] + drag * cx + mc * v[k])
                    state[1, y, w, to, :] = part * (m2 * v[k] + fy + forced[1, y, w, at, :] + drag * cy - mc * u[k])
        return carry

    lax.fori_loop(0, NSUB, subcycle, 0)

    for r in range(tiles):
        at = slice(8 * r, 8 * r + 8)
        to = slice(FRONT + 8 * r, FRONT + 8 * r + 8)
        for y in range(2):
            base = still[2, y, 0, at, :]
            dx = state[0, y, 0, to, :] - forced[2, y, 0, at, :]
            dy = state[1, y, 0, to, :] - forced[3, y, 0, at, :]
            factor = base * jnp.sqrt(dx * dx + dy * dy + DRAG_FLOOR)
            for k, x in enumerate((factor * dx, factor * dy, base * (1.0 / CW))):
                out8[pl.ds(64 * r + 2 * k + y, 8, stride=8), :] = x
    for y in range(2):
        for k in range(2):
            moved[k, :, y * BX : (y + 1) * BX] = state[k, y, 0, FRONT + 2 : FRONT + 2 + count, :]

    def answer(o, _):
        for j in range(per):
            b = pl.multiple_of((ids[o, j] + 2) * 8, 8)
            back[o, 6 * j : 6 * j + 6, :] = out8[pl.ds(b, 6), :]
        return 0

    lax.fori_loop(0, n, answer, 0)


def ice_step(ids, recv, begin, still):
    n, per = ids.shape[0], ids.shape[1] // 3
    count = n * per
    height = (count + 4 + 7) // 8 * 8
    tall = height + 2 * FRONT
    scratch = [
        (height * STEP, BX), (height, BX), (height, BX),
        (5, 2, 2, tall, BX), (4, 2, 2, height, BX), (2, tall, BX), (height * 8, BX),
    ]
    return pl.pallas_call(
        functools.partial(ice_kernel, n, per, count),
        out_shape=[f32(n, 6 * per, BX), f32(2, count, 2 * BX)],
        in_specs=[SMEM] + [VMEM] * 3,
        out_specs=[VMEM] * 2,
        scratch_shapes=[pltpu.VMEM(s, jnp.float32) for s in scratch],
        compiler_params=params(12),
        name="ice_step",
    )(ids, recv, begin, still)


def final_kernel(n, per, flag, got, opened, moved, out):
    @pl.when(flag[0] == 0)
    def _():
        def tile(t, _):
            for y in range(2):
                cells = slice(y * BX, (y + 1) * BX)
                gx, gy, gc = [got[t, pl.ds(2 * k + y, per, stride=6), :] for k in range(3)]
                out[0, t, :, cells] = gx + (1.0 - gc) * opened[t, 2 * y]
                out[1, t, :, cells] = gy + (1.0 - gc) * opened[t, 2 * y + 1]
            return 0

        lax.fori_loop(0, n, tile, 0)

    @pl.when(flag[0] != 0)
    def _():
        out[...] = moved[...]


def final(flag, got, opened, moved):
    n, _, per, _ = opened.shape
    return pl.pallas_call(
        functools.partial(final_kernel, n, per),
        out_shape=f32(2, n, per, 2 * BX),
        in_specs=[SMEM] + [VMEM] * 3,
        out_specs=VMEM,
        compiler_params=params(8),
        name="final",
    )(flag, got, opened, moved)


def per_device(fields, block_owner, ice_covered, land_mask):
    nlat, nlon = lax.axis_size("lat"), lax.axis_size("lon")
    n = nlat * nlon
    count = block_owner.shape[0]
    per = count // n
    side = lax.axis_index("comp")
    flag = side.reshape(1)
    fields = fields[0]
    local = (block_owner % count).reshape(nlat, nlon, per)
    idb = jnp.broadcast_to(local.reshape(n, per, 1), (n, per, BX))
    ids = jnp.concatenate([local, jnp.roll(local, 1, 1), jnp.roll(local, -1, 1)], 2).reshape(n, 3 * per)
    split = fields.reshape(7, n, per, 2 * BX)
    pay, opened, active, ends = first(flag, split, idb, ice_covered.reshape(count, 1), land_mask, nlat, nlon)
    pay = lax.ppermute(pay, "comp", [(0, 1)])
    every = ("comp", "lat", "lon")
    tiles = [(i, j) for i in range(nlat) for j in range(nlon)]
    east_pairs = [(n + i * nlon + j, n + i * nlon + (j + 1) % nlon) for i, j in tiles]
    west = lax.ppermute(ends, every, east_pairs)
    east = lax.ppermute(ends, every, [(j, i) for i, j in east_pairs])

    def everyone(x):
        return lax.all_to_all(x, ("lat", "lon"), split_axis=0, concat_axis=0, tiled=True)

    def ice_side(pay, ids, active, west, east):
        recv = everyone(pay)
        sides, north, south = ice_rows(fields, active, west, east)
        line = [(i, i + 1) for i in range(nlat - 1)]
        below = lax.ppermute(north, "lat", line)
        above = lax.ppermute(south, "lat", [(j, i) for i, j in line])
        return recv, ids, sides, below, above

    def ocean_side(pay, ids, active, west, east):
        row = jnp.zeros((34, BX), jnp.float32)
        return jnp.zeros(pay.shape, jnp.float32), everyone(ids), jnp.zeros(west.shape, jnp.float32), row, row

    recv, owner, sides, below, above = lax.cond(side == 1, ice_side, ocean_side, pay, ids, active, west, east)
    swap = lax.ppermute(owner, "comp", [(0, 1), (1, 0)])
    begin, still = prep(fields, active, sides, below, above)
    back, moved = ice_step(swap, recv, begin, still)
    back = lax.cond(side == 1, everyone, lambda x: x, back)
    got = lax.ppermute(back, "comp", [(1, 0)])
    out = final(flag, got, opened, moved.reshape(2, n, per, 2 * BX))
    return out.reshape(1, 2, count, 2 * BX)


def solution(mesh):
    placed = (
        P("comp", None, ("lat", "lon"), None),
        P(("lat", "lon")),
        P(("lat", "lon")),
        P(("lat", "lon"), None),
    )
    return jax.shard_map(
        per_device,
        mesh=mesh,
        in_specs=placed,
        out_specs=P("comp", None, ("lat", "lon"), None),
        check_vma=False,
    )
```

```python
import functools

import jax
import jax.numpy as jnp
from jax import lax
from jax.experimental import pallas as pl
from jax.experimental.pallas import tpu as pltpu
from jax.sharding import PartitionSpec as P

BX = 128
NSUB = 4
FRONT = 8
STEP = 13
REPLY = 7

CD_ICE = 0.1
CW = 1.5
CSTAR = 2.0
CORIO = 0.3
DRAG_FLOOR = 0.1

VMEM = pl.BlockSpec(memory_space=pltpu.VMEM)
SMEM = pl.BlockSpec(memory_space=pltpu.SMEM)


def params(mib):
    return pltpu.CompilerParams(vmem_limit_bytes=mib * 1024 * 1024)


def f32(*shape):
    return jax.ShapeDtypeStruct(shape, jnp.float32)


def lanes(rows):
    return lax.broadcasted_iota(jnp.int32, (rows, BX), 1)


def roll(x, by):
    return pltpu.roll(x, by % BX, 1)


def at_end(q, west, east):
    return jnp.where(q, west, east)


def column(row):
    parts = []
    for lo in range(0, row.shape[1], BX):
        diag = lax.broadcasted_iota(jnp.int32, (BX, BX), 0) == lanes(BX)
        parts.append(jnp.sum(jnp.where(diag, row[:, lo : lo + BX].astype(jnp.float32), 0.0), axis=1, keepdims=True))
    return jnp.concatenate(parts, 0) if len(parts) > 1 else parts[0]


def pack_body(nlat, nlon, per, count, raw, owner, pay, opened, edge, rim, idb):
    n = nlat * nlon
    idb[...] = jnp.broadcast_to(column(owner[...]), (count, BX)).astype(jnp.int32)
    lane = lanes(per)
    group = lane // 8
    lat_base = 13 * per

    def tile(t, _):
        def half(ch, y):
            return raw[ch, t, :, y * BX : (y + 1) * BX]

        planes = [None] * 12
        for y in range(2):
            wx, wy, rho = half(0, y), half(1, y), half(6, y)
            scale = rho * CD_ICE * jnp.sqrt(wx * wx + wy * wy + 1.0)
            planes[y] = scale * wx
            planes[2 + y] = scale * wy
            for ch in range(2, 6):
                planes[2 * ch + y] = half(ch, y)
            rx, ry = wx - planes[4 + y], wy - planes[6 + y]
            speed = jnp.sqrt(rx * rx + ry * ry + 1.0)
            rate = rho * (0.1 + 0.05 * speed) * speed
            opened[t, 2 * y] = rate * rx
            opened[t, 2 * y + 1] = rate * ry
        ends = jnp.zeros((per, BX), jnp.float32)
        for p in range(12):
            pay[t, pl.ds(p, per, stride=12), :] = planes[p]
            ends = jnp.where(group == p, roll(planes[p], 8 * p + 4), ends)
        edge[t] = ends
        spot = t * per
        ids = idb[pl.ds(pl.multiple_of(spot, per), per), :] - t * count

        def pick(block, value):
            return jnp.sum(jnp.where(ids == block, value, 0.0), axis=0, keepdims=True)

        rows = [pick(0, x) for x in planes] + [pick(1, x) for x in planes[0::2]]
        rows += [pick(count - 1, x) for x in planes]
        rows += [pick(count - 2, x) for x in planes[1::2]]
        rows += [pick(b, ends) for b in (0, 1, count - 1, count - 2)]
        for k, row in enumerate(rows):
            rim[t, k : k + 1, :] = row
        return 0

    lax.fori_loop(0, n, tile, 0)

    def dest(d, _):
        i, j = d // nlon, d % nlon
        jw, je = (j + nlon - 1) % nlon, (j + 1) % nlon
        q8 = (lane % 8) < 4
        pay[d, 12 * per : 13 * per, :] = at_end(q8, edge[i * nlon + jw], edge[i * nlon + je])
        for ii, ok, lo, c in (
            (jnp.minimum(i + 1, nlat - 1), i + 1 < nlat, 0, 36),
            (jnp.maximum(i - 1, 0), i > 0, 18, 38),
        ):
            scale = jnp.where(ok, 1.0, 0.0)
            pay[d, lat_base + lo : lat_base + lo + 18, :] = rim[ii * nlon + j, lo : lo + 18, :] * scale
            q2 = (lanes(2) % 8) < 4
            corner = at_end(q2, rim[ii * nlon + jw, c : c + 2, :], rim[ii * nlon + je, c : c + 2, :])
            pay[d, lat_base + c : lat_base + c + 2, :] = corner * scale
        return 0

    lax.fori_loop(0, n, dest, 0)


def ends_body(ice, covered, land, active, ends):
    count = covered.shape[1]
    lane = lanes(count)
    group = lane // 8
    total = jnp.zeros((count, BX), jnp.float32)
    cover = column(covered[...])
    for y in range(2):
        cells = slice(y * BX, (y + 1) * BX)
        act = cover * (1 - land[:, cells]).astype(jnp.float32)
        active[:, cells] = act
        for ch in range(8):
            x = act if ch == 7 else ice[ch, :, :, cells].reshape(count, BX)
            p = 2 * ch + y
            total = jnp.where(group == p, roll(x, 8 * p + 4), total)
    ends[...] = total


def first_kernel(nlat, nlon, per, flag, raw, owner, covered, land, pay, opened, active, ends, edge, rim, idb):
    @pl.when(flag[0] == 0)
    def _():
        pack_body(nlat, nlon, per, nlat * nlon * per, raw, owner, pay, opened, edge, rim, idb)

    @pl.when(flag[0] != 0)
    def _():
        ends_body(raw, covered, land, active, ends)


def first(flag, raw, owner, covered, land, nlat, nlon):
    _, n, per, _ = raw.shape
    count = n * per
    return pl.pallas_call(
        functools.partial(first_kernel, nlat, nlon, per),
        out_shape=[f32(n, 13 * per + 40, BX), f32(n, 4, per, BX), f32(count, 2 * BX), f32(count, BX)],
        in_specs=[SMEM] + [VMEM] * 4,
        out_specs=[VMEM] * 4,
        scratch_shapes=[pltpu.VMEM((n, per, BX), jnp.float32), pltpu.VMEM((n, 40, BX), jnp.float32),
                        pltpu.VMEM((count, BX), jnp.int32)],
        compiler_params=params(12),
        name="first",
    )(flag, raw, owner, covered, land)


def rows_kernel(ice, active, west, east, sides, north, south):
    count = active.shape[0]
    q = (lanes(count) % 8) < 4
    sides[...] = jnp.where(q, west[...], east[...])
    for out, lo in ((north, count - 2), (south, 0)):
        for y in range(2):
            cells = slice(y * BX, (y + 1) * BX)
            for ch in range(8):
                p = 2 * ch + y
                x = active[lo : lo + 2, cells] if ch == 7 else ice[ch, lo : lo + 2, cells]
                out[2 * p : 2 * p + 2, :] = x
        out[32:34, :] = sides[lo : lo + 2, :]


def ice_rows(ice, active, west, east):
    count = active.shape[0]
    return pl.pallas_call(
        rows_kernel,
        out_shape=[f32(count, BX), f32(34, BX), f32(34, BX)],
        in_specs=[VMEM] * 4,
        out_specs=[VMEM] * 3,
        compiler_params=params(8),
        name="ice_rows",
    )(ice, active, west, east)


def east_of(first, second, last):
    a, b = roll(first, -1), roll(second, -1)
    return jnp.where(last, b, a), jnp.where(last, a, b)


def west_of(first, second, start):
    a, b = roll(first, 1), roll(second, 1)
    return jnp.where(start, b, a), jnp.where(start, a, b)


def prep_kernel(count, height, ice, active, sides, below, above, begin, still, grid):
    for ch in range(8):
        for y in range(2):
            p = 2 * ch + y
            cells = slice(y * BX, (y + 1) * BX)
            shift = -(8 * p + 4)
            grid[ch, y, 0, 2 : 2 + count, :] = active[:, cells] if ch == 7 else ice[ch, :, cells]
            grid[ch, y, 1, 2 : 2 + count, :] = roll(sides[...], shift)
            for lo, msg in ((0, below), (count + 2, above)):
                grid[ch, y, 0, lo : lo + 2, :] = msg[2 * p : 2 * p + 2, :]
                grid[ch, y, 1, lo : lo + 2, :] = roll(msg[32:34, :], shift)
            grid[ch, y, 0, count + 4 :, :] = jnp.zeros((height - count - 4, BX), jnp.float32)
            grid[ch, y, 1, count + 4 :, :] = jnp.zeros((height - count - 4, BX), jnp.float32)

    for r in range(height // 8):
        at = slice(8 * r, 8 * r + 8)
        for y in range(2):
            for w in range(2):
                u, v, mass, conc, s1, s2, s12, act = [grid[ch, y, w, at, :] for ch in range(8)]
                for k, x in enumerate((u, v, 0.5 * s1, 0.5 * s2, s12)):
                    begin[k, y, w, at, :] = x
                still[0, y, w, at, :] = mass * jnp.exp(CSTAR * (conc - 1.0)) * act * (1.0 / 6.0)
                still[1, y, w, at, :] = 2.0 * mass
                still[2, y, w, at, :] = CW * conc * act
                still[3, y, w, at, :] = act
                still[4, y, w, at, :] = conc


def prep(ice, active, sides, below, above):
    count = active.shape[0]
    height = (count + 4 + 7) // 8 * 8
    return pl.pallas_call(
        functools.partial(prep_kernel, count, height),
        out_shape=[f32(5, 2, 2, height, BX)] * 2,
        in_specs=[VMEM] * 5,
        out_specs=[VMEM] * 2,
        scratch_shapes=[pltpu.VMEM((8, 2, 2, height, BX), jnp.float32)],
        compiler_params=params(12),
        name="prep",
    )(ice, active, sides, below, above)


def ice_kernel(n, per, count, ids, recv, begin, still, back, moved,
               spot, hw, he, state, forced, cross, out8):
    tiles = (count + 4 + 7) // 8
    height = tiles * 8
    blank = jnp.zeros((8, BX), jnp.float32)
    for k in (0, 8):
        spot[k : k + 8, :] = blank
    for k in range((count + 3) * STEP, height * STEP, 8):
        spot[k : k + 8, :] = blank
    for k in (0, height - 8):
        hw[k : k + 8, :] = blank
        he[k : k + 8, :] = blank

    def place(o, acc):
        for j in range(per):
            b = (ids[o, j] + 2) * STEP
            spot[pl.ds(b, 12), :] = recv[o, 12 * j : 12 * j + 12, :]
            row = recv[o, 12 * per + j : 12 * per + j + 1, :]
            hw[pl.ds(ids[o, per + j] + 2, 1), :] = row
            he[pl.ds(ids[o, 2 * per + j] + 2, 1), :] = row
        return acc + recv[o, 13 * per : 13 * per + 40, :]

    rim = lax.fori_loop(0, n, place, jnp.zeros((40, BX), jnp.float32))
    up, down = (count + 2) * STEP, STEP
    spot[up : up + 12, :] = rim[0:12]
    spot[down : down + 12, :] = rim[18:30]
    for ch in range(6):
        k = up + STEP + 2 * ch
        spot[k : k + 1, :] = rim[12 + ch : 13 + ch]
        k = 2 * ch + 1
        spot[k : k + 1, :] = rim[30 + ch : 31 + ch]
    for ref in (hw, he):
        ref[count + 2 : count + 4, :] = rim[36:38]
        ref[1:2, :] = rim[38:39]
        ref[0:1, :] = rim[39:40]

    q = (lanes(8) % 8) < 4
    for r in range(tiles):
        at = slice(8 * r, 8 * r + 8)
        to = slice(FRONT + 8 * r, FRONT + 8 * r + 8)
        ends = jnp.where(q, hw[at, :], he[at, :])
        for y in range(2):
            for w in range(2):
                if w == 0:
                    f = [spot[pl.ds(8 * r * STEP + 2 * ch + y, 8, stride=STEP), :] for ch in range(6)]
                else:
                    f = [roll(ends, -(8 * (2 * ch + y) + 4)) for ch in range(6)]
                for k in range(5):
                    state[k, y, w, to, :] = begin[k, y, w, at, :]
                mass, act, conc = [still[k, y, w, at, :] for k in (1, 3, 4)]
                mass = 0.5 * mass
                forced[0, y, w, at, :] = act * (conc * f[0] - mass * f[4])
                forced[1, y, w, at, :] = act * (conc * f[1] - mass * f[5])
                forced[2, y, w, at, :] = f[2]
                forced[3, y, w, at, :] = f[3]

    tail = FRONT + height
    for k in range(2):
        for y in range(2):
            for w in range(2):
                state[k, y, w, tail : tail + 8, :] = blank
    for w in range(2):
        state[4, 1, w, 0:8, :] = blank
        cross[w, 0:8, :] = blank

    lane = lanes(8)
    last, start = lane == BX - 1, lane == 0
    both = [(y, w) for y in range(2) for w in range(2)]

    def subcycle(_, carry):
        for r in range(tiles):
            at = slice(8 * r, 8 * r + 8)
            lo = FRONT + 8 * r
            to, up1, down1 = slice(lo, lo + 8), slice(lo + 1, lo + 9), slice(lo - 1, lo + 7)
            u = {k: state[0, k[0], k[1], to, :] for k in both}
            v = {k: state[1, k[0], k[1], to, :] for k in both}
            un = {(0, w): u[1, w] for w in range(2)} | {(1, w): state[0, 0, w, up1, :] for w in range(2)}
            vn = {(0, w): v[1, w] for w in range(2)} | {(1, w): state[1, 0, w, up1, :] for w in range(2)}
            a, c, s12 = {}, {}, {}
            for y in range(2):
                ue = east_of(u[y, 0], u[y, 1], last)
                ve = east_of(v[y, 0], v[y, 1], last)
                for w in range(2):
                    k = y, w
                    sxx = ue[w] - u[k]
                    syy = vn[k] - v[k]
                    shear = (un[k] - u[k]) + (ve[w] - v[k])
                    div, ten = sxx + syy, sxx - syy
                    twice = div + div
                    inv = lax.rsqrt(twice * twice + (ten * ten + shear * shear) + 1.0)
                    hard = still[0, y, w, at, :]
                    kr = hard * inv
                    half = 0.5 * kr
                    t1 = (state[2, y, w, to, :] * (2.0 / 3.0) - hard) + kr * twice
                    t2 = state[3, y, w, to, :] * (2.0 / 3.0) + half * ten
                    t3 = state[4, y, w, to, :] * (2.0 / 3.0) + half * shear
                    state[2, y, w, to, :] = t1
                    state[3, y, w, to, :] = t2
                    state[4, y, w, to, :] = t3
                    s12[k] = t3
                    a[k] = t1 + t2
                    c[k] = t1 - t2
            for w in range(2):
                cross[w, to, :] = c[1, w]
            for y in range(2):
                aw = west_of(a[y, 0], a[y, 1], start)
                sw = west_of(s12[y, 0], s12[y, 1], start)
                for w in range(2):
                    k = y, w
                    if y == 1:
                        s12s, cs = s12[0, w], c[0, w]
                    else:
                        s12s, cs = state[4, 1, w, down1, :], cross[w, down1, :]
                    fx = (a[k] - aw[w]) + (s12[k] - s12s)
                    fy = (s12[k] - sw[w]) + (c[k] - cs)
                    m2, base = still[1, y, w, at, :], still[2, y, w, at, :]
                    cx, cy = forced[2, y, w, at, :], forced[3, y, w, at, :]
                    dx, dy = cx - u[k], cy - v[k]
                    y2 = dx * dx + dy * dy + DRAG_FLOOR
                    drag = base * (y2 * lax.rsqrt(y2))
                    part = still[3, y, w, at, :] * (1.0 / (jnp.maximum(m2, 1.0) + drag))
                    mc = (0.5 * CORIO) * m2
                    state[0, y, w, to, :] = part * (m2 * u[k] + fx + forced[0, y, w, at, :] + drag * cx + mc * v[k])
                    state[1, y, w, to, :] = part * (m2 * v[k] + fy + forced[1, y, w, at, :] + drag * cy - mc * u[k])
        return carry

    lax.fori_loop(0, NSUB, subcycle, 0)

    for r in range(tiles):
        at = slice(8 * r, 8 * r + 8)
        to = slice(FRONT + 8 * r, FRONT + 8 * r + 8)
        for y in range(2):
            base = still[2, y, 0, at, :]
            dx = state[0, y, 0, to, :] - forced[2, y, 0, at, :]
            dy = state[1, y, 0, to, :] - forced[3, y, 0, at, :]
            factor = base * jnp.sqrt(dx * dx + dy * dy + DRAG_FLOOR)
            for k, x in enumerate((factor * dx, factor * dy, base * (1.0 / CW))):
                out8[pl.ds(8 * r * REPLY + 2 * k + y, 8, stride=REPLY), :] = x
    for y in range(2):
        for k in range(2):
            moved[k, :, y * BX : (y + 1) * BX] = state[k, y, 0, FRONT + 2 : FRONT + 2 + count, :]

    def answer(o, _):
        for j in range(per):
            b = (ids[o, j] + 2) * REPLY
            back[o, 6 * j : 6 * j + 6, :] = out8[pl.ds(b, 6), :]
        return 0

    lax.fori_loop(0, n, answer, 0)


def ice_step(ids, recv, begin, still):
    n, per = ids.shape[0], ids.shape[1] // 3
    count = n * per
    height = (count + 4 + 7) // 8 * 8
    tall = height + 2 * FRONT
    scratch = [
        (height * STEP + 8, BX), (height, BX), (height, BX),
        (5, 2, 2, tall, BX), (4, 2, 2, height, BX), (2, tall, BX), (height * REPLY + 8, BX),
    ]
    return pl.pallas_call(
        functools.partial(ice_kernel, n, per, count),
        out_shape=[f32(n, 6 * per, BX), f32(2, count, 2 * BX)],
        in_specs=[SMEM] + [VMEM] * 3,
        out_specs=[VMEM] * 2,
        scratch_shapes=[pltpu.VMEM(s, jnp.float32) for s in scratch],
        compiler_params=params(12),
        name="ice_step",
    )(ids, recv, begin, still)


def final_kernel(n, per, flag, got, opened, moved, out):
    @pl.when(flag[0] == 0)
    def _():
        def tile(t, _):
            for y in range(2):
                cells = slice(y * BX, (y + 1) * BX)
                gx, gy, gc = [got[t, pl.ds(2 * k + y, per, stride=6), :] for k in range(3)]
                out[0, t, :, cells] = gx + (1.0 - gc) * opened[t, 2 * y]
                out[1, t, :, cells] = gy + (1.0 - gc) * opened[t, 2 * y + 1]
            return 0

        lax.fori_loop(0, n, tile, 0)

    @pl.when(flag[0] != 0)
    def _():
        out[...] = moved[...]


def final(flag, got, opened, moved):
    n, _, per, _ = opened.shape
    return pl.pallas_call(
        functools.partial(final_kernel, n, per),
        out_shape=f32(2, n, per, 2 * BX),
        in_specs=[SMEM] + [VMEM] * 3,
        out_specs=VMEM,
        compiler_params=params(8),
        name="final",
    )(flag, got, opened, moved)


def per_device(fields, block_owner, ice_covered, land_mask):
    nlat, nlon = lax.axis_size("lat"), lax.axis_size("lon")
    n = nlat * nlon
    count = block_owner.shape[0]
    per = count // n
    side = lax.axis_index("comp")
    flag = side.reshape(1)
    fields = fields[0]
    local = (block_owner % count).reshape(nlat, nlon, per)
    ids = jnp.concatenate([local, jnp.roll(local, 1, 1), jnp.roll(local, -1, 1)], 2).reshape(n, 3 * per)
    split = fields.reshape(7, n, per, 2 * BX)
    pay, opened, active, ends = first(
        flag, split, block_owner.reshape(1, count), ice_covered.reshape(1, count), land_mask, nlat, nlon
    )
    pay = lax.ppermute(pay, "comp", [(0, 1)])
    def everyone(x):
        return lax.all_to_all(x, ("lat", "lon"), split_axis=0, concat_axis=0, tiled=True)

    def ice_side(pay, ids, active, ends):
        recv = everyone(pay)
        ring = [(i, (i + 1) % nlon) for i in range(nlon)]
        west = lax.ppermute(ends, "lon", ring)
        east = lax.ppermute(ends, "lon", [(j, i) for i, j in ring])
        sides, north, south = ice_rows(fields, active, west, east)
        line = [(i, i + 1) for i in range(nlat - 1)]
        below = lax.ppermute(north, "lat", line)
        above = lax.ppermute(south, "lat", [(j, i) for i, j in line])
        return recv, ids, sides, below, above

    def ocean_side(pay, ids, active, ends):
        row = ends[:34]
        return jnp.zeros(pay.shape, jnp.float32), everyone(ids), ends, row, row

    recv, owner, sides, below, above = lax.cond(side == 1, ice_side, ocean_side, pay, ids, active, ends)
    swap = lax.ppermute(owner, "comp", [(0, 1), (1, 0)])
    begin, still = prep(fields, active, sides, below, above)
    back, moved = ice_step(swap, recv, begin, still)
    back = lax.cond(side == 1, everyone, lambda x: x, back)
    got = lax.ppermute(back, "comp", [(1, 0)])
    out = final(flag, got, opened, moved.reshape(2, n, per, 2 * BX))
    return out.reshape(1, 2, count, 2 * BX)


def solution(mesh):
    placed = (
        P("comp", None, ("lat", "lon"), None),
        P(("lat", "lon")),
        P(("lat", "lon")),
        P(("lat", "lon"), None),
    )
    return jax.shard_map(
        per_device,
        mesh=mesh,
        in_specs=placed,
        out_specs=P("comp", None, ("lat", "lon"), None),
        check_vma=False,
    )
```

```python
import functools

import jax
import jax.numpy as jnp
from jax import lax
from jax.experimental import pallas as pl
from jax.experimental.pallas import tpu as pltpu
from jax.sharding import PartitionSpec as P

BX = 128
NSUB = 4
FRONT = 8
STEP = 13
REPLY = 7
PARTS = 4

CD_ICE = 0.1
CW = 1.5
CSTAR = 2.0
CORIO = 0.3
DRAG_FLOOR = 0.1

VMEM = pl.BlockSpec(memory_space=pltpu.VMEM)
SMEM = pl.BlockSpec(memory_space=pltpu.SMEM)


def params(mib):
    return pltpu.CompilerParams(vmem_limit_bytes=mib * 1024 * 1024)


def f32(*shape):
    return jax.ShapeDtypeStruct(shape, jnp.float32)


def lanes(rows):
    return lax.broadcasted_iota(jnp.int32, (rows, BX), 1)


def roll(x, by):
    return pltpu.roll(x, by % BX, 1)


def at_end(q, west, east):
    return jnp.where(q, west, east)


def column(row):
    parts = []
    for lo in range(0, row.shape[1], BX):
        diag = lax.broadcasted_iota(jnp.int32, (BX, BX), 0) == lanes(BX)
        parts.append(jnp.sum(jnp.where(diag, row[:, lo : lo + BX].astype(jnp.float32), 0.0), axis=1, keepdims=True))
    return jnp.concatenate(parts, 0) if len(parts) > 1 else parts[0]


def pack_body(nlat, nlon, per, count, raw, owner, pay, opened, edge, rim, idb, parts, field):
    n = nlat * nlon
    idb[...] = jnp.broadcast_to(column(owner[...]), (count, BX)).astype(jnp.int32)
    lane = lanes(per)
    group = lane // 8
    lat_base = 13 * per

    def tile(t, _):
        def half(ch, y):
            return raw[ch, t, :, y * BX : (y + 1) * BX]

        planes = [None] * 12
        for y in range(2):
            wx, wy, rho = half(0, y), half(1, y), half(6, y)
            scale = rho * CD_ICE * jnp.sqrt(wx * wx + wy * wy + 1.0)
            planes[y] = scale * wx
            planes[2 + y] = scale * wy
            for ch in range(2, 6):
                planes[2 * ch + y] = half(ch, y)
            rx, ry = wx - planes[4 + y], wy - planes[6 + y]
            speed = jnp.sqrt(rx * rx + ry * ry + 1.0)
            rate = rho * (0.1 + 0.05 * speed) * speed
            opened[t, 2 * y] = rate * rx
            opened[t, 2 * y + 1] = rate * ry
        ends = jnp.zeros((per, BX), jnp.float32)
        for p in range(12):
            pay[t, pl.ds(p, per, stride=12), :] = planes[p]
            ends = jnp.where(group == p, roll(planes[p], 8 * p + 4), ends)
        edge[t] = ends
        spot = t * per
        ids = idb[pl.ds(pl.multiple_of(spot, per), per), :] - t * count

        def pick(block, value):
            return jnp.sum(jnp.where(ids == block, value, 0.0), axis=0, keepdims=True)

        rows = [pick(0, x) for x in planes] + [pick(1, x) for x in planes[0::2]]
        rows += [pick(count - 1, x) for x in planes]
        rows += [pick(count - 2, x) for x in planes[1::2]]
        rows += [pick(b, ends) for b in (0, 1, count - 1, count - 2)]
        for k, row in enumerate(rows):
            rim[t, k : k + 1, :] = row
        return 0

    for c in range(parts):
        field(c).wait()
        lax.fori_loop(c * (n // parts), (c + 1) * (n // parts), tile, 0)

    def dest(d, _):
        i, j = d // nlon, d % nlon
        jw, je = (j + nlon - 1) % nlon, (j + 1) % nlon
        q8 = (lane % 8) < 4
        pay[d, 12 * per : 13 * per, :] = at_end(q8, edge[i * nlon + jw], edge[i * nlon + je])
        for ii, ok, lo, c in (
            (jnp.minimum(i + 1, nlat - 1), i + 1 < nlat, 0, 36),
            (jnp.maximum(i - 1, 0), i > 0, 18, 38),
        ):
            scale = jnp.where(ok, 1.0, 0.0)
            pay[d, lat_base + lo : lat_base + lo + 18, :] = rim[ii * nlon + j, lo : lo + 18, :] * scale
            q2 = (lanes(2) % 8) < 4
            corner = at_end(q2, rim[ii * nlon + jw, c : c + 2, :], rim[ii * nlon + je, c : c + 2, :])
            pay[d, lat_base + c : lat_base + c + 2, :] = corner * scale
        return 0

    lax.fori_loop(0, n, dest, 0)


def ends_body(ice, covered, land, active, ends):
    count = covered.shape[1]
    lane = lanes(count)
    group = lane // 8
    total = jnp.zeros((count, BX), jnp.float32)
    cover = column(covered[...])
    for y in range(2):
        cells = slice(y * BX, (y + 1) * BX)
        act = cover * (1 - land[:, cells]).astype(jnp.float32)
        active[:, cells] = act
        for ch in range(8):
            x = act if ch == 7 else ice[ch, :, :, cells].reshape(count, BX)
            p = 2 * ch + y
            total = jnp.where(group == p, roll(x, 8 * p + 4), total)
    ends[...] = total


def first_kernel(nlat, nlon, per, raw_in, owner_in, cover_in, land_in, pay, opened, active, ends,
                 raw, owner, cover, land, edge, rim, idb, sems):
    n = nlat * nlon
    parts = PARTS if n % PARTS == 0 else 1
    step = n // parts

    def field(c):
        at = pl.ds(c * step, step)
        return pltpu.make_async_copy(raw_in.at[:, at], raw.at[:, at], sems.at[c])

    is_ocean = lax.axis_index("comp") == 0

    @pl.when(is_ocean)
    def _():
        ids = pltpu.make_async_copy(owner_in, owner, sems.at[PARTS])
        ids.start()
        for c in range(parts):
            field(c).start()
        ids.wait()
        pack_body(nlat, nlon, per, n * per, raw, owner, pay, opened, edge, rim, idb, parts, field)

    @pl.when(jnp.logical_not(is_ocean))
    def _():
        mask = pltpu.make_async_copy(land_in, land, sems.at[PARTS + 1])
        blocks = pltpu.make_async_copy(cover_in, cover, sems.at[PARTS + 2])
        blocks.start()
        mask.start()
        for c in range(parts):
            field(c).start()
        blocks.wait()
        mask.wait()
        for c in range(parts):
            field(c).wait()
        ends_body(raw, cover, land, active, ends)


def first(raw, owner, covered, land, nlat, nlon):
    _, n, per, cells = raw.shape
    count = n * per
    return pl.pallas_call(
        functools.partial(first_kernel, nlat, nlon, per),
        out_shape=[f32(n, 13 * per + 40, BX), f32(n, 4, per, BX), f32(count, cells), f32(count, BX)],
        in_specs=[pl.BlockSpec(memory_space=pltpu.HBM)] * 4,
        out_specs=[VMEM] * 4,
        scratch_shapes=[
            pltpu.VMEM(raw.shape, jnp.float32),
            pltpu.VMEM((1, count), jnp.int32),
            pltpu.VMEM((1, count), jnp.int32),
            pltpu.VMEM((count, cells), jnp.int32),
            pltpu.VMEM((n, per, BX), jnp.float32),
            pltpu.VMEM((n, 40, BX), jnp.float32),
            pltpu.VMEM((count, BX), jnp.int32),
            pltpu.SemaphoreType.DMA((PARTS + 3,)),
        ],
        compiler_params=params(12),
        name="first",
    )(raw, owner, covered, land)


def rows_kernel(ice, active, west, east, sides, north, south):
    count = active.shape[0]
    q = (lanes(count) % 8) < 4
    sides[...] = jnp.where(q, west[...], east[...])
    for out, lo in ((north, count - 2), (south, 0)):
        for y in range(2):
            cells = slice(y * BX, (y + 1) * BX)
            for ch in range(8):
                p = 2 * ch + y
                x = active[lo : lo + 2, cells] if ch == 7 else ice[ch, lo : lo + 2, cells]
                out[2 * p : 2 * p + 2, :] = x
        out[32:34, :] = sides[lo : lo + 2, :]


def ice_rows(ice, active, west, east):
    count = active.shape[0]
    return pl.pallas_call(
        rows_kernel,
        out_shape=[f32(count, BX), f32(34, BX), f32(34, BX)],
        in_specs=[VMEM] * 4,
        out_specs=[VMEM] * 3,
        compiler_params=params(8),
        name="ice_rows",
    )(ice, active, west, east)


def middle(rows):
    lane = lanes(rows)
    return (lane >= BX // 4) & (lane < 3 * BX // 4)


def side_plane(ends, ch, mid):
    odd = roll(ends, BX // 2 - (8 * (2 * ch + 1) + 4))
    return jnp.where(mid, odd, roll(ends, -(16 * ch + 4)))


def prep_kernel(count, height, ice, active, sides, below, above, begin, still, grid):
    mid, mid2 = middle(count), middle(2)
    pad = jnp.zeros((height - count - 4, BX), jnp.float32)
    for ch in range(8):
        for y in range(2):
            cells = slice(y * BX, (y + 1) * BX)
            grid[ch, y, 2 : 2 + count, :] = active[:, cells] if ch == 7 else ice[ch, :, cells]
            p = 2 * ch + y
            for lo, msg in ((0, below), (count + 2, above)):
                grid[ch, y, lo : lo + 2, :] = msg[2 * p : 2 * p + 2, :]
        grid[ch, 2, 2 : 2 + count, :] = side_plane(sides[...], ch, mid)
        for lo, msg in ((0, below), (count + 2, above)):
            grid[ch, 2, lo : lo + 2, :] = side_plane(msg[32:34, :], ch, mid2)
        for z in range(3):
            grid[ch, z, count + 4 :, :] = pad

    for r in range(height // 8):
        at = slice(8 * r, 8 * r + 8)
        for z in range(3):
            u, v, mass, conc, s1, s2, s12, act = [grid[ch, z, at, :] for ch in range(8)]
            for k, x in enumerate((u, v, 0.5 * s1, 0.5 * s2, s12)):
                begin[k, z, at, :] = x
            still[0, z, at, :] = mass * jnp.exp(CSTAR * (conc - 1.0)) * act * (1.0 / 6.0)
            still[1, z, at, :] = 2.0 * mass
            still[2, z, at, :] = CW * conc * act
            still[3, z, at, :] = act
            still[4, z, at, :] = conc


def prep(ice, active, sides, below, above):
    count = active.shape[0]
    height = (count + 4 + 7) // 8 * 8
    return pl.pallas_call(
        functools.partial(prep_kernel, count, height),
        out_shape=[f32(5, 3, height, BX)] * 2,
        in_specs=[VMEM] * 5,
        out_specs=[VMEM] * 2,
        scratch_shapes=[pltpu.VMEM((8, 3, height, BX), jnp.float32)],
        compiler_params=params(12),
        name="prep",
    )(ice, active, sides, below, above)


def east_of(even, odd, side, at127, at63):
    e, o, s = roll(even, -1), roll(odd, -1), roll(side, -1)
    wide = jnp.where(at127, e, jnp.where(at63, roll(odd, 63), s))
    return jnp.where(at127, s, e), jnp.where(at127, roll(side, 63), o), wide


def west_of(even, odd, side, at0, at64):
    e, o, s = roll(even, 1), roll(odd, 1), roll(side, 1)
    wide = jnp.where(at0, e, jnp.where(at64, roll(odd, 65), s))
    return jnp.where(at0, s, e), jnp.where(at0, roll(side, -63), o), wide


def ice_kernel(n, per, count, ids, recv, begin, still, back, moved,
               spot, hw, he, speed, state, forced, out8):
    tiles = (count + 4 + 7) // 8
    height = tiles * 8
    blank = jnp.zeros((8, BX), jnp.float32)
    for k in (0, 8):
        spot[k : k + 8, :] = blank
    for k in range((count + 3) * STEP, height * STEP, 8):
        spot[k : k + 8, :] = blank
    for k in (0, height - 8):
        hw[k : k + 8, :] = blank
        he[k : k + 8, :] = blank

    def place(o, acc):
        for j in range(per):
            b = (ids[o, j] + 2) * STEP
            spot[pl.ds(b, 12), :] = recv[o, 12 * j : 12 * j + 12, :]
            row = recv[o, 12 * per + j : 12 * per + j + 1, :]
            hw[pl.ds(ids[o, per + j] + 2, 1), :] = row
            he[pl.ds(ids[o, 2 * per + j] + 2, 1), :] = row
        return acc + recv[o, 13 * per : 13 * per + 40, :]

    rim = lax.fori_loop(0, n, place, jnp.zeros((40, BX), jnp.float32))
    up, down = (count + 2) * STEP, STEP
    spot[up : up + 12, :] = rim[0:12]
    spot[down : down + 12, :] = rim[18:30]
    for ch in range(6):
        k = up + STEP + 2 * ch
        spot[k : k + 1, :] = rim[12 + ch : 13 + ch]
        k = 2 * ch + 1
        spot[k : k + 1, :] = rim[30 + ch : 31 + ch]
    for ref in (hw, he):
        ref[count + 2 : count + 4, :] = rim[36:38]
        ref[1:2, :] = rim[38:39]
        ref[0:1, :] = rim[39:40]

    q, mid = (lanes(8) % 8) < 4, middle(8)
    for r in range(tiles):
        at = slice(8 * r, 8 * r + 8)
        to = slice(FRONT + 8 * r, FRONT + 8 * r + 8)
        ends = jnp.where(q, hw[at, :], he[at, :])
        for z in range(3):
            if z < 2:
                f = [spot[pl.ds(8 * r * STEP + 2 * ch + z, 8, stride=STEP), :] for ch in range(6)]
            else:
                f = [side_plane(ends, ch, mid) for ch in range(6)]
            for k in range(2):
                speed[k, z, to, :] = begin[k, z, at, :]
            for k in range(3):
                state[k, z, to, :] = begin[2 + k, z, at, :]
            mass, act, conc = [still[k, z, at, :] for k in (1, 3, 4)]
            mass = 0.5 * mass
            forced[0, z, at, :] = act * (conc * f[0] - mass * f[4])
            forced[1, z, at, :] = act * (conc * f[1] - mass * f[5])
            forced[2, z, at, :] = f[2]
            forced[3, z, at, :] = f[3]

    tail = FRONT + height
    for z in range(3):
        for k in range(2):
            speed[k, z, tail : tail + 8, :] = blank
        for k in range(3):
            state[k, z, 0:8, :] = blank

    lane = lanes(8)
    ends_at = [lane == k for k in (BX - 1, BX // 2 - 1, 0, BX // 2)]
    at127, at63, at0, at64 = ends_at

    def rows_of(r):
        row = 8 * r
        return pl.ds(row, 8), pl.ds(row + FRONT, 8), pl.ds(row + FRONT + 1, 8), pl.ds(row + FRONT - 1, 8)

    def stresses(r):
        at, to, up1, _ = rows_of(r)
        u = [speed[0, z, to, :] for z in range(3)]
        v = [speed[1, z, to, :] for z in range(3)]

        def north(k, x):
            return x[1], speed[k, 0, up1, :], roll(jnp.where(mid, x[2], speed[k, 2, up1, :]), BX // 2)

        un, vn = north(0, u), north(1, v)
        ue = east_of(*u, at127, at63)
        ve = east_of(*v, at127, at63)
        for z in range(3):
            sxx = ue[z] - u[z]
            syy = vn[z] - v[z]
            shear = (un[z] - u[z]) + (ve[z] - v[z])
            div, ten = sxx + syy, sxx - syy
            twice = div + div
            inv = lax.rsqrt(twice * twice + (ten * ten + shear * shear) + 1.0)
            hard = still[0, z, at, :]
            kr = hard * inv
            half = 0.5 * kr
            state[0, z, to, :] = (state[0, z, to, :] * (2.0 / 3.0) - hard) + kr * twice
            state[1, z, to, :] = state[1, z, to, :] * (2.0 / 3.0) + half * ten
            state[2, z, to, :] = state[2, z, to, :] * (2.0 / 3.0) + half * shear

    def speeds(r):
        at, to, _, down1 = rows_of(r)
        s1, s2, s12 = [[state[k, z, to, :] for z in range(3)] for k in range(3)]
        a = [x + y for x, y in zip(s1, s2)]
        c = [x - y for x, y in zip(s1, s2)]
        aw = west_of(*a, at0, at64)
        sw = west_of(*s12, at0, at64)

        def south(x, lower):
            return lower(1), x[0], roll(jnp.where(mid, lower(2), x[2]), BX // 2)

        ss = south(s12, lambda z: state[2, z, down1, :])
        cs = south(c, lambda z: state[0, z, down1, :] - state[1, z, down1, :])
        for z in range(3):
            u, v = speed[0, z, to, :], speed[1, z, to, :]
            fx = (a[z] - aw[z]) + (s12[z] - ss[z])
            fy = (s12[z] - sw[z]) + (c[z] - cs[z])
            m2, base = still[1, z, at, :], still[2, z, at, :]
            cx, cy = forced[2, z, at, :], forced[3, z, at, :]
            dx, dy = cx - u, cy - v
            y2 = dx * dx + dy * dy + DRAG_FLOOR
            drag = base * (y2 * lax.rsqrt(y2))
            part = still[3, z, at, :] * (1.0 / (jnp.maximum(m2, 1.0) + drag))
            mc = (0.5 * CORIO) * m2
            speed[0, z, to, :] = part * (m2 * u + fx + forced[0, z, at, :] + drag * cx + mc * v)
            speed[1, z, to, :] = part * (m2 * v + fy + forced[1, z, at, :] + drag * cy - mc * u)

    def subcycle(_, carry):
        for r in range(tiles):
            stresses(r)
        for r in range(tiles):
            speeds(r)
        return carry

    lax.fori_loop(0, NSUB, subcycle, 0)

    for r in range(tiles):
        at = slice(8 * r, 8 * r + 8)
        to = slice(FRONT + 8 * r, FRONT + 8 * r + 8)
        for y in range(2):
            base = still[2, y, at, :]
            dx = speed[0, y, to, :] - forced[2, y, at, :]
            dy = speed[1, y, to, :] - forced[3, y, at, :]
            y2 = dx * dx + dy * dy + DRAG_FLOOR
            factor = base * (y2 * lax.rsqrt(y2))
            for k, x in enumerate((factor * dx, factor * dy, base * (1.0 / CW))):
                out8[pl.ds(8 * r * REPLY + 2 * k + y, 8, stride=REPLY), :] = x
    for y in range(2):
        for k in range(2):
            moved[k, :, y * BX : (y + 1) * BX] = speed[k, y, FRONT + 2 : FRONT + 2 + count, :]

    def answer(o, _):
        for j in range(per):
            b = (ids[o, j] + 2) * REPLY
            back[o, 6 * j : 6 * j + 6, :] = out8[pl.ds(b, 6), :]
        return 0

    lax.fori_loop(0, n, answer, 0)


def ice_step(ids, recv, begin, still):
    n, per = ids.shape[0], ids.shape[1] // 3
    count = n * per
    height = (count + 4 + 7) // 8 * 8
    tall = height + 2 * FRONT
    scratch = [
        (height * STEP + 8, BX), (height, BX), (height, BX),
        (2, 3, tall, BX), (3, 3, tall, BX), (4, 3, height, BX), (height * REPLY + 8, BX),
    ]
    return pl.pallas_call(
        functools.partial(ice_kernel, n, per, count),
        out_shape=[f32(n, 6 * per, BX), f32(2, count, 2 * BX)],
        in_specs=[SMEM] + [VMEM] * 3,
        out_specs=[VMEM] * 2,
        scratch_shapes=[pltpu.VMEM(s, jnp.float32) for s in scratch],
        compiler_params=params(12),
        name="ice_step",
    )(ids, recv, begin, still)


def final_kernel(n, per, got, opened, moved, out):
    is_ocean = lax.axis_index("comp") == 0

    @pl.when(is_ocean)
    def _():
        def tile(t, _):
            for y in range(2):
                cells = slice(y * BX, (y + 1) * BX)
                gx, gy, gc = [got[t, pl.ds(2 * k + y, per, stride=6), :] for k in range(3)]
                out[0, t, :, cells] = gx + (1.0 - gc) * opened[t, 2 * y]
                out[1, t, :, cells] = gy + (1.0 - gc) * opened[t, 2 * y + 1]
            return 0

        lax.fori_loop(0, n, tile, 0)

    @pl.when(jnp.logical_not(is_ocean))
    def _():
        out[...] = moved[...]


def final(got, opened, moved):
    n, _, per, _ = opened.shape
    return pl.pallas_call(
        functools.partial(final_kernel, n, per),
        out_shape=f32(2, n, per, 2 * BX),
        in_specs=[VMEM] * 3,
        out_specs=VMEM,
        compiler_params=params(8),
        name="final",
    )(got, opened, moved)


def per_device(fields, block_owner, ice_covered, land_mask):
    nlat, nlon = lax.axis_size("lat"), lax.axis_size("lon")
    n = nlat * nlon
    count = block_owner.shape[0]
    per = count // n
    side = lax.axis_index("comp")
    fields = fields[0]
    local = (block_owner % count).reshape(nlat, nlon, per)
    ids = jnp.concatenate([local, jnp.roll(local, 1, 1), jnp.roll(local, -1, 1)], 2).reshape(n, 3 * per)
    split = fields.reshape(7, n, per, 2 * BX)
    pay, opened, active, ends = first(
        split, block_owner.reshape(1, count), ice_covered.reshape(1, count), land_mask, nlat, nlon
    )
    pay = lax.ppermute(pay, "comp", [(0, 1), (1, 0)])
    def everyone(x):
        return lax.all_to_all(x, ("lat", "lon"), split_axis=0, concat_axis=0, tiled=True)

    def ice_side(pay, ids, active, ends):
        recv = everyone(pay)
        ring = [(i, (i + 1) % nlon) for i in range(nlon)]
        west = lax.ppermute(ends, "lon", ring)
        east = lax.ppermute(ends, "lon", [(j, i) for i, j in ring])
        sides, north, south = ice_rows(fields, active, west, east)
        line = [(i, i + 1) for i in range(nlat - 1)]
        below = lax.ppermute(north, "lat", line)
        above = lax.ppermute(south, "lat", [(j, i) for i, j in line])
        return recv, ids, sides, below, above

    def ocean_side(pay, ids, active, ends):
        row = ends[:34]
        return jnp.zeros(pay.shape, jnp.float32), everyone(ids), ends, row, row

    recv, owner, sides, below, above = lax.cond(side == 1, ice_side, ocean_side, pay, ids, active, ends)
    swap = lax.ppermute(owner, "comp", [(0, 1), (1, 0)])
    begin, still = prep(fields, active, sides, below, above)
    back, moved = ice_step(swap, recv, begin, still)
    back = lax.cond(side == 1, everyone, lambda x: x, back)
    got = lax.ppermute(back, "comp", [(0, 1), (1, 0)])
    out = final(got, opened, moved.reshape(2, n, per, 2 * BX))
    return out.reshape(1, 2, count, 2 * BX)


def solution(mesh):
    placed = (
        P("comp", None, ("lat", "lon"), None),
        P(("lat", "lon")),
        P(("lat", "lon")),
        P(("lat", "lon"), None),
    )
    return jax.shard_map(
        per_device,
        mesh=mesh,
        in_specs=placed,
        out_specs=P("comp", None, ("lat", "lon"), None),
        check_vma=False,
    )
```

```python
import functools

import jax
import jax.numpy as jnp
from jax import lax
from jax.experimental import pallas as pl
from jax.experimental.pallas import tpu as pltpu
from jax.sharding import PartitionSpec as P

BX = 128
NSUB = 4
FRONT = 8
STEP = 13
REPLY = 7
PARTS = 4

CD_ICE = 0.1
CW = 1.5
CSTAR = 2.0
CORIO = 0.3
DRAG_FLOOR = 0.1

VMEM = pl.BlockSpec(memory_space=pltpu.VMEM)
SMEM = pl.BlockSpec(memory_space=pltpu.SMEM)


def params(mib):
    return pltpu.CompilerParams(vmem_limit_bytes=mib * 1024 * 1024)


def f32(*shape):
    return jax.ShapeDtypeStruct(shape, jnp.float32)


def lanes(rows):
    return lax.broadcasted_iota(jnp.int32, (rows, BX), 1)


def roll(x, by):
    return pltpu.roll(x, by % BX, 1)


def at_end(q, west, east):
    return jnp.where(q, west, east)


def column(row):
    parts = []
    for lo in range(0, row.shape[1], BX):
        diag = lax.broadcasted_iota(jnp.int32, (BX, BX), 0) == lanes(BX)
        parts.append(jnp.sum(jnp.where(diag, row[:, lo : lo + BX].astype(jnp.float32), 0.0), axis=1, keepdims=True))
    return jnp.concatenate(parts, 0) if len(parts) > 1 else parts[0]


def steps(lo, hi, body):
    if hi - lo <= 32:
        for k in range(lo, hi):
            body(k, 0)
    else:
        lax.fori_loop(lo, hi, body, 0)


def pack_body(nlat, nlon, per, count, raw, owner, pay, opened, edge, rim, parts, field):
    n = nlat * nlon
    lane = lanes(per)
    group = lane // 8
    slot = lax.broadcasted_iota(jnp.int32, (per, BX), 0)
    lat_base = 13 * per

    def tile(t, _):
        def half(ch, y):
            return raw[ch, t, :, y * BX : (y + 1) * BX]

        planes = [None] * 12
        for y in range(2):
            wx, wy, rho = half(0, y), half(1, y), half(6, y)
            scale = rho * CD_ICE * jnp.sqrt(wx * wx + wy * wy + 1.0)
            planes[y] = scale * wx
            planes[2 + y] = scale * wy
            for ch in range(2, 6):
                planes[2 * ch + y] = half(ch, y)
            rx, ry = wx - planes[4 + y], wy - planes[6 + y]
            speed = jnp.sqrt(rx * rx + ry * ry + 1.0)
            rate = rho * (0.1 + 0.05 * speed) * speed
            opened[t, 2 * y] = rate * rx
            opened[t, 2 * y + 1] = rate * ry
        ends = jnp.zeros((per, BX), jnp.float32)
        for p in range(12):
            pay[t, pl.ds(p, per, stride=12), :] = planes[p]
            ends = jnp.where(group == p, roll(planes[p], 8 * p + 4), ends)
        edge[t] = ends
        ids = jnp.zeros((per, BX), jnp.int32)
        for j in range(per):
            ids = jnp.where(slot == j, owner[0, t * per + j] - t * count, ids)

        def pick(block, value):
            return jnp.sum(jnp.where(ids == block, value, 0.0), axis=0, keepdims=True)

        rows = [pick(0, x) for x in planes] + [pick(1, x) for x in planes[0::2]]
        rows += [pick(count - 1, x) for x in planes]
        rows += [pick(count - 2, x) for x in planes[1::2]]
        rows += [pick(b, ends) for b in (0, 1, count - 1, count - 2)]
        for k, row in enumerate(rows):
            rim[t, k : k + 1, :] = row
        return 0

    for c in range(parts):
        field(c).wait()
        steps(c * (n // parts), (c + 1) * (n // parts), tile)

    def dest(d, _):
        i, j = d // nlon, d % nlon
        jw, je = (j + nlon - 1) % nlon, (j + 1) % nlon
        q8 = (lane % 8) < 4
        pay[d, 12 * per : 13 * per, :] = at_end(q8, edge[i * nlon + jw], edge[i * nlon + je])
        for ii, ok, lo, c in (
            (jnp.minimum(i + 1, nlat - 1), i + 1 < nlat, 0, 36),
            (jnp.maximum(i - 1, 0), i > 0, 18, 38),
        ):
            scale = jnp.where(ok, 1.0, 0.0)
            pay[d, lat_base + lo : lat_base + lo + 18, :] = rim[ii * nlon + j, lo : lo + 18, :] * scale
            q2 = (lanes(2) % 8) < 4
            corner = at_end(q2, rim[ii * nlon + jw, c : c + 2, :], rim[ii * nlon + je, c : c + 2, :])
            pay[d, lat_base + c : lat_base + c + 2, :] = corner * scale
        return 0

    steps(0, n, dest)


def ends_kernel(nlat, nlon, per, ice, covered, land, owner, active, ends, ids):
    def tile(t, _):
        i, j = t // nlon, t % nlon
        near = [t, i * nlon + (j + nlon - 1) % nlon, i * nlon + (j + 1) % nlon]
        for k, other in enumerate(near):
            for slot in range(per):
                ids[t, k * per + slot] = owner[0, other * per + slot] - other * (nlat * nlon * per)
        return 0

    steps(0, nlat * nlon, tile)

    count = covered.shape[1]
    lane = lanes(count)
    group = lane // 8
    total = jnp.zeros((count, BX), jnp.float32)
    cover = column(covered[...])
    for y in range(2):
        cells = slice(y * BX, (y + 1) * BX)
        act = cover * (1 - land[:, cells]).astype(jnp.float32)
        active[:, cells] = act
        for ch in range(8):
            x = act if ch == 7 else ice[ch, :, cells]
            p = 2 * ch + y
            total = jnp.where(group == p, roll(x, 8 * p + 4), total)
    ends[...] = total


def pack_kernel(nlat, nlon, per, raw_in, owner, pay, opened, raw, edge, rim, sems):
    n = nlat * nlon
    parts = PARTS if n % PARTS == 0 else 1
    step = n // parts

    def field(c):
        at = pl.ds(c * step, step)
        return pltpu.make_async_copy(raw_in.at[:, at], raw.at[:, at], sems.at[c])

    @pl.when(lax.axis_index("comp") == 0)
    def _():
        for c in range(parts):
            field(c).start()
        pack_body(nlat, nlon, per, n * per, raw, owner, pay, opened, edge, rim, parts, field)


def pack(raw, owner, nlat, nlon):
    _, n, per, _ = raw.shape
    return pl.pallas_call(
        functools.partial(pack_kernel, nlat, nlon, per),
        out_shape=[f32(n, 13 * per + 40, BX), f32(n, 4, per, BX)],
        in_specs=[pl.BlockSpec(memory_space=pltpu.HBM), SMEM],
        out_specs=[VMEM] * 2,
        scratch_shapes=[
            pltpu.VMEM(raw.shape, jnp.float32),
            pltpu.VMEM((n, per, BX), jnp.float32),
            pltpu.VMEM((n, 40, BX), jnp.float32),
            pltpu.SemaphoreType.DMA((PARTS,)),
        ],
        compiler_params=params(12),
        name="pack",
    )(raw, owner)


def ice_ends(ice, covered, land, owner, nlat, nlon):
    count = land.shape[0]
    n = nlat * nlon
    per = count // n
    return pl.pallas_call(
        functools.partial(ends_kernel, nlat, nlon, per),
        out_shape=[f32(count, 2 * BX), f32(count, BX), jax.ShapeDtypeStruct((n, 3 * per), jnp.int32)],
        in_specs=[VMEM] * 3 + [SMEM],
        out_specs=[VMEM] * 2 + [SMEM],
        compiler_params=params(8),
        name="ice_ends",
    )(ice, covered, land, owner)


def rows_kernel(ice, active, west, east, sides, north, south):
    count = active.shape[0]
    q = (lanes(count) % 8) < 4
    sides[...] = jnp.where(q, west[...], east[...])
    for out, lo in ((north, count - 2), (south, 0)):
        for y in range(2):
            cells = slice(y * BX, (y + 1) * BX)
            for ch in range(8):
                p = 2 * ch + y
                x = active[lo : lo + 2, cells] if ch == 7 else ice[ch, lo : lo + 2, cells]
                out[2 * p : 2 * p + 2, :] = x
        out[32:34, :] = sides[lo : lo + 2, :]


def ice_rows(ice, active, west, east):
    count = active.shape[0]
    return pl.pallas_call(
        rows_kernel,
        out_shape=[f32(count, BX), f32(34, BX), f32(34, BX)],
        in_specs=[VMEM] * 4,
        out_specs=[VMEM] * 3,
        compiler_params=params(8),
        name="ice_rows",
    )(ice, active, west, east)


def middle(rows):
    lane = lanes(rows)
    return (lane >= BX // 4) & (lane < 3 * BX // 4)


def side_plane(ends, ch, mid):
    odd = roll(ends, BX // 2 - (8 * (2 * ch + 1) + 4))
    return jnp.where(mid, odd, roll(ends, -(16 * ch + 4)))


def prep_kernel(count, height, ice, active, sides, below_in, above_in, recv_in, begin, still, recv,
                grid, below, above, sems):
    copies = [
        pltpu.make_async_copy(x, y, sems.at[k])
        for k, (x, y) in enumerate(((below_in, below), (above_in, above), (recv_in, recv)))
    ]
    for copy in copies:
        copy.start()
    mid, mid2 = middle(count), middle(2)
    pad = jnp.zeros((height - count - 4, BX), jnp.float32)
    for ch in range(8):
        for y in range(2):
            cells = slice(y * BX, (y + 1) * BX)
            grid[ch, y, 2 : 2 + count, :] = active[:, cells] if ch == 7 else ice[ch, :, cells]
        grid[ch, 2, 2 : 2 + count, :] = side_plane(sides[...], ch, mid)
        for z in range(3):
            grid[ch, z, count + 4 :, :] = pad

    def convert(r):
        at = slice(8 * r, 8 * r + 8)
        for z in range(3):
            u, v, mass, conc, s1, s2, s12, act = [grid[ch, z, at, :] for ch in range(8)]
            for k, x in enumerate((u, v, 0.5 * s1, 0.5 * s2, s12)):
                begin[k, z, at, :] = x
            still[0, z, at, :] = mass * jnp.exp(CSTAR * (conc - 1.0)) * act * (1.0 / 6.0)
            still[1, z, at, :] = 2.0 * mass
            still[2, z, at, :] = CW * conc * act
            still[3, z, at, :] = act
            still[4, z, at, :] = conc

    outer = [0] + list(range((count + 2) // 8, height // 8))
    for r in range(height // 8):
        if r not in outer:
            convert(r)
    copies[0].wait()
    copies[1].wait()
    for lo, msg in ((0, below), (count + 2, above)):
        for ch in range(8):
            for y in range(2):
                p = 2 * ch + y
                grid[ch, y, lo : lo + 2, :] = msg[2 * p : 2 * p + 2, :]
            grid[ch, 2, lo : lo + 2, :] = side_plane(msg[32:34, :], ch, mid2)
    for r in outer:
        convert(r)
    copies[2].wait()


def prep(ice, active, sides, below, above, recv):
    count = active.shape[0]
    height = (count + 4 + 7) // 8 * 8
    return pl.pallas_call(
        functools.partial(prep_kernel, count, height),
        out_shape=[f32(5, 3, height, BX)] * 2 + [f32(*recv.shape)],
        in_specs=[VMEM] * 3 + [pl.BlockSpec(memory_space=pl.ANY)] * 3,
        out_specs=[VMEM] * 3,
        scratch_shapes=[
            pltpu.VMEM((8, 3, height, BX), jnp.float32),
            pltpu.VMEM(below.shape, jnp.float32),
            pltpu.VMEM(above.shape, jnp.float32),
            pltpu.SemaphoreType.DMA((3,)),
        ],
        compiler_params=params(12),
        name="prep",
    )(ice, active, sides, below, above, recv)


def east_of(even, odd, side, at127, at63):
    e, o, s = roll(even, -1), roll(odd, -1), roll(side, -1)
    wide = jnp.where(at127, e, jnp.where(at63, roll(odd, 63), s))
    return jnp.where(at127, s, e), jnp.where(at127, roll(side, 63), o), wide


def west_of(even, odd, side, at0, at64):
    e, o, s = roll(even, 1), roll(odd, 1), roll(side, 1)
    wide = jnp.where(at0, e, jnp.where(at64, roll(odd, 65), s))
    return jnp.where(at0, s, e), jnp.where(at0, roll(side, -63), o), wide


def ice_kernel(n, per, count, ids, recv, begin, still, back, moved,
               spot, hw, he, speed, state, forced, out8):
    tiles = (count + 4 + 7) // 8
    height = tiles * 8
    blank = jnp.zeros((8, BX), jnp.float32)
    for k in (0, 8):
        spot[k : k + 8, :] = blank
    for k in range((count + 3) * STEP, height * STEP, 8):
        spot[k : k + 8, :] = blank
    for k in (0, height - 8):
        hw[k : k + 8, :] = blank
        he[k : k + 8, :] = blank

    def place(o, acc):
        for j in range(per):
            b = (ids[o, j] + 2) * STEP
            spot[pl.ds(b, 12), :] = recv[o, 12 * j : 12 * j + 12, :]
            row = recv[o, 12 * per + j : 12 * per + j + 1, :]
            hw[pl.ds(ids[o, per + j] + 2, 1), :] = row
            he[pl.ds(ids[o, 2 * per + j] + 2, 1), :] = row
        return acc + recv[o, 13 * per : 13 * per + 40, :]

    rim = lax.fori_loop(0, n, place, jnp.zeros((40, BX), jnp.float32))
    up, down = (count + 2) * STEP, STEP
    spot[up : up + 12, :] = rim[0:12]
    spot[down : down + 12, :] = rim[18:30]
    for ch in range(6):
        k = up + STEP + 2 * ch
        spot[k : k + 1, :] = rim[12 + ch : 13 + ch]
        k = 2 * ch + 1
        spot[k : k + 1, :] = rim[30 + ch : 31 + ch]
    for ref in (hw, he):
        ref[count + 2 : count + 4, :] = rim[36:38]
        ref[1:2, :] = rim[38:39]
        ref[0:1, :] = rim[39:40]

    q, mid = (lanes(8) % 8) < 4, middle(8)
    for r in range(tiles):
        at = slice(8 * r, 8 * r + 8)
        to = slice(FRONT + 8 * r, FRONT + 8 * r + 8)
        ends = jnp.where(q, hw[at, :], he[at, :])
        for z in range(3):
            if z < 2:
                f = [spot[pl.ds(8 * r * STEP + 2 * ch + z, 8, stride=STEP), :] for ch in range(6)]
            else:
                f = [side_plane(ends, ch, mid) for ch in range(6)]
            for k in range(2):
                speed[k, z, to, :] = begin[k, z, at, :]
            for k in range(3):
                state[k, z, to, :] = begin[2 + k, z, at, :]
            mass, act, conc = [still[k, z, at, :] for k in (1, 3, 4)]
            mass = 0.5 * mass
            forced[0, z, at, :] = act * (conc * f[0] - mass * f[4])
            forced[1, z, at, :] = act * (conc * f[1] - mass * f[5])
            forced[2, z, at, :] = f[2]
            forced[3, z, at, :] = f[3]

    tail = FRONT + height
    for z in range(3):
        for k in range(2):
            speed[k, z, tail : tail + 8, :] = blank
        for k in range(3):
            state[k, z, 0:8, :] = blank

    lane = lanes(8)
    ends_at = [lane == k for k in (BX - 1, BX // 2 - 1, 0, BX // 2)]
    at127, at63, at0, at64 = ends_at

    def rows_of(r):
        row = 8 * r
        return pl.ds(row, 8), pl.ds(row + FRONT, 8), pl.ds(row + FRONT + 1, 8), pl.ds(row + FRONT - 1, 8)

    def stresses(r):
        at, to, up1, _ = rows_of(r)
        u = [speed[0, z, to, :] for z in range(3)]
        v = [speed[1, z, to, :] for z in range(3)]

        def north(k, x):
            return x[1], speed[k, 0, up1, :], roll(jnp.where(mid, x[2], speed[k, 2, up1, :]), BX // 2)

        un, vn = north(0, u), north(1, v)
        ue = east_of(*u, at127, at63)
        ve = east_of(*v, at127, at63)
        for z in range(3):
            sxx = ue[z] - u[z]
            syy = vn[z] - v[z]
            shear = (un[z] - u[z]) + (ve[z] - v[z])
            div, ten = sxx + syy, sxx - syy
            twice = div + div
            inv = lax.rsqrt(twice * twice + (ten * ten + shear * shear) + 1.0)
            hard = still[0, z, at, :]
            kr = hard * inv
            half = 0.5 * kr
            state[0, z, to, :] = (state[0, z, to, :] * (2.0 / 3.0) - hard) + kr * twice
            state[1, z, to, :] = state[1, z, to, :] * (2.0 / 3.0) + half * ten
            state[2, z, to, :] = state[2, z, to, :] * (2.0 / 3.0) + half * shear

    def speeds(r):
        at, to, _, down1 = rows_of(r)
        s1, s2, s12 = [[state[k, z, to, :] for z in range(3)] for k in range(3)]
        a = [x + y for x, y in zip(s1, s2)]
        c = [x - y for x, y in zip(s1, s2)]
        aw = west_of(*a, at0, at64)
        sw = west_of(*s12, at0, at64)

        def south(x, lower):
            return lower(1), x[0], roll(jnp.where(mid, lower(2), x[2]), BX // 2)

        ss = south(s12, lambda z: state[2, z, down1, :])
        cs = south(c, lambda z: state[0, z, down1, :] - state[1, z, down1, :])
        for z in range(3):
            u, v = speed[0, z, to, :], speed[1, z, to, :]
            fx = (a[z] - aw[z]) + (s12[z] - ss[z])
            fy = (s12[z] - sw[z]) + (c[z] - cs[z])
            m2, base = still[1, z, at, :], still[2, z, at, :]
            cx, cy = forced[2, z, at, :], forced[3, z, at, :]
            dx, dy = cx - u, cy - v
            y2 = dx * dx + dy * dy + DRAG_FLOOR
            drag = base * (y2 * lax.rsqrt(y2))
            part = still[3, z, at, :] * (1.0 / (jnp.maximum(m2, 1.0) + drag))
            mc = (0.5 * CORIO) * m2
            speed[0, z, to, :] = part * (m2 * u + fx + forced[0, z, at, :] + drag * cx + mc * v)
            speed[1, z, to, :] = part * (m2 * v + fy + forced[1, z, at, :] + drag * cy - mc * u)

    def subcycle(_, carry):
        for r in range(tiles):
            stresses(r)
        for r in range(tiles):
            speeds(r)
        return carry

    lax.fori_loop(0, NSUB, subcycle, 0)

    for r in range(tiles):
        at = slice(8 * r, 8 * r + 8)
        to = slice(FRONT + 8 * r, FRONT + 8 * r + 8)
        for y in range(2):
            base = still[2, y, at, :]
            dx = speed[0, y, to, :] - forced[2, y, at, :]
            dy = speed[1, y, to, :] - forced[3, y, at, :]
            y2 = dx * dx + dy * dy + DRAG_FLOOR
            factor = base * (y2 * lax.rsqrt(y2))
            for k, x in enumerate((factor * dx, factor * dy, base * (1.0 / CW))):
                out8[pl.ds(8 * r * REPLY + 2 * k + y, 8, stride=REPLY), :] = x
    for y in range(2):
        for k in range(2):
            moved[k, :, y * BX : (y + 1) * BX] = speed[k, y, FRONT + 2 : FRONT + 2 + count, :]

    def answer(o, _):
        for j in range(per):
            b = (ids[o, j] + 2) * REPLY
            back[o, 6 * j : 6 * j + 6, :] = out8[pl.ds(b, 6), :]
        return 0

    lax.fori_loop(0, n, answer, 0)


def ice_step(ids, recv, begin, still):
    n, per = ids.shape[0], ids.shape[1] // 3
    count = n * per
    height = (count + 4 + 7) // 8 * 8
    tall = height + 2 * FRONT
    scratch = [
        (height * STEP + 8, BX), (height, BX), (height, BX),
        (2, 3, tall, BX), (3, 3, tall, BX), (4, 3, height, BX), (height * REPLY + 8, BX),
    ]
    return pl.pallas_call(
        functools.partial(ice_kernel, n, per, count),
        out_shape=[f32(n, 6 * per, BX), f32(2, count, 2 * BX)],
        in_specs=[SMEM] + [VMEM] * 3,
        out_specs=[VMEM] * 2,
        scratch_shapes=[pltpu.VMEM(s, jnp.float32) for s in scratch],
        compiler_params=params(12),
        name="ice_step",
    )(ids, recv, begin, still)


def final_kernel(n, per, got, opened, moved, out):
    is_ocean = lax.axis_index("comp") == 0

    @pl.when(is_ocean)
    def _():
        def tile(t, _):
            for y in range(2):
                cells = slice(y * BX, (y + 1) * BX)
                gx, gy, gc = [got[t, pl.ds(2 * k + y, per, stride=6), :] for k in range(3)]
                out[0, t, :, cells] = gx + (1.0 - gc) * opened[t, 2 * y]
                out[1, t, :, cells] = gy + (1.0 - gc) * opened[t, 2 * y + 1]
            return 0

        lax.fori_loop(0, n, tile, 0)

    @pl.when(jnp.logical_not(is_ocean))
    def _():
        out[...] = moved[...]


def final(got, opened, moved):
    n, _, per, _ = opened.shape
    return pl.pallas_call(
        functools.partial(final_kernel, n, per),
        out_shape=f32(2, n, per, 2 * BX),
        in_specs=[VMEM] * 3,
        out_specs=VMEM,
        compiler_params=params(8),
        name="final",
    )(got, opened, moved)


def per_device(fields, block_owner, ice_covered, land_mask):
    nlat, nlon = lax.axis_size("lat"), lax.axis_size("lon")
    n = nlat * nlon
    count = block_owner.shape[0]
    per = count // n
    side = lax.axis_index("comp")
    fields = fields[0]
    split = fields.reshape(7, n, per, 2 * BX)
    owner = block_owner.reshape(1, count)
    pay, opened = pack(split, owner, nlat, nlon)
    pay = lax.ppermute(pay, "comp", [(0, 1), (1, 0)])
    active, ends, ids = ice_ends(fields, ice_covered.reshape(1, count), land_mask, owner, nlat, nlon)

    def everyone(x):
        return lax.all_to_all(x, ("lat", "lon"), split_axis=0, concat_axis=0, tiled=True)

    def ice_side(pay, ids, active, ends):
        recv = everyone(pay)
        ring = [(i, (i + 1) % nlon) for i in range(nlon)]
        west = lax.ppermute(ends, "lon", ring)
        east = lax.ppermute(ends, "lon", [(j, i) for i, j in ring])
        sides, north, south = ice_rows(fields, active, west, east)
        line = [(i, i + 1) for i in range(nlat - 1)]
        below = lax.ppermute(north, "lat", line)
        above = lax.ppermute(south, "lat", [(j, i) for i, j in line])
        return recv, ids, sides, below, above

    def ocean_side(pay, ids, active, ends):
        row = ends[:34]
        return jnp.zeros(pay.shape, jnp.float32), everyone(ids), ends, row, row

    recv, owned, sides, below, above = lax.cond(side == 1, ice_side, ocean_side, pay, ids, active, ends)
    swap = lax.ppermute(owned, "comp", [(0, 1), (1, 0)])
    begin, still, recv = prep(fields, active, sides, below, above, recv)
    back, moved = ice_step(swap, recv, begin, still)
    back = lax.cond(side == 1, everyone, lambda x: x, back)
    got = lax.ppermute(back, "comp", [(0, 1), (1, 0)])
    out = final(got, opened, moved.reshape(2, n, per, 2 * BX))
    return out.reshape(1, 2, count, 2 * BX)


def solution(mesh):
    placed = (
        P("comp", None, ("lat", "lon"), None),
        P(("lat", "lon")),
        P(("lat", "lon")),
        P(("lat", "lon"), None),
    )
    return jax.shard_map(
        per_device,
        mesh=mesh,
        in_specs=placed,
        out_specs=P("comp", None, ("lat", "lon"), None),
        check_vma=False,
    )
```

```python
import functools

import jax
import jax.numpy as jnp
from jax import lax
from jax.experimental import pallas as pl
from jax.experimental.pallas import tpu as pltpu
from jax.sharding import PartitionSpec as P

BX = 128
NSUB = 4
FRONT = 8
STEP = 13
REPLY = 7
PARTS = 4

CD_ICE = 0.1
CW = 1.5
CSTAR = 2.0
CORIO = 0.3
DRAG_FLOOR = 0.1

VMEM = pl.BlockSpec(memory_space=pltpu.VMEM)
SMEM = pl.BlockSpec(memory_space=pltpu.SMEM)


def params(mib):
    return pltpu.CompilerParams(vmem_limit_bytes=mib * 1024 * 1024)


def f32(*shape):
    return jax.ShapeDtypeStruct(shape, jnp.float32)


def lanes(rows):
    return lax.broadcasted_iota(jnp.int32, (rows, BX), 1)


def roll(x, by):
    return pltpu.roll(x, by % BX, 1)


def at_end(q, west, east):
    return jnp.where(q, west, east)


def column(row):
    parts = []
    for lo in range(0, row.shape[1], BX):
        diag = lax.broadcasted_iota(jnp.int32, (BX, BX), 0) == lanes(BX)
        parts.append(jnp.sum(jnp.where(diag, row[:, lo : lo + BX].astype(jnp.float32), 0.0), axis=1, keepdims=True))
    return jnp.concatenate(parts, 0) if len(parts) > 1 else parts[0]


def steps(lo, hi, body):
    if hi - lo <= 32:
        for k in range(lo, hi):
            body(k, 0)
    else:
        lax.fori_loop(lo, hi, body, 0)


def pack_body(nlat, nlon, per, count, raw, owner, pay, opened, edge, rim, parts, field):
    n = nlat * nlon
    lane = lanes(per)
    group = lane // 8
    slot = lax.broadcasted_iota(jnp.int32, (per, BX), 0)
    lat_base = 13 * per

    def tile(t, _):
        def half(ch, y):
            return raw[ch, t, :, y * BX : (y + 1) * BX]

        planes = [None] * 12
        for y in range(2):
            wx, wy, rho = half(0, y), half(1, y), half(6, y)
            scale = rho * CD_ICE * jnp.sqrt(wx * wx + wy * wy + 1.0)
            planes[y] = scale * wx
            planes[2 + y] = scale * wy
            for ch in range(2, 6):
                planes[2 * ch + y] = half(ch, y)
            rx, ry = wx - planes[4 + y], wy - planes[6 + y]
            speed = jnp.sqrt(rx * rx + ry * ry + 1.0)
            rate = rho * (0.1 + 0.05 * speed) * speed
            opened[t, 2 * y] = rate * rx
            opened[t, 2 * y + 1] = rate * ry
        ends = jnp.zeros((per, BX), jnp.float32)
        for p in range(12):
            pay[t, pl.ds(p, per, stride=12), :] = planes[p]
            ends = jnp.where(group == p, roll(planes[p], 8 * p + 4), ends)
        edge[t] = ends
        ids = jnp.zeros((per, BX), jnp.int32)
        for j in range(per):
            ids = jnp.where(slot == j, owner[0, t * per + j] - t * count, ids)

        def pick(block, value):
            return jnp.sum(jnp.where(ids == block, value, 0.0), axis=0, keepdims=True)

        rows = [pick(0, x) for x in planes] + [pick(1, x) for x in planes[0::2]]
        rows += [pick(count - 1, x) for x in planes]
        rows += [pick(count - 2, x) for x in planes[1::2]]
        rows += [pick(b, ends) for b in (0, 1, count - 1, count - 2)]
        for k, row in enumerate(rows):
            rim[t, k : k + 1, :] = row
        return 0

    for c in range(parts):
        field(c).wait()
        steps(c * (n // parts), (c + 1) * (n // parts), tile)

    def dest(d, _):
        i, j = d // nlon, d % nlon
        jw, je = (j + nlon - 1) % nlon, (j + 1) % nlon
        q8 = (lane % 8) < 4
        pay[d, 12 * per : 13 * per, :] = at_end(q8, edge[i * nlon + jw], edge[i * nlon + je])
        for ii, ok, lo, c in (
            (jnp.minimum(i + 1, nlat - 1), i + 1 < nlat, 0, 36),
            (jnp.maximum(i - 1, 0), i > 0, 18, 38),
        ):
            scale = jnp.where(ok, 1.0, 0.0)
            pay[d, lat_base + lo : lat_base + lo + 18, :] = rim[ii * nlon + j, lo : lo + 18, :] * scale
            q2 = (lanes(2) % 8) < 4
            corner = at_end(q2, rim[ii * nlon + jw, c : c + 2, :], rim[ii * nlon + je, c : c + 2, :])
            pay[d, lat_base + c : lat_base + c + 2, :] = corner * scale
        return 0

    steps(0, n, dest)


def ends_kernel(ice, covered, land, active, ends):
    count = covered.shape[1]
    lane = lanes(count)
    group = lane // 8
    total = jnp.zeros((count, BX), jnp.float32)
    cover = column(covered[...])
    for y in range(2):
        cells = slice(y * BX, (y + 1) * BX)
        act = cover * (1 - land[:, cells]).astype(jnp.float32)
        active[:, cells] = act
        for ch in range(8):
            x = act if ch == 7 else ice[ch, :, cells]
            p = 2 * ch + y
            total = jnp.where(group == p, roll(x, 8 * p + 4), total)
    ends[...] = total


def pack_kernel(nlat, nlon, per, raw_in, owner, pay, opened, raw, edge, rim, sems):
    n = nlat * nlon
    parts = PARTS if n % PARTS == 0 else 1
    step = n // parts

    def field(c):
        at = pl.ds(c * step, step)
        return pltpu.make_async_copy(raw_in.at[:, at], raw.at[:, at], sems.at[c])

    @pl.when(lax.axis_index("comp") == 0)
    def _():
        for c in range(parts):
            field(c).start()
        pack_body(nlat, nlon, per, n * per, raw, owner, pay, opened, edge, rim, parts, field)


def pack(raw, owner, nlat, nlon):
    _, n, per, _ = raw.shape
    return pl.pallas_call(
        functools.partial(pack_kernel, nlat, nlon, per),
        out_shape=[f32(n, 13 * per + 40, BX), f32(n, 4, per, BX)],
        in_specs=[pl.BlockSpec(memory_space=pltpu.HBM), SMEM],
        out_specs=[VMEM] * 2,
        scratch_shapes=[
            pltpu.VMEM(raw.shape, jnp.float32),
            pltpu.VMEM((n, per, BX), jnp.float32),
            pltpu.VMEM((n, 40, BX), jnp.float32),
            pltpu.SemaphoreType.DMA((PARTS,)),
        ],
        compiler_params=params(12),
        name="pack",
    )(raw, owner)


def ice_ends(ice, covered, land):
    count = land.shape[0]
    return pl.pallas_call(
        ends_kernel,
        out_shape=[f32(count, 2 * BX), f32(count, BX)],
        in_specs=[VMEM] * 3,
        out_specs=[VMEM] * 2,
        compiler_params=params(8),
        name="ice_ends",
    )(ice, covered, land)


def table_kernel(nlat, nlon, per, owner, ids):
    def tile(t, _):
        i, j = t // nlon, t % nlon
        near = [t, i * nlon + (j + nlon - 1) % nlon, i * nlon + (j + 1) % nlon]
        for k, other in enumerate(near):
            for slot in range(per):
                ids[t, k * per + slot] = owner[0, other * per + slot] - other * (nlat * nlon * per)
        return 0

    steps(0, nlat * nlon, tile)


def table(owner, nlat, nlon):
    n = nlat * nlon
    per = owner.shape[1] // n
    return pl.pallas_call(
        functools.partial(table_kernel, nlat, nlon, per),
        out_shape=jax.ShapeDtypeStruct((n, 3 * per), jnp.int32),
        in_specs=[SMEM],
        out_specs=SMEM,
        compiler_params=params(4),
        name="table",
    )(owner)


def rows_kernel(ice, active, west, east, sides, north, south):
    count = active.shape[0]
    q = (lanes(count) % 8) < 4
    sides[...] = jnp.where(q, west[...], east[...])
    for out, lo in ((north, count - 2), (south, 0)):
        for y in range(2):
            cells = slice(y * BX, (y + 1) * BX)
            for ch in range(8):
                p = 2 * ch + y
                x = active[lo : lo + 2, cells] if ch == 7 else ice[ch, lo : lo + 2, cells]
                out[2 * p : 2 * p + 2, :] = x
        out[32:34, :] = sides[lo : lo + 2, :]


def ice_rows(ice, active, west, east):
    count = active.shape[0]
    return pl.pallas_call(
        rows_kernel,
        out_shape=[f32(count, BX), f32(34, BX), f32(34, BX)],
        in_specs=[VMEM] * 4,
        out_specs=[VMEM] * 3,
        compiler_params=params(8),
        name="ice_rows",
    )(ice, active, west, east)


def middle(rows):
    lane = lanes(rows)
    return (lane >= BX // 4) & (lane < 3 * BX // 4)


def side_plane(ends, ch, mid):
    odd = roll(ends, BX // 2 - (8 * (2 * ch + 1) + 4))
    return jnp.where(mid, odd, roll(ends, -(16 * ch + 4)))


def statics(mass, conc, act):
    return mass * jnp.exp(CSTAR * (conc - 1.0)) * act * (1.0 / 6.0), 2.0 * mass, CW * conc * act, act, conc


def prep_kernel(count, height, ice, active, sides, begin, still, grid):
    mid = middle(count)
    for ch in range(8):
        for y in range(2):
            cells = slice(y * BX, (y + 1) * BX)
            grid[ch, y, 2 : 2 + count, :] = active[:, cells] if ch == 7 else ice[ch, :, cells]
        grid[ch, 2, 2 : 2 + count, :] = side_plane(sides[...], ch, mid)
        for z in range(3):
            grid[ch, z, 0:2, :] = jnp.zeros((2, BX), jnp.float32)
            grid[ch, z, count + 2 :, :] = jnp.zeros((height - count - 2, BX), jnp.float32)

    for r in range(height // 8):
        at = slice(8 * r, 8 * r + 8)
        for z in range(3):
            u, v, mass, conc, s1, s2, s12, act = [grid[ch, z, at, :] for ch in range(8)]
            for k, x in enumerate((u, v, 0.5 * s1, 0.5 * s2, s12)):
                begin[k, z, at, :] = x
            for k, x in enumerate(statics(mass, conc, act)):
                still[k, z, at, :] = x


def prep(ice, active, sides):
    count = active.shape[0]
    height = (count + 4 + 7) // 8 * 8
    return pl.pallas_call(
        functools.partial(prep_kernel, count, height),
        out_shape=[f32(5, 3, height, BX)] * 2,
        in_specs=[VMEM] * 3,
        out_specs=[VMEM] * 2,
        scratch_shapes=[pltpu.VMEM((8, 3, height, BX), jnp.float32)],
        compiler_params=params(12),
        name="prep",
    )(ice, active, sides)


def fetch_kernel(*refs):
    k = len(refs) // 2
    copies = [pltpu.make_async_copy(refs[i], refs[k + i], refs[-1].at[i]) for i in range(k)]
    for copy in copies:
        copy.start()
    for copy in copies:
        copy.wait()


def fetch(*arrays):
    return pl.pallas_call(
        fetch_kernel,
        out_shape=[f32(*x.shape) for x in arrays],
        in_specs=[pl.BlockSpec(memory_space=pl.ANY)] * len(arrays),
        out_specs=[VMEM] * len(arrays),
        scratch_shapes=[pltpu.SemaphoreType.DMA((len(arrays),))],
        compiler_params=params(4),
        name="fetch",
    )(*arrays)


def east_of(even, odd, side, at127, at63):
    e, o, s = roll(even, -1), roll(odd, -1), roll(side, -1)
    wide = jnp.where(at127, e, jnp.where(at63, roll(odd, 63), s))
    return jnp.where(at127, s, e), jnp.where(at127, roll(side, 63), o), wide


def west_of(even, odd, side, at0, at64):
    e, o, s = roll(even, 1), roll(odd, 1), roll(side, 1)
    wide = jnp.where(at0, e, jnp.where(at64, roll(odd, 65), s))
    return jnp.where(at0, s, e), jnp.where(at0, roll(side, -63), o), wide


def ice_kernel(n, per, count, ids, recv, begin, fixed, below, above, back, moved,
               spot, hw, he, speed, state, forced, out8, still):
    tiles = (count + 4 + 7) // 8
    height = tiles * 8
    blank = jnp.zeros((8, BX), jnp.float32)
    for k in (0, 8):
        spot[k : k + 8, :] = blank
    for k in range((count + 3) * STEP, height * STEP, 8):
        spot[k : k + 8, :] = blank
    for k in (0, height - 8):
        hw[k : k + 8, :] = blank
        he[k : k + 8, :] = blank

    def place(o, acc):
        for j in range(per):
            b = (ids[o, j] + 2) * STEP
            spot[pl.ds(b, 12), :] = recv[o, 12 * j : 12 * j + 12, :]
            row = recv[o, 12 * per + j : 12 * per + j + 1, :]
            hw[pl.ds(ids[o, per + j] + 2, 1), :] = row
            he[pl.ds(ids[o, 2 * per + j] + 2, 1), :] = row
        return acc + recv[o, 13 * per : 13 * per + 40, :]

    rim = lax.fori_loop(0, n, place, jnp.zeros((40, BX), jnp.float32))
    up, down = (count + 2) * STEP, STEP
    spot[up : up + 12, :] = rim[0:12]
    spot[down : down + 12, :] = rim[18:30]
    for ch in range(6):
        k = up + STEP + 2 * ch
        spot[k : k + 1, :] = rim[12 + ch : 13 + ch]
        k = 2 * ch + 1
        spot[k : k + 1, :] = rim[30 + ch : 31 + ch]
    for ref in (hw, he):
        ref[count + 2 : count + 4, :] = rim[36:38]
        ref[1:2, :] = rim[38:39]
        ref[0:1, :] = rim[39:40]

    q, mid, mid2 = (lanes(8) % 8) < 4, middle(8), middle(2)
    for r in range(tiles):
        at = slice(8 * r, 8 * r + 8)
        to = slice(FRONT + 8 * r, FRONT + 8 * r + 8)
        for z in range(3):
            for k in range(2):
                speed[k, z, to, :] = begin[k, z, at, :]
            for k in range(3):
                state[k, z, to, :] = begin[2 + k, z, at, :]
            for k in range(5):
                still[k, z, at, :] = fixed[k, z, at, :]
    for lo, msg in ((0, below), (count + 2, above)):
        at, to = slice(lo, lo + 2), slice(FRONT + lo, FRONT + lo + 2)
        for z in range(3):
            if z < 2:
                raw = [msg[4 * ch + 2 * z : 4 * ch + 2 * z + 2, :] for ch in range(8)]
            else:
                raw = [side_plane(msg[32:34, :], ch, mid2) for ch in range(8)]
            u, v, mass, conc, s1, s2, s12, act = raw
            speed[0, z, to, :] = u
            speed[1, z, to, :] = v
            state[0, z, to, :] = 0.5 * s1
            state[1, z, to, :] = 0.5 * s2
            state[2, z, to, :] = s12
            for k, x in enumerate(statics(mass, conc, act)):
                still[k, z, at, :] = x

    for r in range(tiles):
        at = slice(8 * r, 8 * r + 8)
        ends = jnp.where(q, hw[at, :], he[at, :])
        for z in range(3):
            if z < 2:
                f = [spot[pl.ds(8 * r * STEP + 2 * ch + z, 8, stride=STEP), :] for ch in range(6)]
            else:
                f = [side_plane(ends, ch, mid) for ch in range(6)]
            mass, act, conc = [still[k, z, at, :] for k in (1, 3, 4)]
            mass = 0.5 * mass
            forced[0, z, at, :] = act * (conc * f[0] - mass * f[4])
            forced[1, z, at, :] = act * (conc * f[1] - mass * f[5])
            forced[2, z, at, :] = f[2]
            forced[3, z, at, :] = f[3]

    tail = FRONT + height
    for z in range(3):
        for k in range(2):
            speed[k, z, tail : tail + 8, :] = blank
        for k in range(3):
            state[k, z, 0:8, :] = blank

    lane = lanes(8)
    ends_at = [lane == k for k in (BX - 1, BX // 2 - 1, 0, BX // 2)]
    at127, at63, at0, at64 = ends_at

    def rows_of(r):
        row = 8 * r
        return pl.ds(row, 8), pl.ds(row + FRONT, 8), pl.ds(row + FRONT + 1, 8), pl.ds(row + FRONT - 1, 8)

    def stresses(r):
        at, to, up1, _ = rows_of(r)
        u = [speed[0, z, to, :] for z in range(3)]
        v = [speed[1, z, to, :] for z in range(3)]

        def north(k, x):
            return x[1], speed[k, 0, up1, :], roll(jnp.where(mid, x[2], speed[k, 2, up1, :]), BX // 2)

        un, vn = north(0, u), north(1, v)
        ue = east_of(*u, at127, at63)
        ve = east_of(*v, at127, at63)
        for z in range(3):
            sxx = ue[z] - u[z]
            syy = vn[z] - v[z]
            shear = (un[z] - u[z]) + (ve[z] - v[z])
            div, ten = sxx + syy, sxx - syy
            twice = div + div
            inv = lax.rsqrt(twice * twice + (ten * ten + shear * shear) + 1.0)
            hard = still[0, z, at, :]
            kr = hard * inv
            half = 0.5 * kr
            state[0, z, to, :] = (state[0, z, to, :] * (2.0 / 3.0) - hard) + kr * twice
            state[1, z, to, :] = state[1, z, to, :] * (2.0 / 3.0) + half * ten
            state[2, z, to, :] = state[2, z, to, :] * (2.0 / 3.0) + half * shear

    def speeds(r):
        at, to, _, down1 = rows_of(r)
        s1, s2, s12 = [[state[k, z, to, :] for z in range(3)] for k in range(3)]
        a = [x + y for x, y in zip(s1, s2)]
        c = [x - y for x, y in zip(s1, s2)]
        aw = west_of(*a, at0, at64)
        sw = west_of(*s12, at0, at64)

        def south(x, lower):
            return lower(1), x[0], roll(jnp.where(mid, lower(2), x[2]), BX // 2)

        ss = south(s12, lambda z: state[2, z, down1, :])
        cs = south(c, lambda z: state[0, z, down1, :] - state[1, z, down1, :])
        for z in range(3):
            u, v = speed[0, z, to, :], speed[1, z, to, :]
            fx = (a[z] - aw[z]) + (s12[z] - ss[z])
            fy = (s12[z] - sw[z]) + (c[z] - cs[z])
            m2, base = still[1, z, at, :], still[2, z, at, :]
            cx, cy = forced[2, z, at, :], forced[3, z, at, :]
            dx, dy = cx - u, cy - v
            y2 = dx * dx + dy * dy + DRAG_FLOOR
            drag = base * (y2 * lax.rsqrt(y2))
            part = still[3, z, at, :] * (1.0 / (jnp.maximum(m2, 1.0) + drag))
            mc = (0.5 * CORIO) * m2
            speed[0, z, to, :] = part * (m2 * u + fx + forced[0, z, at, :] + drag * cx + mc * v)
            speed[1, z, to, :] = part * (m2 * v + fy + forced[1, z, at, :] + drag * cy - mc * u)

    def subcycle(_, carry):
        for r in range(tiles):
            stresses(r)
        for r in range(tiles):
            speeds(r)
        return carry

    lax.fori_loop(0, NSUB, subcycle, 0)

    for r in range(tiles):
        at = slice(8 * r, 8 * r + 8)
        to = slice(FRONT + 8 * r, FRONT + 8 * r + 8)
        for y in range(2):
            base = still[2, y, at, :]
            dx = speed[0, y, to, :] - forced[2, y, at, :]
            dy = speed[1, y, to, :] - forced[3, y, at, :]
            y2 = dx * dx + dy * dy + DRAG_FLOOR
            factor = base * (y2 * lax.rsqrt(y2))
            for k, x in enumerate((factor * dx, factor * dy, base * (1.0 / CW))):
                out8[pl.ds(8 * r * REPLY + 2 * k + y, 8, stride=REPLY), :] = x
    for y in range(2):
        for k in range(2):
            moved[k, :, y * BX : (y + 1) * BX] = speed[k, y, FRONT + 2 : FRONT + 2 + count, :]

    def answer(o, _):
        for j in range(per):
            b = (ids[o, j] + 2) * REPLY
            back[o, 6 * j : 6 * j + 6, :] = out8[pl.ds(b, 6), :]
        return 0

    lax.fori_loop(0, n, answer, 0)


def ice_step(ids, recv, begin, fixed, below, above):
    n, per = ids.shape[0], ids.shape[1] // 3
    count = n * per
    height = (count + 4 + 7) // 8 * 8
    tall = height + 2 * FRONT
    scratch = [
        (height * STEP + 8, BX), (height, BX), (height, BX),
        (2, 3, tall, BX), (3, 3, tall, BX), (4, 3, height, BX), (height * REPLY + 8, BX), (5, 3, height, BX),
    ]
    return pl.pallas_call(
        functools.partial(ice_kernel, n, per, count),
        out_shape=[f32(n, 6 * per, BX), f32(2, count, 2 * BX)],
        in_specs=[SMEM] + [VMEM] * 5,
        out_specs=[VMEM] * 2,
        scratch_shapes=[pltpu.VMEM(s, jnp.float32) for s in scratch],
        compiler_params=params(16),
        name="ice_step",
    )(ids, recv, begin, fixed, below, above)


def final_kernel(n, per, got, opened, moved, out):
    is_ocean = lax.axis_index("comp") == 0

    @pl.when(is_ocean)
    def _():
        def tile(t, _):
            for y in range(2):
                cells = slice(y * BX, (y + 1) * BX)
                gx, gy, gc = [got[t, pl.ds(2 * k + y, per, stride=6), :] for k in range(3)]
                out[0, t, :, cells] = gx + (1.0 - gc) * opened[t, 2 * y]
                out[1, t, :, cells] = gy + (1.0 - gc) * opened[t, 2 * y + 1]
            return 0

        lax.fori_loop(0, n, tile, 0)

    @pl.when(jnp.logical_not(is_ocean))
    def _():
        out[...] = moved[...]


def final(got, opened, moved):
    n, _, per, _ = opened.shape
    return pl.pallas_call(
        functools.partial(final_kernel, n, per),
        out_shape=f32(2, n, per, 2 * BX),
        in_specs=[VMEM] * 3,
        out_specs=VMEM,
        compiler_params=params(8),
        name="final",
    )(got, opened, moved)


def per_device(fields, block_owner, ice_covered, land_mask):
    nlat, nlon = lax.axis_size("lat"), lax.axis_size("lon")
    n = nlat * nlon
    count = block_owner.shape[0]
    per = count // n
    side = lax.axis_index("comp")
    fields = fields[0]
    split = fields.reshape(7, n, per, 2 * BX)
    owner = block_owner.reshape(1, count)
    pay, opened = pack(split, owner, nlat, nlon)
    pay = lax.ppermute(pay, "comp", [(0, 1), (1, 0)])
    def everyone(x):
        return lax.all_to_all(x, ("lat", "lon"), split_axis=0, concat_axis=0, tiled=True)

    height = (count + 4 + 7) // 8 * 8

    def ice_side(pay, fields, covered, land, owner):
        recv = everyone(pay)
        active, ends = ice_ends(fields, covered, land)
        ring = [(i, (i + 1) % nlon) for i in range(nlon)]
        west = lax.ppermute(ends, "lon", ring)
        east = lax.ppermute(ends, "lon", [(j, i) for i, j in ring])
        sides, north, south = ice_rows(fields, active, west, east)
        line = [(i, i + 1) for i in range(nlat - 1)]
        below = lax.ppermute(north, "lat", line)
        above = lax.ppermute(south, "lat", [(j, i) for i, j in line])
        begin, fixed = prep(fields, active, sides)
        return recv, jnp.zeros((n, 3 * per), jnp.int32), below, above, begin, fixed

    def ocean_side(pay, fields, covered, land, owner):
        row = jnp.zeros((34, BX), jnp.float32)
        blank = jnp.zeros((5, 3, height, BX), jnp.float32)
        return jnp.zeros(pay.shape, jnp.float32), everyone(table(owner, nlat, nlon)), row, row, blank, blank

    recv, owned, below, above, begin, fixed = lax.cond(
        side == 1, ice_side, ocean_side, pay, fields, ice_covered.reshape(1, count), land_mask, owner
    )
    swap = lax.ppermute(owned, "comp", [(0, 1), (1, 0)])
    recv, below, above = fetch(recv, below, above)
    back, moved = ice_step(swap, recv, begin, fixed, below, above)
    back = lax.cond(side == 1, everyone, lambda x: x, back)
    got = lax.ppermute(back, "comp", [(0, 1), (1, 0)])
    out = final(got, opened, moved.reshape(2, n, per, 2 * BX))
    return out.reshape(1, 2, count, 2 * BX)


def solution(mesh):
    placed = (
        P("comp", None, ("lat", "lon"), None),
        P(("lat", "lon")),
        P(("lat", "lon")),
        P(("lat", "lon"), None),
    )
    return jax.shard_map(
        per_device,
        mesh=mesh,
        in_specs=placed,
        out_specs=P("comp", None, ("lat", "lon"), None),
        check_vma=False,
    )
```

```python
import functools

import jax
import jax.numpy as jnp
from jax import lax
from jax.experimental import pallas as pl
from jax.experimental.pallas import tpu as pltpu
from jax.sharding import PartitionSpec as P

BX = 128
NSUB = 4
FRONT = 8
STEP = 13
REPLY = 7

CD_ICE = 0.1
CW = 1.5
CSTAR = 2.0
CORIO = 0.3
DRAG_FLOOR = 0.1

VMEM = pl.BlockSpec(memory_space=pltpu.VMEM)
SMEM = pl.BlockSpec(memory_space=pltpu.SMEM)


def params(mib):
    return pltpu.CompilerParams(vmem_limit_bytes=mib * 1024 * 1024)


def f32(*shape):
    return jax.ShapeDtypeStruct(shape, jnp.float32)


def lanes(rows):
    return lax.broadcasted_iota(jnp.int32, (rows, BX), 1)


def roll(x, by):
    return pltpu.roll(x, by % BX, 1)


def at_end(q, west, east):
    return jnp.where(q, west, east)


def column(row):
    parts = []
    for lo in range(0, row.shape[1], BX):
        diag = lax.broadcasted_iota(jnp.int32, (BX, BX), 0) == lanes(BX)
        parts.append(jnp.sum(jnp.where(diag, row[:, lo : lo + BX].astype(jnp.float32), 0.0), axis=1, keepdims=True))
    return jnp.concatenate(parts, 0) if len(parts) > 1 else parts[0]


def steps(lo, hi, body):
    if hi - lo <= 32:
        for k in range(lo, hi):
            body(k, 0)
    else:
        lax.fori_loop(lo, hi, body, 0)


def pack_body(nlat, nlon, per, count, raw, owner, pay, edge, rim):
    n = nlat * nlon
    lane = lanes(per)
    group = lane // 8
    slot = lax.broadcasted_iota(jnp.int32, (per, BX), 0)
    lat_base = 13 * per

    def tile(t, _):
        def half(ch, y):
            return raw[ch, t, :, y * BX : (y + 1) * BX]

        planes = [None] * 12
        for y in range(2):
            wx, wy, rho = half(0, y), half(1, y), half(6, y)
            scale = rho * CD_ICE * jnp.sqrt(wx * wx + wy * wy + 1.0)
            planes[y] = scale * wx
            planes[2 + y] = scale * wy
            for ch in range(2, 6):
                planes[2 * ch + y] = half(ch, y)
        ends = jnp.zeros((per, BX), jnp.float32)
        for p in range(12):
            pay[t, pl.ds(p, per, stride=12), :] = planes[p]
            ends = jnp.where(group == p, roll(planes[p], 8 * p + 4), ends)
        edge[t] = ends
        ids = jnp.zeros((per, BX), jnp.int32)
        for j in range(per):
            ids = jnp.where(slot == j, owner[0, t * per + j] - t * count, ids)

        def pick(block, value):
            return jnp.sum(jnp.where(ids == block, value, 0.0), axis=0, keepdims=True)

        rows = [pick(0, x) for x in planes] + [pick(1, x) for x in planes[0::2]]
        rows += [pick(count - 1, x) for x in planes]
        rows += [pick(count - 2, x) for x in planes[1::2]]
        rows += [pick(b, ends) for b in (0, 1, count - 1, count - 2)]
        for k, row in enumerate(rows):
            rim[t, k : k + 1, :] = row
        return 0

    steps(0, n, tile)

    def dest(d, _):
        i, j = d // nlon, d % nlon
        jw, je = (j + nlon - 1) % nlon, (j + 1) % nlon
        q8 = (lane % 8) < 4
        pay[d, 12 * per : 13 * per, :] = at_end(q8, edge[i * nlon + jw], edge[i * nlon + je])
        for ii, ok, lo, c in (
            (jnp.minimum(i + 1, nlat - 1), i + 1 < nlat, 0, 36),
            (jnp.maximum(i - 1, 0), i > 0, 18, 38),
        ):
            scale = jnp.where(ok, 1.0, 0.0)
            pay[d, lat_base + lo : lat_base + lo + 18, :] = rim[ii * nlon + j, lo : lo + 18, :] * scale
            q2 = (lanes(2) % 8) < 4
            corner = at_end(q2, rim[ii * nlon + jw, c : c + 2, :], rim[ii * nlon + je, c : c + 2, :])
            pay[d, lat_base + c : lat_base + c + 2, :] = corner * scale
        return 0

    steps(0, n, dest)


def ends_kernel(ice, covered, land, active, ends):
    count = covered.shape[1]
    lane = lanes(count)
    group = lane // 8
    total = jnp.zeros((count, BX), jnp.float32)
    cover = column(covered[...])
    for y in range(2):
        cells = slice(y * BX, (y + 1) * BX)
        act = cover * (1 - land[:, cells]).astype(jnp.float32)
        active[:, cells] = act
        for ch in range(8):
            x = act if ch == 7 else ice[ch, :, cells]
            p = 2 * ch + y
            total = jnp.where(group == p, roll(x, 8 * p + 4), total)
    ends[...] = total


def pack_kernel(nlat, nlon, per, raw, owner, pay, edge, rim):
    @pl.when(lax.axis_index("comp") == 1)
    def _():
        pack_body(nlat, nlon, per, nlat * nlon * per, raw, owner, pay, edge, rim)


def pack(raw, owner, nlat, nlon):
    _, n, per, _ = raw.shape
    return pl.pallas_call(
        functools.partial(pack_kernel, nlat, nlon, per),
        out_shape=f32(n, 13 * per + 40, BX),
        in_specs=[VMEM, SMEM],
        out_specs=VMEM,
        scratch_shapes=[pltpu.VMEM((n, per, BX), jnp.float32), pltpu.VMEM((n, 40, BX), jnp.float32)],
        compiler_params=params(24),
        name="pack",
    )(raw, owner)


def open_kernel(n, per, raw, opened):
    @pl.when(lax.axis_index("comp") == 0)
    def _():
        def tile(t, _):
            for y in range(2):
                wx, wy, cx, cy, rho = [raw[ch, t, :, y * BX : (y + 1) * BX] for ch in (0, 1, 2, 3, 6)]
                rx, ry = wx - cx, wy - cy
                speed = jnp.sqrt(rx * rx + ry * ry + 1.0)
                rate = rho * (0.1 + 0.05 * speed) * speed
                opened[t, 2 * y] = rate * rx
                opened[t, 2 * y + 1] = rate * ry
            return 0

        steps(0, n, tile)


def open_stress(raw):
    _, n, per, _ = raw.shape
    return pl.pallas_call(
        functools.partial(open_kernel, n, per),
        out_shape=f32(n, 4, per, BX),
        in_specs=[VMEM],
        out_specs=VMEM,
        compiler_params=params(24),
        name="open_stress",
    )(raw)


def ice_ends(ice, covered, land):
    count = land.shape[0]
    return pl.pallas_call(
        ends_kernel,
        out_shape=[f32(count, 2 * BX), f32(count, BX)],
        in_specs=[VMEM] * 3,
        out_specs=[VMEM] * 2,
        compiler_params=params(8),
        name="ice_ends",
    )(ice, covered, land)


def table_kernel(nlat, nlon, per, owner, ids):
    def tile(t, _):
        i, j = t // nlon, t % nlon
        near = [t, i * nlon + (j + nlon - 1) % nlon, i * nlon + (j + 1) % nlon]
        for k, other in enumerate(near):
            for slot in range(per):
                ids[t, k * per + slot] = owner[0, other * per + slot] - other * (nlat * nlon * per)
        return 0

    steps(0, nlat * nlon, tile)


def table(owner, nlat, nlon):
    n = nlat * nlon
    per = owner.shape[1] // n
    return pl.pallas_call(
        functools.partial(table_kernel, nlat, nlon, per),
        out_shape=jax.ShapeDtypeStruct((n, 3 * per), jnp.int32),
        in_specs=[SMEM],
        out_specs=SMEM,
        compiler_params=params(4),
        name="table",
    )(owner)


def rows_kernel(ice, active, west, east, sides, north, south):
    count = active.shape[0]
    q = (lanes(count) % 8) < 4
    sides[...] = jnp.where(q, west[...], east[...])
    for out, lo in ((north, count - 2), (south, 0)):
        for y in range(2):
            cells = slice(y * BX, (y + 1) * BX)
            for ch in range(8):
                p = 2 * ch + y
                x = active[lo : lo + 2, cells] if ch == 7 else ice[ch, lo : lo + 2, cells]
                out[2 * p : 2 * p + 2, :] = x
        out[32:34, :] = sides[lo : lo + 2, :]


def ice_rows(ice, active, west, east):
    count = active.shape[0]
    return pl.pallas_call(
        rows_kernel,
        out_shape=[f32(count, BX), f32(34, BX), f32(34, BX)],
        in_specs=[VMEM] * 4,
        out_specs=[VMEM] * 3,
        compiler_params=params(8),
        name="ice_rows",
    )(ice, active, west, east)


def middle(rows):
    lane = lanes(rows)
    return (lane >= BX // 4) & (lane < 3 * BX // 4)


def side_plane(ends, ch, mid):
    odd = roll(ends, BX // 2 - (8 * (2 * ch + 1) + 4))
    return jnp.where(mid, odd, roll(ends, -(16 * ch + 4)))


def statics(mass, conc, act):
    return mass * jnp.exp(CSTAR * (conc - 1.0)) * act * (1.0 / 6.0), 2.0 * mass, CW * conc * act, act, conc


def prep_kernel(count, height, ice, active, sides, begin, still, grid):
    mid = middle(count)
    for ch in range(8):
        for y in range(2):
            cells = slice(y * BX, (y + 1) * BX)
            grid[ch, y, 2 : 2 + count, :] = active[:, cells] if ch == 7 else ice[ch, :, cells]
        grid[ch, 2, 2 : 2 + count, :] = side_plane(sides[...], ch, mid)
        for z in range(3):
            grid[ch, z, 0:2, :] = jnp.zeros((2, BX), jnp.float32)
            grid[ch, z, count + 2 :, :] = jnp.zeros((height - count - 2, BX), jnp.float32)

    for r in range(height // 8):
        at = slice(8 * r, 8 * r + 8)
        for z in range(3):
            u, v, mass, conc, s1, s2, s12, act = [grid[ch, z, at, :] for ch in range(8)]
            for k, x in enumerate((u, v, 0.5 * s1, 0.5 * s2, s12)):
                begin[k, z, at, :] = x
            for k, x in enumerate(statics(mass, conc, act)):
                still[k, z, at, :] = x


def prep(ice, active, sides):
    count = active.shape[0]
    height = (count + 4 + 7) // 8 * 8
    return pl.pallas_call(
        functools.partial(prep_kernel, count, height),
        out_shape=[f32(5, 3, height, BX)] * 2,
        in_specs=[VMEM] * 3,
        out_specs=[VMEM] * 2,
        scratch_shapes=[pltpu.VMEM((8, 3, height, BX), jnp.float32)],
        compiler_params=params(12),
        name="prep",
    )(ice, active, sides)


def fetch_kernel(*refs):
    k = len(refs) // 2
    copies = [pltpu.make_async_copy(refs[i], refs[k + i], refs[-1].at[i]) for i in range(k)]
    for copy in copies:
        copy.start()
    for copy in copies:
        copy.wait()


def fetch(*arrays):
    return pl.pallas_call(
        fetch_kernel,
        out_shape=[f32(*x.shape) for x in arrays],
        in_specs=[pl.BlockSpec(memory_space=pl.ANY)] * len(arrays),
        out_specs=[VMEM] * len(arrays),
        scratch_shapes=[pltpu.SemaphoreType.DMA((len(arrays),))],
        compiler_params=params(4),
        name="fetch",
    )(*arrays)


def east_of(even, odd, side, at127, at63):
    e, o, s = roll(even, -1), roll(odd, -1), roll(side, -1)
    wide = jnp.where(at127, e, jnp.where(at63, roll(odd, 63), s))
    return jnp.where(at127, s, e), jnp.where(at127, roll(side, 63), o), wide


def west_of(even, odd, side, at0, at64):
    e, o, s = roll(even, 1), roll(odd, 1), roll(side, 1)
    wide = jnp.where(at0, e, jnp.where(at64, roll(odd, 65), s))
    return jnp.where(at0, s, e), jnp.where(at0, roll(side, -63), o), wide


def ice_kernel(n, per, count, ids, recv, begin, fixed, below, above, back, moved,
               spot, hw, he, speed, state, forced, out8, still):
    tiles = (count + 4 + 7) // 8
    height = tiles * 8
    blank = jnp.zeros((8, BX), jnp.float32)
    for k in (0, 8):
        spot[k : k + 8, :] = blank
    for k in range((count + 3) * STEP, height * STEP, 8):
        spot[k : k + 8, :] = blank
    for k in (0, height - 8):
        hw[k : k + 8, :] = blank
        he[k : k + 8, :] = blank

    def place(o, acc):
        for j in range(per):
            b = (ids[o, j] + 2) * STEP
            spot[pl.ds(b, 12), :] = recv[o, 12 * j : 12 * j + 12, :]
            row = recv[o, 12 * per + j : 12 * per + j + 1, :]
            hw[pl.ds(ids[o, per + j] + 2, 1), :] = row
            he[pl.ds(ids[o, 2 * per + j] + 2, 1), :] = row
        return acc + recv[o, 13 * per : 13 * per + 40, :]

    rim = lax.fori_loop(0, n, place, jnp.zeros((40, BX), jnp.float32))
    up, down = (count + 2) * STEP, STEP
    spot[up : up + 12, :] = rim[0:12]
    spot[down : down + 12, :] = rim[18:30]
    for ch in range(6):
        k = up + STEP + 2 * ch
        spot[k : k + 1, :] = rim[12 + ch : 13 + ch]
        k = 2 * ch + 1
        spot[k : k + 1, :] = rim[30 + ch : 31 + ch]
    for ref in (hw, he):
        ref[count + 2 : count + 4, :] = rim[36:38]
        ref[1:2, :] = rim[38:39]
        ref[0:1, :] = rim[39:40]

    q, mid, mid2 = (lanes(8) % 8) < 4, middle(8), middle(2)
    for r in range(tiles):
        at = slice(8 * r, 8 * r + 8)
        to = slice(FRONT + 8 * r, FRONT + 8 * r + 8)
        for z in range(3):
            for k in range(2):
                speed[k, z, to, :] = begin[k, z, at, :]
            for k in range(3):
                state[k, z, to, :] = begin[2 + k, z, at, :]
            for k in range(5):
                still[k, z, at, :] = fixed[k, z, at, :]
    for lo, msg in ((0, below), (count + 2, above)):
        at, to = slice(lo, lo + 2), slice(FRONT + lo, FRONT + lo + 2)
        for z in range(3):
            if z < 2:
                raw = [msg[4 * ch + 2 * z : 4 * ch + 2 * z + 2, :] for ch in range(8)]
            else:
                raw = [side_plane(msg[32:34, :], ch, mid2) for ch in range(8)]
            u, v, mass, conc, s1, s2, s12, act = raw
            speed[0, z, to, :] = u
            speed[1, z, to, :] = v
            state[0, z, to, :] = 0.5 * s1
            state[1, z, to, :] = 0.5 * s2
            state[2, z, to, :] = s12
            for k, x in enumerate(statics(mass, conc, act)):
                still[k, z, at, :] = x

    for r in range(tiles):
        at = slice(8 * r, 8 * r + 8)
        ends = jnp.where(q, hw[at, :], he[at, :])
        for z in range(3):
            if z < 2:
                f = [spot[pl.ds(8 * r * STEP + 2 * ch + z, 8, stride=STEP), :] for ch in range(6)]
            else:
                f = [side_plane(ends, ch, mid) for ch in range(6)]
            mass, act, conc = [still[k, z, at, :] for k in (1, 3, 4)]
            mass = 0.5 * mass
            forced[0, z, at, :] = act * (conc * f[0] - mass * f[4])
            forced[1, z, at, :] = act * (conc * f[1] - mass * f[5])
            forced[2, z, at, :] = f[2]
            forced[3, z, at, :] = f[3]

    tail = FRONT + height
    for z in range(3):
        for k in range(2):
            speed[k, z, tail : tail + 8, :] = blank
        for k in range(3):
            state[k, z, 0:8, :] = blank

    lane = lanes(8)
    ends_at = [lane == k for k in (BX - 1, BX // 2 - 1, 0, BX // 2)]
    at127, at63, at0, at64 = ends_at

    def rows_of(r):
        row = 8 * r
        return pl.ds(row, 8), pl.ds(row + FRONT, 8), pl.ds(row + FRONT + 1, 8), pl.ds(row + FRONT - 1, 8)

    def stresses(r):
        at, to, up1, _ = rows_of(r)
        u = [speed[0, z, to, :] for z in range(3)]
        v = [speed[1, z, to, :] for z in range(3)]

        def north(k, x):
            return x[1], speed[k, 0, up1, :], roll(jnp.where(mid, x[2], speed[k, 2, up1, :]), BX // 2)

        un, vn = north(0, u), north(1, v)
        ue = east_of(*u, at127, at63)
        ve = east_of(*v, at127, at63)
        for z in range(3):
            sxx = ue[z] - u[z]
            syy = vn[z] - v[z]
            shear = (un[z] - u[z]) + (ve[z] - v[z])
            div, ten = sxx + syy, sxx - syy
            twice = div + div
            inv = lax.rsqrt(twice * twice + (ten * ten + shear * shear) + 1.0)
            hard = still[0, z, at, :]
            kr = hard * inv
            half = 0.5 * kr
            state[0, z, to, :] = (state[0, z, to, :] * (2.0 / 3.0) - hard) + kr * twice
            state[1, z, to, :] = state[1, z, to, :] * (2.0 / 3.0) + half * ten
            state[2, z, to, :] = state[2, z, to, :] * (2.0 / 3.0) + half * shear

    def speeds(r):
        at, to, _, down1 = rows_of(r)
        s1, s2, s12 = [[state[k, z, to, :] for z in range(3)] for k in range(3)]
        a = [x + y for x, y in zip(s1, s2)]
        c = [x - y for x, y in zip(s1, s2)]
        aw = west_of(*a, at0, at64)
        sw = west_of(*s12, at0, at64)

        def south(x, lower):
            return lower(1), x[0], roll(jnp.where(mid, lower(2), x[2]), BX // 2)

        ss = south(s12, lambda z: state[2, z, down1, :])
        cs = south(c, lambda z: state[0, z, down1, :] - state[1, z, down1, :])
        for z in range(3):
            u, v = speed[0, z, to, :], speed[1, z, to, :]
            fx = (a[z] - aw[z]) + (s12[z] - ss[z])
            fy = (s12[z] - sw[z]) + (c[z] - cs[z])
            m2, base = still[1, z, at, :], still[2, z, at, :]
            cx, cy = forced[2, z, at, :], forced[3, z, at, :]
            dx, dy = cx - u, cy - v
            y2 = dx * dx + dy * dy + DRAG_FLOOR
            drag = base * (y2 * lax.rsqrt(y2))
            part = still[3, z, at, :] * (1.0 / (jnp.maximum(m2, 1.0) + drag))
            mc = (0.5 * CORIO) * m2
            speed[0, z, to, :] = part * (m2 * u + fx + forced[0, z, at, :] + drag * cx + mc * v)
            speed[1, z, to, :] = part * (m2 * v + fy + forced[1, z, at, :] + drag * cy - mc * u)

    def subcycle(_, carry):
        for r in range(tiles):
            stresses(r)
        for r in range(tiles):
            speeds(r)
        return carry

    lax.fori_loop(0, NSUB, subcycle, 0)

    for r in range(tiles):
        at = slice(8 * r, 8 * r + 8)
        to = slice(FRONT + 8 * r, FRONT + 8 * r + 8)
        for y in range(2):
            base = still[2, y, at, :]
            dx = speed[0, y, to, :] - forced[2, y, at, :]
            dy = speed[1, y, to, :] - forced[3, y, at, :]
            y2 = dx * dx + dy * dy + DRAG_FLOOR
            factor = base * (y2 * lax.rsqrt(y2))
            for k, x in enumerate((factor * dx, factor * dy, base * (1.0 / CW))):
                out8[pl.ds(8 * r * REPLY + 2 * k + y, 8, stride=REPLY), :] = x
    for y in range(2):
        for k in range(2):
            moved[k, :, y * BX : (y + 1) * BX] = speed[k, y, FRONT + 2 : FRONT + 2 + count, :]

    def answer(o, _):
        for j in range(per):
            b = (ids[o, j] + 2) * REPLY
            back[o, 6 * j : 6 * j + 6, :] = out8[pl.ds(b, 6), :]
        return 0

    lax.fori_loop(0, n, answer, 0)


def ice_step(ids, recv, begin, fixed, below, above):
    n, per = ids.shape[0], ids.shape[1] // 3
    count = n * per
    height = (count + 4 + 7) // 8 * 8
    tall = height + 2 * FRONT
    scratch = [
        (height * STEP + 8, BX), (height, BX), (height, BX),
        (2, 3, tall, BX), (3, 3, tall, BX), (4, 3, height, BX), (height * REPLY + 8, BX), (5, 3, height, BX),
    ]
    return pl.pallas_call(
        functools.partial(ice_kernel, n, per, count),
        out_shape=[f32(n, 6 * per, BX), f32(2, count, 2 * BX)],
        in_specs=[SMEM] + [VMEM] * 5,
        out_specs=[VMEM] * 2,
        scratch_shapes=[pltpu.VMEM(s, jnp.float32) for s in scratch],
        compiler_params=params(16),
        name="ice_step",
    )(ids, recv, begin, fixed, below, above)


def final_kernel(n, per, got, opened, moved, out):
    is_ocean = lax.axis_index("comp") == 0

    @pl.when(is_ocean)
    def _():
        def tile(t, _):
            for y in range(2):
                cells = slice(y * BX, (y + 1) * BX)
                gx, gy, gc = [got[t, pl.ds(2 * k + y, per, stride=6), :] for k in range(3)]
                out[0, t, :, cells] = gx + (1.0 - gc) * opened[t, 2 * y]
                out[1, t, :, cells] = gy + (1.0 - gc) * opened[t, 2 * y + 1]
            return 0

        lax.fori_loop(0, n, tile, 0)

    @pl.when(jnp.logical_not(is_ocean))
    def _():
        out[...] = moved[...]


def final(got, opened, moved):
    n, _, per, _ = opened.shape
    return pl.pallas_call(
        functools.partial(final_kernel, n, per),
        out_shape=f32(2, n, per, 2 * BX),
        in_specs=[VMEM] * 3,
        out_specs=VMEM,
        compiler_params=params(8),
        name="final",
    )(got, opened, moved)


def per_device(fields, block_owner, ice_covered, land_mask):
    nlat, nlon = lax.axis_size("lat"), lax.axis_size("lon")
    n = nlat * nlon
    count = block_owner.shape[0]
    per = count // n
    side = lax.axis_index("comp")
    fields = fields[0]
    split = fields.reshape(7, n, per, 2 * BX)
    owner = block_owner.reshape(1, count)
    other = lax.ppermute(split, "comp", [(0, 1), (1, 0)])
    opened = open_stress(split)
    pay = pack(other, owner, nlat, nlon)
    def everyone(x):
        return lax.all_to_all(x, ("lat", "lon"), split_axis=0, concat_axis=0, tiled=True)

    height = (count + 4 + 7) // 8 * 8

    def ice_side(pay, fields, covered, land, owner):
        recv = everyone(pay)
        active, ends = ice_ends(fields, covered, land)
        ring = [(i, (i + 1) % nlon) for i in range(nlon)]
        west = lax.ppermute(ends, "lon", ring)
        east = lax.ppermute(ends, "lon", [(j, i) for i, j in ring])
        sides, north, south = ice_rows(fields, active, west, east)
        line = [(i, i + 1) for i in range(nlat - 1)]
        below = lax.ppermute(north, "lat", line)
        above = lax.ppermute(south, "lat", [(j, i) for i, j in line])
        begin, fixed = prep(fields, active, sides)
        return recv, jnp.zeros((n, 3 * per), jnp.int32), below, above, begin, fixed

    def ocean_side(pay, fields, covered, land, owner):
        row = jnp.zeros((34, BX), jnp.float32)
        blank = jnp.zeros((5, 3, height, BX), jnp.float32)
        return jnp.zeros(pay.shape, jnp.float32), everyone(table(owner, nlat, nlon)), row, row, blank, blank

    recv, owned, below, above, begin, fixed = lax.cond(
        side == 1, ice_side, ocean_side, pay, fields, ice_covered.reshape(1, count), land_mask, owner
    )
    swap = lax.ppermute(owned, "comp", [(0, 1), (1, 0)])
    recv, below, above = fetch(recv, below, above)
    back, moved = ice_step(swap, recv, begin, fixed, below, above)
    back = lax.cond(side == 1, everyone, lambda x: x, back)
    got = lax.ppermute(back, "comp", [(0, 1), (1, 0)])
    out = final(got, opened, moved.reshape(2, n, per, 2 * BX))
    return out.reshape(1, 2, count, 2 * BX)


def solution(mesh):
    placed = (
        P("comp", None, ("lat", "lon"), None),
        P(("lat", "lon")),
        P(("lat", "lon")),
        P(("lat", "lon"), None),
    )
    return jax.shard_map(
        per_device,
        mesh=mesh,
        in_specs=placed,
        out_specs=P("comp", None, ("lat", "lon"), None),
        check_vma=False,
    )
```

```python
import functools

import jax
import jax.numpy as jnp
from jax import lax
from jax.experimental import pallas as pl
from jax.experimental.pallas import tpu as pltpu
from jax.sharding import PartitionSpec as P

BX = 128
NSUB = 4
FRONT = 8
STEP = 13
REPLY = 7

CD_ICE = 0.1
CW = 1.5
CSTAR = 2.0
CORIO = 0.3
DRAG_FLOOR = 0.1

VMEM = pl.BlockSpec(memory_space=pltpu.VMEM)
SMEM = pl.BlockSpec(memory_space=pltpu.SMEM)


def params(mib):
    return pltpu.CompilerParams(vmem_limit_bytes=mib * 1024 * 1024)


def f32(*shape):
    return jax.ShapeDtypeStruct(shape, jnp.float32)


def lanes(rows):
    return lax.broadcasted_iota(jnp.int32, (rows, BX), 1)


def roll(x, by):
    return pltpu.roll(x, by % BX, 1)


def at_end(q, west, east):
    return jnp.where(q, west, east)


def column(row):
    parts = []
    for lo in range(0, row.shape[1], BX):
        diag = lax.broadcasted_iota(jnp.int32, (BX, BX), 0) == lanes(BX)
        parts.append(jnp.sum(jnp.where(diag, row[:, lo : lo + BX].astype(jnp.float32), 0.0), axis=1, keepdims=True))
    return jnp.concatenate(parts, 0) if len(parts) > 1 else parts[0]


def steps(lo, hi, body):
    if hi - lo <= 32:
        for k in range(lo, hi):
            body(k, 0)
    else:
        lax.fori_loop(lo, hi, body, 0)


def pack_kernel(nlat, nlon, per, raw, owner, out, pay, edge, rim, sems):
    n = nlat * nlon
    count = n * per
    cut = 12 * per if (12 * per) % 8 == 0 else 0

    def send(d, k):
        at = pl.ds(0, cut) if k == 0 else pl.ds(cut, 13 * per + 40 - cut)
        return pltpu.make_async_copy(pay.at[d, at], out.at[d, at], sems.at[k, d])

    lane = lanes(per)
    group = lane // 8
    slot = lax.broadcasted_iota(jnp.int32, (per, BX), 0)
    lat_base = 13 * per

    def tile(t, _):
        def half(ch, y):
            return raw[ch, t, :, y * BX : (y + 1) * BX]

        planes = [None] * 12
        for y in range(2):
            wx, wy, rho = half(0, y), half(1, y), half(6, y)
            scale = rho * CD_ICE * jnp.sqrt(wx * wx + wy * wy + 1.0)
            planes[y] = scale * wx
            planes[2 + y] = scale * wy
            for ch in range(2, 6):
                planes[2 * ch + y] = half(ch, y)
        ends = jnp.zeros((per, BX), jnp.float32)
        for p in range(12):
            pay[t, pl.ds(p, per, stride=12), :] = planes[p]
            ends = jnp.where(group == p, roll(planes[p], 8 * p + 4), ends)
        edge[t] = ends
        ids = jnp.zeros((per, BX), jnp.int32)
        for j in range(per):
            ids = jnp.where(slot == j, owner[0, t * per + j] - t * count, ids)

        def pick(block, value):
            return jnp.sum(jnp.where(ids == block, value, 0.0), axis=0, keepdims=True)

        rows = [pick(0, x) for x in planes] + [pick(1, x) for x in planes[0::2]]
        rows += [pick(count - 1, x) for x in planes]
        rows += [pick(count - 2, x) for x in planes[1::2]]
        rows += [pick(b, ends) for b in (0, 1, count - 1, count - 2)]
        for k, row in enumerate(rows):
            rim[t, k : k + 1, :] = row
        if cut:
            send(t, 0).start()
        return 0

    steps(0, n, tile)

    def dest(d, _):
        i, j = d // nlon, d % nlon
        jw, je = (j + nlon - 1) % nlon, (j + 1) % nlon
        q8 = (lane % 8) < 4
        pay[d, 12 * per : 13 * per, :] = at_end(q8, edge[i * nlon + jw], edge[i * nlon + je])
        for ii, ok, lo, c in (
            (jnp.minimum(i + 1, nlat - 1), i + 1 < nlat, 0, 36),
            (jnp.maximum(i - 1, 0), i > 0, 18, 38),
        ):
            scale = jnp.where(ok, 1.0, 0.0)
            pay[d, lat_base + lo : lat_base + lo + 18, :] = rim[ii * nlon + j, lo : lo + 18, :] * scale
            q2 = (lanes(2) % 8) < 4
            corner = at_end(q2, rim[ii * nlon + jw, c : c + 2, :], rim[ii * nlon + je, c : c + 2, :])
            pay[d, lat_base + c : lat_base + c + 2, :] = corner * scale
        send(d, 1).start()
        return 0

    def finish(d, _):
        if cut:
            send(d, 0).wait()
        send(d, 1).wait()
        return 0

    steps(0, n, dest)
    steps(0, n, finish)


def ends_kernel(ice, covered, land, active, ends):
    count = covered.shape[1]
    lane = lanes(count)
    group = lane // 8
    total = jnp.zeros((count, BX), jnp.float32)
    cover = column(covered[...])
    for y in range(2):
        cells = slice(y * BX, (y + 1) * BX)
        act = cover * (1 - land[:, cells]).astype(jnp.float32)
        active[:, cells] = act
        for ch in range(8):
            x = act if ch == 7 else ice[ch, :, cells]
            p = 2 * ch + y
            total = jnp.where(group == p, roll(x, 8 * p + 4), total)
    ends[...] = total


def pack(raw, owner, nlat, nlon):
    _, n, per, _ = raw.shape
    rows = 13 * per + 40
    return pl.pallas_call(
        functools.partial(pack_kernel, nlat, nlon, per),
        out_shape=f32(n, rows, BX),
        in_specs=[VMEM, SMEM],
        out_specs=pl.BlockSpec(memory_space=pl.ANY),
        scratch_shapes=[
            pltpu.VMEM((n, rows, BX), jnp.float32),
            pltpu.VMEM((n, per, BX), jnp.float32),
            pltpu.VMEM((n, 40, BX), jnp.float32),
            pltpu.SemaphoreType.DMA((2, n)),
        ],
        compiler_params=params(24),
        name="pack",
    )(raw, owner)


def open_kernel(n, per, raw, opened):
    @pl.when(lax.axis_index("comp") == 0)
    def _():
        def tile(t, _):
            for y in range(2):
                wx, wy, cx, cy, rho = [raw[ch, t, :, y * BX : (y + 1) * BX] for ch in (0, 1, 2, 3, 6)]
                rx, ry = wx - cx, wy - cy
                speed = jnp.sqrt(rx * rx + ry * ry + 1.0)
                rate = rho * (0.1 + 0.05 * speed) * speed
                opened[t, 2 * y] = rate * rx
                opened[t, 2 * y + 1] = rate * ry
            return 0

        steps(0, n, tile)


def open_stress(raw):
    _, n, per, _ = raw.shape
    return pl.pallas_call(
        functools.partial(open_kernel, n, per),
        out_shape=f32(n, 4, per, BX),
        in_specs=[VMEM],
        out_specs=VMEM,
        compiler_params=params(24),
        name="open_stress",
    )(raw)


def ice_ends(ice, covered, land):
    count = land.shape[0]
    return pl.pallas_call(
        ends_kernel,
        out_shape=[f32(count, 2 * BX), f32(count, BX)],
        in_specs=[VMEM] * 3,
        out_specs=[VMEM] * 2,
        compiler_params=params(8),
        name="ice_ends",
    )(ice, covered, land)


def table_kernel(nlat, nlon, per, owner, ids):
    def tile(t, _):
        i, j = t // nlon, t % nlon
        near = [t, i * nlon + (j + nlon - 1) % nlon, i * nlon + (j + 1) % nlon]
        for k, other in enumerate(near):
            for slot in range(per):
                ids[t, k * per + slot] = owner[0, other * per + slot] - other * (nlat * nlon * per)
        return 0

    steps(0, nlat * nlon, tile)


def table(owner, nlat, nlon):
    n = nlat * nlon
    per = owner.shape[1] // n
    return pl.pallas_call(
        functools.partial(table_kernel, nlat, nlon, per),
        out_shape=jax.ShapeDtypeStruct((n, 3 * per), jnp.int32),
        in_specs=[SMEM],
        out_specs=SMEM,
        compiler_params=params(4),
        name="table",
    )(owner)


def rows_kernel(ice, active, west, east, sides, north, south):
    count = active.shape[0]
    q = (lanes(count) % 8) < 4
    sides[...] = jnp.where(q, west[...], east[...])
    for out, lo in ((north, count - 2), (south, 0)):
        for y in range(2):
            cells = slice(y * BX, (y + 1) * BX)
            for ch in range(8):
                p = 2 * ch + y
                x = active[lo : lo + 2, cells] if ch == 7 else ice[ch, lo : lo + 2, cells]
                out[2 * p : 2 * p + 2, :] = x
        out[32:34, :] = sides[lo : lo + 2, :]


def ice_rows(ice, active, west, east):
    count = active.shape[0]
    return pl.pallas_call(
        rows_kernel,
        out_shape=[f32(count, BX), f32(34, BX), f32(34, BX)],
        in_specs=[VMEM] * 4,
        out_specs=[VMEM] * 3,
        compiler_params=params(8),
        name="ice_rows",
    )(ice, active, west, east)


def middle(rows):
    lane = lanes(rows)
    return (lane >= BX // 4) & (lane < 3 * BX // 4)


def side_plane(ends, ch, mid):
    odd = roll(ends, BX // 2 - (8 * (2 * ch + 1) + 4))
    return jnp.where(mid, odd, roll(ends, -(16 * ch + 4)))


def statics(mass, conc, act):
    return mass * jnp.exp(CSTAR * (conc - 1.0)) * act * (1.0 / 6.0), 2.0 * mass, CW * conc * act, act, conc


def prep_kernel(count, height, ice, active, sides, begin, still, grid):
    mid = middle(count)
    for ch in range(8):
        for y in range(2):
            cells = slice(y * BX, (y + 1) * BX)
            grid[ch, y, 2 : 2 + count, :] = active[:, cells] if ch == 7 else ice[ch, :, cells]
        grid[ch, 2, 2 : 2 + count, :] = side_plane(sides[...], ch, mid)
        for z in range(3):
            grid[ch, z, 0:2, :] = jnp.zeros((2, BX), jnp.float32)
            grid[ch, z, count + 2 :, :] = jnp.zeros((height - count - 2, BX), jnp.float32)

    for r in range(height // 8):
        at = slice(8 * r, 8 * r + 8)
        for z in range(3):
            u, v, mass, conc, s1, s2, s12, act = [grid[ch, z, at, :] for ch in range(8)]
            for k, x in enumerate((u, v, 0.5 * s1, 0.5 * s2, s12)):
                begin[k, z, at, :] = x
            for k, x in enumerate(statics(mass, conc, act)):
                still[k, z, at, :] = x


def prep(ice, active, sides):
    count = active.shape[0]
    height = (count + 4 + 7) // 8 * 8
    return pl.pallas_call(
        functools.partial(prep_kernel, count, height),
        out_shape=[f32(5, 3, height, BX)] * 2,
        in_specs=[VMEM] * 3,
        out_specs=[VMEM] * 2,
        scratch_shapes=[pltpu.VMEM((8, 3, height, BX), jnp.float32)],
        compiler_params=params(12),
        name="prep",
    )(ice, active, sides)


def fetch_kernel(*refs):
    k = len(refs) // 2
    copies = [pltpu.make_async_copy(refs[i], refs[k + i], refs[-1].at[i]) for i in range(k)]
    for copy in copies:
        copy.start()
    for copy in copies:
        copy.wait()


def fetch(*arrays):
    return pl.pallas_call(
        fetch_kernel,
        out_shape=[f32(*x.shape) for x in arrays],
        in_specs=[pl.BlockSpec(memory_space=pl.ANY)] * len(arrays),
        out_specs=[VMEM] * len(arrays),
        scratch_shapes=[pltpu.SemaphoreType.DMA((len(arrays),))],
        compiler_params=params(4),
        name="fetch",
    )(*arrays)


def east_of(even, odd, side, at127, at63):
    e, o, s = roll(even, -1), roll(odd, -1), roll(side, -1)
    wide = jnp.where(at127, e, jnp.where(at63, roll(odd, 63), s))
    return jnp.where(at127, s, e), jnp.where(at127, roll(side, 63), o), wide


def west_of(even, odd, side, at0, at64):
    e, o, s = roll(even, 1), roll(odd, 1), roll(side, 1)
    wide = jnp.where(at0, e, jnp.where(at64, roll(odd, 65), s))
    return jnp.where(at0, s, e), jnp.where(at0, roll(side, -63), o), wide


def ice_kernel(n, per, count, ids, recv, begin, fixed, below, above, back, moved,
               spot, hw, he, speed, state, forced, out8, still):
    tiles = (count + 4 + 7) // 8
    height = tiles * 8
    blank = jnp.zeros((8, BX), jnp.float32)
    for k in (0, 8):
        spot[k : k + 8, :] = blank
    for k in range((count + 3) * STEP, height * STEP, 8):
        spot[k : k + 8, :] = blank
    for k in (0, height - 8):
        hw[k : k + 8, :] = blank
        he[k : k + 8, :] = blank

    def place(o, acc):
        for j in range(per):
            b = (ids[o, j] + 2) * STEP
            spot[pl.ds(b, 12), :] = recv[o, 12 * j : 12 * j + 12, :]
            row = recv[o, 12 * per + j : 12 * per + j + 1, :]
            hw[pl.ds(ids[o, per + j] + 2, 1), :] = row
            he[pl.ds(ids[o, 2 * per + j] + 2, 1), :] = row
        return acc + recv[o, 13 * per : 13 * per + 40, :]

    rim = lax.fori_loop(0, n, place, jnp.zeros((40, BX), jnp.float32))
    up, down = (count + 2) * STEP, STEP
    spot[up : up + 12, :] = rim[0:12]
    spot[down : down + 12, :] = rim[18:30]
    for ch in range(6):
        k = up + STEP + 2 * ch
        spot[k : k + 1, :] = rim[12 + ch : 13 + ch]
        k = 2 * ch + 1
        spot[k : k + 1, :] = rim[30 + ch : 31 + ch]
    for ref in (hw, he):
        ref[count + 2 : count + 4, :] = rim[36:38]
        ref[1:2, :] = rim[38:39]
        ref[0:1, :] = rim[39:40]

    q, mid, mid2 = (lanes(8) % 8) < 4, middle(8), middle(2)
    for r in range(tiles):
        at = slice(8 * r, 8 * r + 8)
        to = slice(FRONT + 8 * r, FRONT + 8 * r + 8)
        for z in range(3):
            for k in range(2):
                speed[k, z, to, :] = begin[k, z, at, :]
            for k in range(3):
                state[k, z, to, :] = begin[2 + k, z, at, :]
            for k in range(5):
                still[k, z, at, :] = fixed[k, z, at, :]
    for lo, msg in ((0, below), (count + 2, above)):
        at, to = slice(lo, lo + 2), slice(FRONT + lo, FRONT + lo + 2)
        for z in range(3):
            if z < 2:
                raw = [msg[4 * ch + 2 * z : 4 * ch + 2 * z + 2, :] for ch in range(8)]
            else:
                raw = [side_plane(msg[32:34, :], ch, mid2) for ch in range(8)]
            u, v, mass, conc, s1, s2, s12, act = raw
            speed[0, z, to, :] = u
            speed[1, z, to, :] = v
            state[0, z, to, :] = 0.5 * s1
            state[1, z, to, :] = 0.5 * s2
            state[2, z, to, :] = s12
            for k, x in enumerate(statics(mass, conc, act)):
                still[k, z, at, :] = x

    for r in range(tiles):
        at = slice(8 * r, 8 * r + 8)
        ends = jnp.where(q, hw[at, :], he[at, :])
        for z in range(3):
            if z < 2:
                f = [spot[pl.ds(8 * r * STEP + 2 * ch + z, 8, stride=STEP), :] for ch in range(6)]
            else:
                f = [side_plane(ends, ch, mid) for ch in range(6)]
            mass, act, conc = [still[k, z, at, :] for k in (1, 3, 4)]
            mass = 0.5 * mass
            forced[0, z, at, :] = act * (conc * f[0] - mass * f[4])
            forced[1, z, at, :] = act * (conc * f[1] - mass * f[5])
            forced[2, z, at, :] = f[2]
            forced[3, z, at, :] = f[3]

    tail = FRONT + height
    for z in range(3):
        for k in range(2):
            speed[k, z, tail : tail + 8, :] = blank
        for k in range(3):
            state[k, z, 0:8, :] = blank

    lane = lanes(8)
    ends_at = [lane == k for k in (BX - 1, BX // 2 - 1, 0, BX // 2)]
    at127, at63, at0, at64 = ends_at

    def rows_of(r):
        row = 8 * r
        return pl.ds(row, 8), pl.ds(row + FRONT, 8), pl.ds(row + FRONT + 1, 8), pl.ds(row + FRONT - 1, 8)

    def stresses(r):
        at, to, up1, _ = rows_of(r)
        u = [speed[0, z, to, :] for z in range(3)]
        v = [speed[1, z, to, :] for z in range(3)]

        def north(k, x):
            return x[1], speed[k, 0, up1, :], roll(jnp.where(mid, x[2], speed[k, 2, up1, :]), BX // 2)

        un, vn = north(0, u), north(1, v)
        ue = east_of(*u, at127, at63)
        ve = east_of(*v, at127, at63)
        for z in range(3):
            sxx = ue[z] - u[z]
            syy = vn[z] - v[z]
            shear = (un[z] - u[z]) + (ve[z] - v[z])
            div, ten = sxx + syy, sxx - syy
            twice = div + div
            inv = lax.rsqrt(twice * twice + (ten * ten + shear * shear) + 1.0)
            hard = still[0, z, at, :]
            kr = hard * inv
            half = 0.5 * kr
            state[0, z, to, :] = (state[0, z, to, :] * (2.0 / 3.0) - hard) + kr * twice
            state[1, z, to, :] = state[1, z, to, :] * (2.0 / 3.0) + half * ten
            state[2, z, to, :] = state[2, z, to, :] * (2.0 / 3.0) + half * shear

    def speeds(r):
        at, to, _, down1 = rows_of(r)
        s1, s2, s12 = [[state[k, z, to, :] for z in range(3)] for k in range(3)]
        a = [x + y for x, y in zip(s1, s2)]
        c = [x - y for x, y in zip(s1, s2)]
        aw = west_of(*a, at0, at64)
        sw = west_of(*s12, at0, at64)

        def south(x, lower):
            return lower(1), x[0], roll(jnp.where(mid, lower(2), x[2]), BX // 2)

        ss = south(s12, lambda z: state[2, z, down1, :])
        cs = south(c, lambda z: state[0, z, down1, :] - state[1, z, down1, :])
        for z in range(3):
            u, v = speed[0, z, to, :], speed[1, z, to, :]
            fx = (a[z] - aw[z]) + (s12[z] - ss[z])
            fy = (s12[z] - sw[z]) + (c[z] - cs[z])
            m2, base = still[1, z, at, :], still[2, z, at, :]
            cx, cy = forced[2, z, at, :], forced[3, z, at, :]
            dx, dy = cx - u, cy - v
            y2 = dx * dx + dy * dy + DRAG_FLOOR
            drag = base * (y2 * lax.rsqrt(y2))
            part = still[3, z, at, :] * (1.0 / (jnp.maximum(m2, 1.0) + drag))
            mc = (0.5 * CORIO) * m2
            speed[0, z, to, :] = part * (m2 * u + fx + forced[0, z, at, :] + drag * cx + mc * v)
            speed[1, z, to, :] = part * (m2 * v + fy + forced[1, z, at, :] + drag * cy - mc * u)

    def subcycle(_, carry):
        for r in range(tiles):
            stresses(r)
        for r in range(tiles):
            speeds(r)
        return carry

    lax.fori_loop(0, NSUB, subcycle, 0)

    for r in range(tiles):
        at = slice(8 * r, 8 * r + 8)
        to = slice(FRONT + 8 * r, FRONT + 8 * r + 8)
        for y in range(2):
            base = still[2, y, at, :]
            dx = speed[0, y, to, :] - forced[2, y, at, :]
            dy = speed[1, y, to, :] - forced[3, y, at, :]
            y2 = dx * dx + dy * dy + DRAG_FLOOR
            factor = base * (y2 * lax.rsqrt(y2))
            for k, x in enumerate((factor * dx, factor * dy, base * (1.0 / CW))):
                out8[pl.ds(8 * r * REPLY + 2 * k + y, 8, stride=REPLY), :] = x
    for y in range(2):
        for k in range(2):
            moved[k, :, y * BX : (y + 1) * BX] = speed[k, y, FRONT + 2 : FRONT + 2 + count, :]

    def answer(o, _):
        for j in range(per):
            b = (ids[o, j] + 2) * REPLY
            back[o, 6 * j : 6 * j + 6, :] = out8[pl.ds(b, 6), :]
        return 0

    lax.fori_loop(0, n, answer, 0)


def ice_step(ids, recv, begin, fixed, below, above):
    n, per = ids.shape[0], ids.shape[1] // 3
    count = n * per
    height = (count + 4 + 7) // 8 * 8
    tall = height + 2 * FRONT
    scratch = [
        (height * STEP + 8, BX), (height, BX), (height, BX),
        (2, 3, tall, BX), (3, 3, tall, BX), (4, 3, height, BX), (height * REPLY + 8, BX), (5, 3, height, BX),
    ]
    return pl.pallas_call(
        functools.partial(ice_kernel, n, per, count),
        out_shape=[f32(n, 6 * per, BX), f32(2, count, 2 * BX)],
        in_specs=[SMEM] + [VMEM] * 5,
        out_specs=[VMEM] * 2,
        scratch_shapes=[pltpu.VMEM(s, jnp.float32) for s in scratch],
        compiler_params=params(16),
        name="ice_step",
    )(ids, recv, begin, fixed, below, above)


def final_kernel(n, per, got, opened, moved, out):
    is_ocean = lax.axis_index("comp") == 0

    @pl.when(is_ocean)
    def _():
        def tile(t, _):
            for y in range(2):
                cells = slice(y * BX, (y + 1) * BX)
                gx, gy, gc = [got[t, pl.ds(2 * k + y, per, stride=6), :] for k in range(3)]
                out[0, t, :, cells] = gx + (1.0 - gc) * opened[t, 2 * y]
                out[1, t, :, cells] = gy + (1.0 - gc) * opened[t, 2 * y + 1]
            return 0

        lax.fori_loop(0, n, tile, 0)

    @pl.when(jnp.logical_not(is_ocean))
    def _():
        out[...] = moved[...]


def final(got, opened, moved):
    n, _, per, _ = opened.shape
    return pl.pallas_call(
        functools.partial(final_kernel, n, per),
        out_shape=f32(2, n, per, 2 * BX),
        in_specs=[VMEM] * 3,
        out_specs=VMEM,
        compiler_params=params(8),
        name="final",
    )(got, opened, moved)


def per_device(fields, block_owner, ice_covered, land_mask):
    nlat, nlon = lax.axis_size("lat"), lax.axis_size("lon")
    n = nlat * nlon
    count = block_owner.shape[0]
    per = count // n
    side = lax.axis_index("comp")
    fields = fields[0]
    split = fields.reshape(7, n, per, 2 * BX)
    owner = block_owner.reshape(1, count)
    other = lax.ppermute(split, "comp", [(0, 1), (1, 0)])
    opened = open_stress(split)
    def everyone(x):
        return lax.all_to_all(x, ("lat", "lon"), split_axis=0, concat_axis=0, tiled=True)

    height = (count + 4 + 7) // 8 * 8

    def ice_side(other, fields, covered, land, owner):
        recv = everyone(pack(other, owner, nlat, nlon))
        active, ends = ice_ends(fields, covered, land)
        ring = [(i, (i + 1) % nlon) for i in range(nlon)]
        west = lax.ppermute(ends, "lon", ring)
        east = lax.ppermute(ends, "lon", [(j, i) for i, j in ring])
        sides, north, south = ice_rows(fields, active, west, east)
        line = [(i, i + 1) for i in range(nlat - 1)]
        below = lax.ppermute(north, "lat", line)
        above = lax.ppermute(south, "lat", [(j, i) for i, j in line])
        begin, fixed = prep(fields, active, sides)
        return recv, jnp.zeros((n, 3 * per), jnp.int32), below, above, begin, fixed

    def ocean_side(other, fields, covered, land, owner):
        row = jnp.zeros((34, BX), jnp.float32)
        blank = jnp.zeros((5, 3, height, BX), jnp.float32)
        return jnp.zeros((n, 13 * per + 40, BX), jnp.float32), everyone(table(owner, nlat, nlon)), row, row, blank, blank

    recv, owned, below, above, begin, fixed = lax.cond(
        side == 1, ice_side, ocean_side, other, fields, ice_covered.reshape(1, count), land_mask, owner
    )
    swap = lax.ppermute(owned, "comp", [(0, 1), (1, 0)])
    recv, below, above = fetch(recv, below, above)
    back, moved = ice_step(swap, recv, begin, fixed, below, above)
    back = lax.cond(side == 1, everyone, lambda x: x, back)
    got = lax.ppermute(back, "comp", [(0, 1), (1, 0)])
    out = final(got, opened, moved.reshape(2, n, per, 2 * BX))
    return out.reshape(1, 2, count, 2 * BX)


def solution(mesh):
    placed = (
        P("comp", None, ("lat", "lon"), None),
        P(("lat", "lon")),
        P(("lat", "lon")),
        P(("lat", "lon"), None),
    )
    return jax.shard_map(
        per_device,
        mesh=mesh,
        in_specs=placed,
        out_specs=P("comp", None, ("lat", "lon"), None),
        check_vma=False,
    )
```

```python
import functools

import jax
import jax.numpy as jnp
from jax import lax
from jax.experimental import pallas as pl
from jax.experimental.pallas import tpu as pltpu
from jax.sharding import PartitionSpec as P

BX = 128
NSUB = 4
FRONT = 8
STEP = 13
REPLY = 5

CD_ICE = 0.1
CW = 1.5
CSTAR = 2.0
CORIO = 0.3
DRAG_FLOOR = 0.1

VMEM = pl.BlockSpec(memory_space=pltpu.VMEM)
SMEM = pl.BlockSpec(memory_space=pltpu.SMEM)


def params(mib):
    return pltpu.CompilerParams(vmem_limit_bytes=mib * 1024 * 1024)


def f32(*shape):
    return jax.ShapeDtypeStruct(shape, jnp.float32)


def lanes(rows):
    return lax.broadcasted_iota(jnp.int32, (rows, BX), 1)


def roll(x, by):
    return pltpu.roll(x, by % BX, 1)


def at_end(q, west, east):
    return jnp.where(q, west, east)


def column(row):
    parts = []
    for lo in range(0, row.shape[1], BX):
        diag = lax.broadcasted_iota(jnp.int32, (BX, BX), 0) == lanes(BX)
        parts.append(jnp.sum(jnp.where(diag, row[:, lo : lo + BX].astype(jnp.float32), 0.0), axis=1, keepdims=True))
    return jnp.concatenate(parts, 0) if len(parts) > 1 else parts[0]


def steps(lo, hi, body):
    if hi - lo <= 32:
        for k in range(lo, hi):
            body(k, 0)
    else:
        lax.fori_loop(lo, hi, body, 0)


def pack_kernel(nlat, nlon, per, raw, owner, out, pay, edge, rim, sems):
    n = nlat * nlon
    count = n * per
    cut = 12 * per if (12 * per) % 8 == 0 else 0

    def send(d, k):
        at = pl.ds(0, cut) if k == 0 else pl.ds(cut, 13 * per + 40 - cut)
        return pltpu.make_async_copy(pay.at[d, at], out.at[d, at], sems.at[k, d])

    lane = lanes(per)
    group = lane // 8
    slot = lax.broadcasted_iota(jnp.int32, (per, BX), 0)
    lat_base = 13 * per

    def tile(t, _):
        def half(ch, y):
            return raw[ch, t, :, y * BX : (y + 1) * BX]

        planes = [None] * 12
        for y in range(2):
            wx, wy, rho = half(0, y), half(1, y), half(6, y)
            scale = rho * CD_ICE * jnp.sqrt(wx * wx + wy * wy + 1.0)
            planes[y] = scale * wx
            planes[2 + y] = scale * wy
            for ch in range(2, 6):
                planes[2 * ch + y] = half(ch, y)
        ends = jnp.zeros((per, BX), jnp.float32)
        for p in range(12):
            pay[t, pl.ds(p, per, stride=12), :] = planes[p]
            ends = jnp.where(group == p, roll(planes[p], 8 * p + 4), ends)
        edge[t] = ends
        ids = jnp.zeros((per, BX), jnp.int32)
        for j in range(per):
            ids = jnp.where(slot == j, owner[0, t * per + j] - t * count, ids)

        def pick(block, value):
            return jnp.sum(jnp.where(ids == block, value, 0.0), axis=0, keepdims=True)

        rows = [pick(0, x) for x in planes] + [pick(1, x) for x in planes[0::2]]
        rows += [pick(count - 1, x) for x in planes]
        rows += [pick(count - 2, x) for x in planes[1::2]]
        rows += [pick(b, ends) for b in (0, 1, count - 1, count - 2)]
        for k, row in enumerate(rows):
            rim[t, k : k + 1, :] = row
        if cut:
            send(t, 0).start()
        return 0

    steps(0, n, tile)

    def dest(d, _):
        i, j = d // nlon, d % nlon
        jw, je = (j + nlon - 1) % nlon, (j + 1) % nlon
        q8 = (lane % 8) < 4
        pay[d, 12 * per : 13 * per, :] = at_end(q8, edge[i * nlon + jw], edge[i * nlon + je])
        for ii, ok, lo, c in (
            (jnp.minimum(i + 1, nlat - 1), i + 1 < nlat, 0, 36),
            (jnp.maximum(i - 1, 0), i > 0, 18, 38),
        ):
            scale = jnp.where(ok, 1.0, 0.0)
            pay[d, lat_base + lo : lat_base + lo + 18, :] = rim[ii * nlon + j, lo : lo + 18, :] * scale
            q2 = (lanes(2) % 8) < 4
            corner = at_end(q2, rim[ii * nlon + jw, c : c + 2, :], rim[ii * nlon + je, c : c + 2, :])
            pay[d, lat_base + c : lat_base + c + 2, :] = corner * scale
        send(d, 1).start()
        return 0

    def finish(d, _):
        if cut:
            send(d, 0).wait()
        send(d, 1).wait()
        return 0

    steps(0, n, dest)
    steps(0, n, finish)


def ends_kernel(ice, covered, land, active, ends):
    count = covered.shape[1]
    lane = lanes(count)
    group = lane // 8
    total = jnp.zeros((count, BX), jnp.float32)
    cover = column(covered[...])
    for y in range(2):
        cells = slice(y * BX, (y + 1) * BX)
        act = cover * (1 - land[:, cells]).astype(jnp.float32)
        active[:, cells] = act
        for ch in range(8):
            x = act if ch == 7 else ice[ch, :, cells]
            p = 2 * ch + y
            total = jnp.where(group == p, roll(x, 8 * p + 4), total)
    ends[...] = total


def pack(raw, owner, nlat, nlon):
    _, n, per, _ = raw.shape
    rows = 13 * per + 40
    return pl.pallas_call(
        functools.partial(pack_kernel, nlat, nlon, per),
        out_shape=f32(n, rows, BX),
        in_specs=[VMEM, SMEM],
        out_specs=pl.BlockSpec(memory_space=pl.ANY),
        scratch_shapes=[
            pltpu.VMEM((n, rows, BX), jnp.float32),
            pltpu.VMEM((n, per, BX), jnp.float32),
            pltpu.VMEM((n, 40, BX), jnp.float32),
            pltpu.SemaphoreType.DMA((2, n)),
        ],
        compiler_params=params(24),
        name="pack",
    )(raw, owner)


def open_kernel(n, per, raw, opened):
    @pl.when(lax.axis_index("comp") == 0)
    def _():
        def tile(t, _):
            for y in range(2):
                wx, wy, cx, cy, rho = [raw[ch, t, :, y * BX : (y + 1) * BX] for ch in (0, 1, 2, 3, 6)]
                rx, ry = wx - cx, wy - cy
                speed = jnp.sqrt(rx * rx + ry * ry + 1.0)
                rate = rho * (0.1 + 0.05 * speed) * speed
                opened[t, 2 * y] = rate * rx
                opened[t, 2 * y + 1] = rate * ry
                opened[t, 4 + 2 * y] = cx
                opened[t, 5 + 2 * y] = cy
            return 0

        steps(0, n, tile)


def open_stress(raw):
    _, n, per, _ = raw.shape
    return pl.pallas_call(
        functools.partial(open_kernel, n, per),
        out_shape=f32(n, 8, per, BX),
        in_specs=[VMEM],
        out_specs=VMEM,
        compiler_params=params(24),
        name="open_stress",
    )(raw)


def ice_ends(ice, covered, land):
    count = land.shape[0]
    return pl.pallas_call(
        ends_kernel,
        out_shape=[f32(count, 2 * BX), f32(count, BX)],
        in_specs=[VMEM] * 3,
        out_specs=[VMEM] * 2,
        compiler_params=params(8),
        name="ice_ends",
    )(ice, covered, land)


def table_kernel(nlat, nlon, per, owner, ids):
    def tile(t, _):
        i, j = t // nlon, t % nlon
        near = [t, i * nlon + (j + nlon - 1) % nlon, i * nlon + (j + 1) % nlon]
        for k, other in enumerate(near):
            for slot in range(per):
                ids[t, k * per + slot] = owner[0, other * per + slot] - other * (nlat * nlon * per)
        return 0

    steps(0, nlat * nlon, tile)


def table(owner, nlat, nlon):
    n = nlat * nlon
    per = owner.shape[1] // n
    return pl.pallas_call(
        functools.partial(table_kernel, nlat, nlon, per),
        out_shape=jax.ShapeDtypeStruct((n, 3 * per), jnp.int32),
        in_specs=[SMEM],
        out_specs=SMEM,
        compiler_params=params(4),
        name="table",
    )(owner)


def rows_kernel(ice, active, west, east, sides, north, south):
    count = active.shape[0]
    q = (lanes(count) % 8) < 4
    sides[...] = jnp.where(q, west[...], east[...])
    for out, lo in ((north, count - 2), (south, 0)):
        for y in range(2):
            cells = slice(y * BX, (y + 1) * BX)
            for ch in range(8):
                p = 2 * ch + y
                x = active[lo : lo + 2, cells] if ch == 7 else ice[ch, lo : lo + 2, cells]
                out[2 * p : 2 * p + 2, :] = x
        out[32:34, :] = sides[lo : lo + 2, :]


def ice_rows(ice, active, west, east):
    count = active.shape[0]
    return pl.pallas_call(
        rows_kernel,
        out_shape=[f32(count, BX), f32(34, BX), f32(34, BX)],
        in_specs=[VMEM] * 4,
        out_specs=[VMEM] * 3,
        compiler_params=params(8),
        name="ice_rows",
    )(ice, active, west, east)


def middle(rows):
    lane = lanes(rows)
    return (lane >= BX // 4) & (lane < 3 * BX // 4)


def side_plane(ends, ch, mid):
    odd = roll(ends, BX // 2 - (8 * (2 * ch + 1) + 4))
    return jnp.where(mid, odd, roll(ends, -(16 * ch + 4)))


def statics(mass, conc, act):
    return mass * jnp.exp(CSTAR * (conc - 1.0)) * act * (1.0 / 6.0), 2.0 * mass, act, conc


def prep_kernel(count, height, ice, active, sides, begin, still, unused, grid):
    mid = middle(count)
    for ch in range(8):
        for y in range(2):
            cells = slice(y * BX, (y + 1) * BX)
            grid[ch, y, 2 : 2 + count, :] = active[:, cells] if ch == 7 else ice[ch, :, cells]
        grid[ch, 2, 2 : 2 + count, :] = side_plane(sides[...], ch, mid)
        for z in range(3):
            grid[ch, z, 0:2, :] = jnp.zeros((2, BX), jnp.float32)
            grid[ch, z, count + 2 :, :] = jnp.zeros((height - count - 2, BX), jnp.float32)

    for r in range(height // 8):
        at = slice(8 * r, 8 * r + 8)
        for z in range(3):
            u, v, mass, conc, s1, s2, s12, act = [grid[ch, z, at, :] for ch in range(8)]
            for k, x in enumerate((u, v, 0.5 * s1, 0.5 * s2, s12)):
                begin[k, z, at, :] = x
            for k, x in enumerate(statics(mass, conc, act)):
                still[k, z, at, :] = x


def prep(ice, active, sides, spare):
    count = active.shape[0]
    height = (count + 4 + 7) // 8 * 8
    return pl.pallas_call(
        functools.partial(prep_kernel, count, height),
        out_shape=[f32(5, 3, height, BX), f32(4, 3, height, BX), f32(*spare)],
        in_specs=[VMEM] * 3,
        out_specs=[VMEM] * 3,
        scratch_shapes=[pltpu.VMEM((8, 3, height, BX), jnp.float32)],
        compiler_params=params(12),
        name="prep",
    )(ice, active, sides)


def fetch_kernel(*refs):
    k = len(refs) // 2
    copies = [pltpu.make_async_copy(refs[i], refs[k + i], refs[-1].at[i]) for i in range(k)]
    for copy in copies:
        copy.start()
    for copy in copies:
        copy.wait()


def fetch(*arrays):
    return pl.pallas_call(
        fetch_kernel,
        out_shape=[f32(*x.shape) for x in arrays],
        in_specs=[pl.BlockSpec(memory_space=pl.ANY)] * len(arrays),
        out_specs=[VMEM] * len(arrays),
        scratch_shapes=[pltpu.SemaphoreType.DMA((len(arrays),))],
        compiler_params=params(4),
        name="fetch",
    )(*arrays)


def east_of(even, odd, side, at127, at63):
    e, o, s = roll(even, -1), roll(odd, -1), roll(side, -1)
    wide = jnp.where(at127, e, jnp.where(at63, roll(odd, 63), s))
    return jnp.where(at127, s, e), jnp.where(at127, roll(side, 63), o), wide


def west_of(even, odd, side, at0, at64):
    e, o, s = roll(even, 1), roll(odd, 1), roll(side, 1)
    wide = jnp.where(at0, e, jnp.where(at64, roll(odd, 65), s))
    return jnp.where(at0, s, e), jnp.where(at0, roll(side, -63), o), wide


def ice_kernel(n, per, count, ids, recv, begin, fixed, below, above, back, moved, unused,
               spot, hw, he, speed, state, forced, out8, still):
    tiles = (count + 4 + 7) // 8
    height = tiles * 8
    blank = jnp.zeros((8, BX), jnp.float32)
    for k in (0, 8):
        spot[k : k + 8, :] = blank
    for k in range((count + 3) * STEP, height * STEP, 8):
        spot[k : k + 8, :] = blank
    for k in (0, height - 8):
        hw[k : k + 8, :] = blank
        he[k : k + 8, :] = blank

    def place(o, acc):
        for j in range(per):
            b = (ids[o, j] + 2) * STEP
            spot[pl.ds(b, 12), :] = recv[o, 12 * j : 12 * j + 12, :]
            row = recv[o, 12 * per + j : 12 * per + j + 1, :]
            hw[pl.ds(ids[o, per + j] + 2, 1), :] = row
            he[pl.ds(ids[o, 2 * per + j] + 2, 1), :] = row
        return acc + recv[o, 13 * per : 13 * per + 40, :]

    rim = lax.fori_loop(0, n, place, jnp.zeros((40, BX), jnp.float32))
    up, down = (count + 2) * STEP, STEP
    spot[up : up + 12, :] = rim[0:12]
    spot[down : down + 12, :] = rim[18:30]
    for ch in range(6):
        k = up + STEP + 2 * ch
        spot[k : k + 1, :] = rim[12 + ch : 13 + ch]
        k = 2 * ch + 1
        spot[k : k + 1, :] = rim[30 + ch : 31 + ch]
    for ref in (hw, he):
        ref[count + 2 : count + 4, :] = rim[36:38]
        ref[1:2, :] = rim[38:39]
        ref[0:1, :] = rim[39:40]

    q, mid, mid2 = (lanes(8) % 8) < 4, middle(8), middle(2)
    for r in range(tiles):
        at = slice(8 * r, 8 * r + 8)
        to = slice(FRONT + 8 * r, FRONT + 8 * r + 8)
        for z in range(3):
            for k in range(2):
                speed[k, z, to, :] = begin[k, z, at, :]
            for k in range(3):
                state[k, z, to, :] = begin[2 + k, z, at, :]
            hard, m2, act, conc = [fixed[k, z, at, :] for k in range(4)]
            for k, x in enumerate((hard, m2, CW * conc * act, act, conc)):
                still[k, z, at, :] = x
    for lo, msg in ((0, below), (count + 2, above)):
        at, to = slice(lo, lo + 2), slice(FRONT + lo, FRONT + lo + 2)
        for z in range(3):
            if z < 2:
                raw = [msg[4 * ch + 2 * z : 4 * ch + 2 * z + 2, :] for ch in range(8)]
            else:
                raw = [side_plane(msg[32:34, :], ch, mid2) for ch in range(8)]
            u, v, mass, conc, s1, s2, s12, act = raw
            speed[0, z, to, :] = u
            speed[1, z, to, :] = v
            state[0, z, to, :] = 0.5 * s1
            state[1, z, to, :] = 0.5 * s2
            state[2, z, to, :] = s12
            hard, m2, act, conc = statics(mass, conc, act)
            for k, x in enumerate((hard, m2, CW * conc * act, act, conc)):
                still[k, z, at, :] = x

    for r in range(tiles):
        at = slice(8 * r, 8 * r + 8)
        ends = jnp.where(q, hw[at, :], he[at, :])
        for z in range(3):
            if z < 2:
                f = [spot[pl.ds(8 * r * STEP + 2 * ch + z, 8, stride=STEP), :] for ch in range(6)]
            else:
                f = [side_plane(ends, ch, mid) for ch in range(6)]
            mass, act, conc = [still[k, z, at, :] for k in (1, 3, 4)]
            mass = 0.5 * mass
            forced[0, z, at, :] = act * (conc * f[0] - mass * f[4])
            forced[1, z, at, :] = act * (conc * f[1] - mass * f[5])
            forced[2, z, at, :] = f[2]
            forced[3, z, at, :] = f[3]

    tail = FRONT + height
    for z in range(3):
        for k in range(2):
            speed[k, z, tail : tail + 8, :] = blank
        for k in range(3):
            state[k, z, 0:8, :] = blank

    lane = lanes(8)
    ends_at = [lane == k for k in (BX - 1, BX // 2 - 1, 0, BX // 2)]
    at127, at63, at0, at64 = ends_at

    def rows_of(r):
        row = 8 * r
        return pl.ds(row, 8), pl.ds(row + FRONT, 8), pl.ds(row + FRONT + 1, 8), pl.ds(row + FRONT - 1, 8)

    def stresses(r):
        at, to, up1, _ = rows_of(r)
        u = [speed[0, z, to, :] for z in range(3)]
        v = [speed[1, z, to, :] for z in range(3)]

        def north(k, x):
            return x[1], speed[k, 0, up1, :], roll(jnp.where(mid, x[2], speed[k, 2, up1, :]), BX // 2)

        un, vn = north(0, u), north(1, v)
        ue = east_of(*u, at127, at63)
        ve = east_of(*v, at127, at63)
        for z in range(3):
            sxx = ue[z] - u[z]
            syy = vn[z] - v[z]
            shear = (un[z] - u[z]) + (ve[z] - v[z])
            div, ten = sxx + syy, sxx - syy
            twice = div + div
            inv = lax.rsqrt(twice * twice + (ten * ten + shear * shear) + 1.0)
            hard = still[0, z, at, :]
            kr = hard * inv
            half = 0.5 * kr
            state[0, z, to, :] = (state[0, z, to, :] * (2.0 / 3.0) - hard) + kr * twice
            state[1, z, to, :] = state[1, z, to, :] * (2.0 / 3.0) + half * ten
            state[2, z, to, :] = state[2, z, to, :] * (2.0 / 3.0) + half * shear

    def speeds(r):
        at, to, _, down1 = rows_of(r)
        s1, s2, s12 = [[state[k, z, to, :] for z in range(3)] for k in range(3)]
        a = [x + y for x, y in zip(s1, s2)]
        c = [x - y for x, y in zip(s1, s2)]
        aw = west_of(*a, at0, at64)
        sw = west_of(*s12, at0, at64)

        def south(x, lower):
            return lower(1), x[0], roll(jnp.where(mid, lower(2), x[2]), BX // 2)

        ss = south(s12, lambda z: state[2, z, down1, :])
        cs = south(c, lambda z: state[0, z, down1, :] - state[1, z, down1, :])
        for z in range(3):
            u, v = speed[0, z, to, :], speed[1, z, to, :]
            fx = (a[z] - aw[z]) + (s12[z] - ss[z])
            fy = (s12[z] - sw[z]) + (c[z] - cs[z])
            m2, base = still[1, z, at, :], still[2, z, at, :]
            cx, cy = forced[2, z, at, :], forced[3, z, at, :]
            dx, dy = cx - u, cy - v
            y2 = dx * dx + dy * dy + DRAG_FLOOR
            drag = base * (y2 * lax.rsqrt(y2))
            part = still[3, z, at, :] * (1.0 / (jnp.maximum(m2, 1.0) + drag))
            mc = (0.5 * CORIO) * m2
            speed[0, z, to, :] = part * (m2 * u + fx + forced[0, z, at, :] + drag * cx + mc * v)
            speed[1, z, to, :] = part * (m2 * v + fy + forced[1, z, at, :] + drag * cy - mc * u)

    def subcycle(_, carry):
        for r in range(tiles):
            stresses(r)
        for r in range(tiles):
            speeds(r)
        return carry

    lax.fori_loop(0, NSUB, subcycle, 0)

    for r in range(tiles):
        to = slice(FRONT + 8 * r, FRONT + 8 * r + 8)
        for y in range(2):
            for k in range(2):
                out8[pl.ds(8 * r * REPLY + 2 * k + y, 8, stride=REPLY), :] = speed[k, y, to, :]
    for y in range(2):
        for k in range(2):
            moved[k, :, y * BX : (y + 1) * BX] = speed[k, y, FRONT + 2 : FRONT + 2 + count, :]

    def answer(o, _):
        for j in range(per):
            b = (ids[o, j] + 2) * REPLY
            back[o, 4 * j : 4 * j + 4, :] = out8[pl.ds(b, 4), :]
        return 0

    lax.fori_loop(0, n, answer, 0)


def ice_step(ids, recv, begin, fixed, below, above):
    n, per = ids.shape[0], ids.shape[1] // 3
    count = n * per
    height = (count + 4 + 7) // 8 * 8
    tall = height + 2 * FRONT
    scratch = [
        (height * STEP + 8, BX), (height, BX), (height, BX),
        (2, 3, tall, BX), (3, 3, tall, BX), (4, 3, height, BX), (height * REPLY + 8, BX), (5, 3, height, BX),
    ]
    return pl.pallas_call(
        functools.partial(ice_kernel, n, per, count),
        out_shape=[f32(n, 4 * per, BX), f32(2, count, 2 * BX), f32(n, 2 * per, BX)],
        in_specs=[SMEM] + [VMEM] * 5,
        out_specs=[VMEM] * 3,
        scratch_shapes=[pltpu.VMEM(s, jnp.float32) for s in scratch],
        compiler_params=params(16),
        name="ice_step",
    )(ids, recv, begin, fixed, below, above)


def cover_kernel(n, per, ids, conc, covered, land, out, spot):
    count = n * per
    cover = column(covered[...])
    for y in range(2):
        cells = slice(y * BX, (y + 1) * BX)
        act = cover * (1 - land[:, cells]).astype(jnp.float32)
        spot[pl.ds(y, count, stride=2), :] = conc[:, cells] * act

    def tile(o, _):
        for j in range(per):
            out[o, 2 * j : 2 * j + 2, :] = spot[pl.ds(2 * ids[o, j], 2), :]
        return 0

    lax.fori_loop(0, n, tile, 0)


def slot_cover(ids, conc, covered, land):
    n, per = ids.shape[0], ids.shape[1] // 3
    count = n * per
    return pl.pallas_call(
        functools.partial(cover_kernel, n, per),
        out_shape=f32(n, 2 * per, BX),
        in_specs=[SMEM] + [VMEM] * 3,
        out_specs=VMEM,
        scratch_shapes=[pltpu.VMEM((2 * count, BX), jnp.float32)],
        compiler_params=params(8),
        name="slot_cover",
    )(ids, conc, covered, land)


def final_kernel(n, per, got, cover, opened, moved, out):
    is_ocean = lax.axis_index("comp") == 0

    @pl.when(is_ocean)
    def _():
        def tile(t, _):
            for y in range(2):
                cells = slice(y * BX, (y + 1) * BX)
                u, v = [got[t, pl.ds(2 * k + y, per, stride=4), :] for k in range(2)]
                part = cover[t, pl.ds(y, per, stride=2), :]
                dx, dy = u - opened[t, 4 + 2 * y], v - opened[t, 5 + 2 * y]
                factor = (CW * part) * jnp.sqrt(dx * dx + dy * dy + DRAG_FLOOR)
                rest = 1.0 - part
                out[0, t, :, cells] = factor * dx + rest * opened[t, 2 * y]
                out[1, t, :, cells] = factor * dy + rest * opened[t, 2 * y + 1]
            return 0

        steps(0, n, tile)

    @pl.when(jnp.logical_not(is_ocean))
    def _():
        out[...] = moved[...]


def final(got, cover, opened, moved):
    n, _, per, _ = opened.shape
    return pl.pallas_call(
        functools.partial(final_kernel, n, per),
        out_shape=f32(2, n, per, 2 * BX),
        in_specs=[VMEM] * 4,
        out_specs=VMEM,
        compiler_params=params(12),
        name="final",
    )(got, cover, opened, moved)


def per_device(fields, block_owner, ice_covered, land_mask):
    nlat, nlon = lax.axis_size("lat"), lax.axis_size("lon")
    n = nlat * nlon
    count = block_owner.shape[0]
    per = count // n
    side = lax.axis_index("comp")
    fields = fields[0]
    split = fields.reshape(7, n, per, 2 * BX)
    owner = block_owner.reshape(1, count)
    other = lax.ppermute(split, "comp", [(0, 1), (1, 0)])
    opened = open_stress(split)
    def everyone(x):
        return lax.all_to_all(x, ("lat", "lon"), split_axis=0, concat_axis=0, tiled=True)

    height = (count + 4 + 7) // 8 * 8

    def ice_side(other, fields, covered, land, owner):
        recv = everyone(pack(other, owner, nlat, nlon))
        active, ends = ice_ends(fields, covered, land)
        ring = [(i, (i + 1) % nlon) for i in range(nlon)]
        west = lax.ppermute(ends, "lon", ring)
        east = lax.ppermute(ends, "lon", [(j, i) for i, j in ring])
        sides, north, south = ice_rows(fields, active, west, east)
        line = [(i, i + 1) for i in range(nlat - 1)]
        below = lax.ppermute(north, "lat", line)
        above = lax.ppermute(south, "lat", [(j, i) for i, j in line])
        begin, fixed, mine = prep(fields, active, sides, (n, 2 * per, BX))
        return recv, jnp.zeros((n, 3 * per), jnp.int32), below, above, begin, fixed, mine

    def ocean_side(other, fields, covered, land, owner):
        row = jnp.zeros((34, BX), jnp.float32)
        blank = jnp.zeros((5, 3, height, BX), jnp.float32)
        owned = everyone(table(owner, nlat, nlon))
        mine = slot_cover(owned, other.reshape(7, count, 2 * BX)[3], covered, land)
        return jnp.zeros((n, 13 * per + 40, BX), jnp.float32), owned, row, row, blank, blank[:4], mine

    recv, owned, below, above, begin, fixed, mine = lax.cond(
        side == 1, ice_side, ocean_side, other, fields, ice_covered.reshape(1, count), land_mask, owner
    )
    swap = lax.ppermute(owned, "comp", [(0, 1), (1, 0)])
    recv, below, above = fetch(recv, below, above)

    def ice_work(ids, recv, begin, fixed, below, above, mine):
        return ice_step(ids, recv, begin, fixed, below, above)

    def ocean_work(ids, recv, begin, fixed, below, above, mine):
        return jnp.zeros((n, 4 * per, BX), jnp.float32), jnp.zeros((2, count, 2 * BX), jnp.float32), everyone(mine)

    back, moved, cover = lax.cond(
        side == 1, ice_work, ocean_work, swap, recv, begin, fixed, below, above, mine
    )
    back = lax.cond(side == 1, everyone, lambda x: x, back)
    got = lax.ppermute(back, "comp", [(0, 1), (1, 0)])
    out = final(got, cover, opened, moved.reshape(2, n, per, 2 * BX))
    return out.reshape(1, 2, count, 2 * BX)


def solution(mesh):
    placed = (
        P("comp", None, ("lat", "lon"), None),
        P(("lat", "lon")),
        P(("lat", "lon")),
        P(("lat", "lon"), None),
    )
    return jax.shard_map(
        per_device,
        mesh=mesh,
        in_specs=placed,
        out_specs=P("comp", None, ("lat", "lon"), None),
        check_vma=False,
    )
```

```python
import functools

import jax
import jax.numpy as jnp
from jax import lax
from jax.experimental import pallas as pl
from jax.experimental.pallas import tpu as pltpu
from jax.sharding import PartitionSpec as P

BX = 128
NSUB = 4
FRONT = 8
STEP = 13
REPLY = 5

CD_ICE = 0.1
CW = 1.5
CSTAR = 2.0
CORIO = 0.3
DRAG_FLOOR = 0.1

VMEM = pl.BlockSpec(memory_space=pltpu.VMEM)
SMEM = pl.BlockSpec(memory_space=pltpu.SMEM)


def params(mib):
    return pltpu.CompilerParams(vmem_limit_bytes=mib * 1024 * 1024)


def f32(*shape):
    return jax.ShapeDtypeStruct(shape, jnp.float32)


def lanes(rows):
    return lax.broadcasted_iota(jnp.int32, (rows, BX), 1)


def roll(x, by):
    return pltpu.roll(x, by % BX, 1)


def at_end(q, west, east):
    return jnp.where(q, west, east)


def column(row):
    parts = []
    for lo in range(0, row.shape[1], BX):
        diag = lax.broadcasted_iota(jnp.int32, (BX, BX), 0) == lanes(BX)
        parts.append(jnp.sum(jnp.where(diag, row[:, lo : lo + BX].astype(jnp.float32), 0.0), axis=1, keepdims=True))
    return jnp.concatenate(parts, 0) if len(parts) > 1 else parts[0]


def steps(lo, hi, body):
    if hi - lo <= 32:
        for k in range(lo, hi):
            body(k, 0)
    else:
        lax.fori_loop(lo, hi, body, 0)


def pack_kernel(nlat, nlon, per, raw, owner_in, out, pay, edge, rim, owner, sems, ready):
    n = nlat * nlon
    count = n * per
    cut = 12 * per if (12 * per) % 8 == 0 else 0

    def send(d, k):
        at = pl.ds(0, cut) if k == 0 else pl.ds(cut, 13 * per + 40 - cut)
        return pltpu.make_async_copy(pay.at[d, at], out.at[d, at], sems.at[k, d])

    fetched = pltpu.make_async_copy(owner_in, owner, ready)
    fetched.start()
    lane = lanes(per)
    group = lane // 8
    slot = lax.broadcasted_iota(jnp.int32, (per, BX), 0)
    lat_base = 13 * per

    def tile(t, _):
        def half(ch, y):
            return raw[ch, t, :, y * BX : (y + 1) * BX]

        planes = [None] * 12
        for y in range(2):
            wx, wy, rho = half(0, y), half(1, y), half(6, y)
            scale = rho * CD_ICE * jnp.sqrt(wx * wx + wy * wy + 1.0)
            planes[y] = scale * wx
            planes[2 + y] = scale * wy
            for ch in range(2, 6):
                planes[2 * ch + y] = half(ch, y)
        ends = jnp.zeros((per, BX), jnp.float32)
        for p in range(12):
            pay[t, pl.ds(p, per, stride=12), :] = planes[p]
            ends = jnp.where(group == p, roll(planes[p], 8 * p + 4), ends)
        edge[t] = ends
        if cut:
            send(t, 0).start()
        return 0

    def rims(t, _):
        planes = [pay[t, pl.ds(p, per, stride=12), :] for p in range(12)]
        ends = edge[t]
        ids = jnp.zeros((per, BX), jnp.int32)
        for j in range(per):
            ids = jnp.where(slot == j, owner[0, t * per + j] - t * count, ids)

        edges = (0, 1, count - 1, count - 2)
        if per == 8:
            where = [jnp.sum(jnp.where(ids == b, slot + 1, 0), axis=0, keepdims=True) for b in edges]
            spot = jnp.zeros((per, BX), jnp.int32)
            for k, x in enumerate(where):
                spot = jnp.where(slot == k, x, spot)
            held, spot = spot > 0, jnp.maximum(spot - 1, 0)
            for p, x in enumerate(planes + [ends]):
                rim[t, 8 * p : 8 * p + 8, :] = jnp.where(held, jnp.take_along_axis(x, spot, axis=0), 0.0)
        else:
            for p, x in enumerate(planes + [ends]):
                for k, b in enumerate(edges):
                    row = jnp.sum(jnp.where(ids == b, x, 0.0), axis=0, keepdims=True)
                    rim[t, 8 * p + k : 8 * p + k + 1, :] = row
        return 0

    steps(0, n, tile)
    fetched.wait()
    steps(0, n, rims)

    def dest(d, _):
        i, j = d // nlon, d % nlon
        jw, je = (j + nlon - 1) % nlon, (j + 1) % nlon
        q8 = (lane % 8) < 4
        pay[d, 12 * per : 13 * per, :] = at_end(q8, edge[i * nlon + jw], edge[i * nlon + je])
        q2 = (lanes(2) % 8) < 4
        for ii, ok, k, lo, c in (
            (jnp.minimum(i + 1, nlat - 1), i + 1 < nlat, 0, 0, 36),
            (jnp.maximum(i - 1, 0), i > 0, 2, 18, 38),
        ):
            scale = jnp.where(ok, 1.0, 0.0)
            near = ii * nlon + j
            both = rim[near, pl.ds(k, 12, stride=8), :] * scale
            single = rim[near, pl.ds(k + 1 + 4 * k, 6, stride=16), :] * scale
            pay[d, lat_base + lo : lat_base + lo + 12, :] = both
            pay[d, lat_base + lo + 12 : lat_base + lo + 18, :] = single
            corner = at_end(q2, rim[ii * nlon + jw, 96 + k : 98 + k, :], rim[ii * nlon + je, 96 + k : 98 + k, :])
            pay[d, lat_base + c : lat_base + c + 2, :] = corner * scale
        send(d, 1).start()
        return 0

    def finish(d, _):
        if cut:
            send(d, 0).wait()
        send(d, 1).wait()
        return 0

    steps(0, n, dest)
    steps(0, n, finish)


def ends_kernel(ice, covered, land, active, ends):
    count = covered.shape[1]
    lane = lanes(count)
    group = lane // 8
    total = jnp.zeros((count, BX), jnp.float32)
    cover = column(covered[...])
    for y in range(2):
        cells = slice(y * BX, (y + 1) * BX)
        act = cover * (1 - land[:, cells]).astype(jnp.float32)
        active[:, cells] = act
        for ch in range(8):
            x = act if ch == 7 else ice[ch, :, cells]
            p = 2 * ch + y
            total = jnp.where(group == p, roll(x, 8 * p + 4), total)
    ends[...] = total


def pack(raw, owner, nlat, nlon):
    _, n, per, _ = raw.shape
    rows = 13 * per + 40
    return pl.pallas_call(
        functools.partial(pack_kernel, nlat, nlon, per),
        out_shape=f32(n, rows, BX),
        in_specs=[VMEM, pl.BlockSpec(memory_space=pl.ANY)],
        out_specs=pl.BlockSpec(memory_space=pl.ANY),
        scratch_shapes=[
            pltpu.VMEM((n, rows, BX), jnp.float32),
            pltpu.VMEM((n, per, BX), jnp.float32),
            pltpu.VMEM((n, 104, BX), jnp.float32),
            pltpu.SMEM(owner.shape, jnp.int32),
            pltpu.SemaphoreType.DMA((2, n)),
            pltpu.SemaphoreType.DMA,
        ],
        compiler_params=params(24),
        name="pack",
    )(raw, owner)


def open_kernel(n, per, raw, opened):
    @pl.when(lax.axis_index("comp") == 0)
    def _():
        def tile(t, _):
            for y in range(2):
                wx, wy, cx, cy, rho = [raw[ch, t, :, y * BX : (y + 1) * BX] for ch in (0, 1, 2, 3, 6)]
                rx, ry = wx - cx, wy - cy
                speed = jnp.sqrt(rx * rx + ry * ry + 1.0)
                rate = rho * (0.1 + 0.05 * speed) * speed
                opened[t, 2 * y] = rate * rx
                opened[t, 2 * y + 1] = rate * ry
                opened[t, 4 + 2 * y] = cx
                opened[t, 5 + 2 * y] = cy
            return 0

        steps(0, n, tile)


def open_stress(raw):
    _, n, per, _ = raw.shape
    return pl.pallas_call(
        functools.partial(open_kernel, n, per),
        out_shape=f32(n, 8, per, BX),
        in_specs=[VMEM],
        out_specs=VMEM,
        compiler_params=params(24),
        name="open_stress",
    )(raw)


def ice_ends(ice, covered, land):
    count = land.shape[0]
    return pl.pallas_call(
        ends_kernel,
        out_shape=[f32(count, 2 * BX), f32(count, BX)],
        in_specs=[VMEM] * 3,
        out_specs=[VMEM] * 2,
        compiler_params=params(8),
        name="ice_ends",
    )(ice, covered, land)


def table_kernel(nlat, nlon, per, owner, ids):
    def tile(t, _):
        i, j = t // nlon, t % nlon
        near = [t, i * nlon + (j + nlon - 1) % nlon, i * nlon + (j + 1) % nlon]
        for k, other in enumerate(near):
            for slot in range(per):
                ids[t, k * per + slot] = owner[0, other * per + slot] - other * (nlat * nlon * per)
        return 0

    steps(0, nlat * nlon, tile)


def table(owner, nlat, nlon):
    n = nlat * nlon
    per = owner.shape[1] // n
    return pl.pallas_call(
        functools.partial(table_kernel, nlat, nlon, per),
        out_shape=jax.ShapeDtypeStruct((n, 3 * per), jnp.int32),
        in_specs=[SMEM],
        out_specs=SMEM,
        compiler_params=params(4),
        name="table",
    )(owner)


def rows_kernel(ice, active, west, east, sides, north, south):
    count = active.shape[0]
    q = (lanes(count) % 8) < 4
    sides[...] = jnp.where(q, west[...], east[...])
    for out, lo in ((north, count - 2), (south, 0)):
        for y in range(2):
            cells = slice(y * BX, (y + 1) * BX)
            for ch in range(8):
                p = 2 * ch + y
                x = active[lo : lo + 2, cells] if ch == 7 else ice[ch, lo : lo + 2, cells]
                out[2 * p : 2 * p + 2, :] = x
        out[32:34, :] = sides[lo : lo + 2, :]


def ice_rows(ice, active, west, east):
    count = active.shape[0]
    return pl.pallas_call(
        rows_kernel,
        out_shape=[f32(count, BX), f32(34, BX), f32(34, BX)],
        in_specs=[VMEM] * 4,
        out_specs=[VMEM] * 3,
        compiler_params=params(8),
        name="ice_rows",
    )(ice, active, west, east)


def middle(rows):
    lane = lanes(rows)
    return (lane >= BX // 4) & (lane < 3 * BX // 4)


def side_plane(ends, ch, mid):
    odd = roll(ends, BX // 2 - (8 * (2 * ch + 1) + 4))
    return jnp.where(mid, odd, roll(ends, -(16 * ch + 4)))


def statics(mass, conc, act):
    return mass * jnp.exp(CSTAR * (conc - 1.0)) * act * (1.0 / 6.0), 2.0 * mass, act, conc


def prep_kernel(count, height, ice, active, sides, begin, still, unused, grid):
    mid = middle(count)
    for ch in range(8):
        for y in range(2):
            cells = slice(y * BX, (y + 1) * BX)
            grid[ch, y, 2 : 2 + count, :] = active[:, cells] if ch == 7 else ice[ch, :, cells]
        grid[ch, 2, 2 : 2 + count, :] = side_plane(sides[...], ch, mid)
        for z in range(3):
            grid[ch, z, 0:2, :] = jnp.zeros((2, BX), jnp.float32)
            grid[ch, z, count + 2 :, :] = jnp.zeros((height - count - 2, BX), jnp.float32)

    for r in range(height // 8):
        at = slice(8 * r, 8 * r + 8)
        for z in range(3):
            u, v, mass, conc, s1, s2, s12, act = [grid[ch, z, at, :] for ch in range(8)]
            for k, x in enumerate((u, v, 0.5 * s1, 0.5 * s2, s12)):
                begin[k, z, at, :] = x
            for k, x in enumerate(statics(mass, conc, act)):
                still[k, z, at, :] = x


def prep(ice, active, sides, spare):
    count = active.shape[0]
    height = (count + 4 + 7) // 8 * 8
    return pl.pallas_call(
        functools.partial(prep_kernel, count, height),
        out_shape=[f32(5, 3, height, BX), f32(4, 3, height, BX), f32(*spare)],
        in_specs=[VMEM] * 3,
        out_specs=[VMEM] * 3,
        scratch_shapes=[pltpu.VMEM((8, 3, height, BX), jnp.float32)],
        compiler_params=params(12),
        name="prep",
    )(ice, active, sides)


def fetch_kernel(*refs):
    k = len(refs) // 2
    copies = [pltpu.make_async_copy(refs[i], refs[k + i], refs[-1].at[i]) for i in range(k)]
    for copy in copies:
        copy.start()
    for copy in copies:
        copy.wait()


def fetch(*arrays):
    return pl.pallas_call(
        fetch_kernel,
        out_shape=[f32(*x.shape) for x in arrays],
        in_specs=[pl.BlockSpec(memory_space=pl.ANY)] * len(arrays),
        out_specs=[VMEM] * len(arrays),
        scratch_shapes=[pltpu.SemaphoreType.DMA((len(arrays),))],
        compiler_params=params(4),
        name="fetch",
    )(*arrays)


def east_of(even, odd, side, at127, at63):
    e, o, s = roll(even, -1), roll(odd, -1), roll(side, -1)
    wide = jnp.where(at127, e, jnp.where(at63, roll(odd, 63), s))
    return jnp.where(at127, s, e), jnp.where(at127, roll(side, 63), o), wide


def west_of(even, odd, side, at0, at64):
    e, o, s = roll(even, 1), roll(odd, 1), roll(side, 1)
    wide = jnp.where(at0, e, jnp.where(at64, roll(odd, 65), s))
    return jnp.where(at0, s, e), jnp.where(at0, roll(side, -63), o), wide


def ice_kernel(n, per, count, ids_in, recv, begin, fixed, below, above, back, moved, unused,
               spot, hw, he, speed, state, forced, out8, still, ids, ready):
    tiles = (count + 4 + 7) // 8
    height = tiles * 8
    fetched = pltpu.make_async_copy(ids_in, ids, ready)
    fetched.start()
    blank = jnp.zeros((8, BX), jnp.float32)
    for k in (0, 8):
        spot[k : k + 8, :] = blank
    for k in range((count + 3) * STEP, height * STEP, 8):
        spot[k : k + 8, :] = blank
    for k in (0, height - 8):
        hw[k : k + 8, :] = blank
        he[k : k + 8, :] = blank

    q, mid, mid2 = (lanes(8) % 8) < 4, middle(8), middle(2)
    for r in range(tiles):
        at = slice(8 * r, 8 * r + 8)
        to = slice(FRONT + 8 * r, FRONT + 8 * r + 8)
        for z in range(3):
            for k in range(2):
                speed[k, z, to, :] = begin[k, z, at, :]
            for k in range(3):
                state[k, z, to, :] = begin[2 + k, z, at, :]
            hard, m2, act, conc = [fixed[k, z, at, :] for k in range(4)]
            for k, x in enumerate((hard, m2, CW * conc * act, act, conc)):
                still[k, z, at, :] = x
    for lo, msg in ((0, below), (count + 2, above)):
        at, to = slice(lo, lo + 2), slice(FRONT + lo, FRONT + lo + 2)
        for z in range(3):
            if z < 2:
                raw = [msg[4 * ch + 2 * z : 4 * ch + 2 * z + 2, :] for ch in range(8)]
            else:
                raw = [side_plane(msg[32:34, :], ch, mid2) for ch in range(8)]
            u, v, mass, conc, s1, s2, s12, act = raw
            speed[0, z, to, :] = u
            speed[1, z, to, :] = v
            state[0, z, to, :] = 0.5 * s1
            state[1, z, to, :] = 0.5 * s2
            state[2, z, to, :] = s12
            hard, m2, act, conc = statics(mass, conc, act)
            for k, x in enumerate((hard, m2, CW * conc * act, act, conc)):
                still[k, z, at, :] = x

    fetched.wait()

    def place(o, acc):
        for j in range(per):
            b = (ids[o, j] + 2) * STEP
            spot[pl.ds(b, 12), :] = recv[o, 12 * j : 12 * j + 12, :]
            row = recv[o, 12 * per + j : 12 * per + j + 1, :]
            hw[pl.ds(ids[o, per + j] + 2, 1), :] = row
            he[pl.ds(ids[o, 2 * per + j] + 2, 1), :] = row
        return acc + recv[o, 13 * per : 13 * per + 40, :]

    rim = lax.fori_loop(0, n, place, jnp.zeros((40, BX), jnp.float32))
    up, down = (count + 2) * STEP, STEP
    spot[up : up + 12, :] = rim[0:12]
    spot[down : down + 12, :] = rim[18:30]
    for ch in range(6):
        k = up + STEP + 2 * ch
        spot[k : k + 1, :] = rim[12 + ch : 13 + ch]
        k = 2 * ch + 1
        spot[k : k + 1, :] = rim[30 + ch : 31 + ch]
    for ref in (hw, he):
        ref[count + 2 : count + 4, :] = rim[36:38]
        ref[1:2, :] = rim[38:39]
        ref[0:1, :] = rim[39:40]

    for r in range(tiles):
        at = slice(8 * r, 8 * r + 8)
        ends = jnp.where(q, hw[at, :], he[at, :])
        for z in range(3):
            if z < 2:
                f = [spot[pl.ds(8 * r * STEP + 2 * ch + z, 8, stride=STEP), :] for ch in range(6)]
            else:
                f = [side_plane(ends, ch, mid) for ch in range(6)]
            mass, act, conc = [still[k, z, at, :] for k in (1, 3, 4)]
            mass = 0.5 * mass
            forced[0, z, at, :] = act * (conc * f[0] - mass * f[4])
            forced[1, z, at, :] = act * (conc * f[1] - mass * f[5])
            forced[2, z, at, :] = f[2]
            forced[3, z, at, :] = f[3]

    tail = FRONT + height
    for z in range(3):
        for k in range(2):
            speed[k, z, tail : tail + 8, :] = blank
        for k in range(3):
            state[k, z, 0:8, :] = blank

    lane = lanes(8)
    ends_at = [lane == k for k in (BX - 1, BX // 2 - 1, 0, BX // 2)]
    at127, at63, at0, at64 = ends_at

    def rows_of(r):
        row = 8 * r
        return pl.ds(row, 8), pl.ds(row + FRONT, 8), pl.ds(row + FRONT + 1, 8), pl.ds(row + FRONT - 1, 8)

    def stresses(r):
        at, to, up1, _ = rows_of(r)
        u = [speed[0, z, to, :] for z in range(3)]
        v = [speed[1, z, to, :] for z in range(3)]

        def north(k, x):
            return x[1], speed[k, 0, up1, :], roll(jnp.where(mid, x[2], speed[k, 2, up1, :]), BX // 2)

        un, vn = north(0, u), north(1, v)
        ue = east_of(*u, at127, at63)
        ve = east_of(*v, at127, at63)
        for z in range(3):
            sxx = ue[z] - u[z]
            syy = vn[z] - v[z]
            shear = (un[z] - u[z]) + (ve[z] - v[z])
            div, ten = sxx + syy, sxx - syy
            twice = div + div
            inv = lax.rsqrt(twice * twice + (ten * ten + shear * shear) + 1.0)
            hard = still[0, z, at, :]
            kr = hard * inv
            half = 0.5 * kr
            state[0, z, to, :] = (state[0, z, to, :] * (2.0 / 3.0) - hard) + kr * twice
            state[1, z, to, :] = state[1, z, to, :] * (2.0 / 3.0) + half * ten
            state[2, z, to, :] = state[2, z, to, :] * (2.0 / 3.0) + half * shear

    def speeds(r):
        at, to, _, down1 = rows_of(r)
        s1, s2, s12 = [[state[k, z, to, :] for z in range(3)] for k in range(3)]
        a = [x + y for x, y in zip(s1, s2)]
        c = [x - y for x, y in zip(s1, s2)]
        aw = west_of(*a, at0, at64)
        sw = west_of(*s12, at0, at64)

        def south(x, lower):
            return lower(1), x[0], roll(jnp.where(mid, lower(2), x[2]), BX // 2)

        ss = south(s12, lambda z: state[2, z, down1, :])
        cs = south(c, lambda z: state[0, z, down1, :] - state[1, z, down1, :])
        for z in range(3):
            u, v = speed[0, z, to, :], speed[1, z, to, :]
            fx = (a[z] - aw[z]) + (s12[z] - ss[z])
            fy = (s12[z] - sw[z]) + (c[z] - cs[z])
            m2, base = still[1, z, at, :], still[2, z, at, :]
            cx, cy = forced[2, z, at, :], forced[3, z, at, :]
            dx, dy = cx - u, cy - v
            y2 = dx * dx + dy * dy + DRAG_FLOOR
            drag = base * (y2 * lax.rsqrt(y2))
            part = still[3, z, at, :] * (1.0 / (jnp.maximum(m2, 1.0) + drag))
            mc = (0.5 * CORIO) * m2
            speed[0, z, to, :] = part * (m2 * u + fx + forced[0, z, at, :] + drag * cx + mc * v)
            speed[1, z, to, :] = part * (m2 * v + fy + forced[1, z, at, :] + drag * cy - mc * u)

    def subcycle():
        for r in range(tiles):
            stresses(r)
        for r in range(tiles):
            speeds(r)

    for _ in range(NSUB):
        subcycle()

    for r in range(tiles):
        to = slice(FRONT + 8 * r, FRONT + 8 * r + 8)
        for y in range(2):
            for k in range(2):
                out8[pl.ds(8 * r * REPLY + 2 * k + y, 8, stride=REPLY), :] = speed[k, y, to, :]
    for y in range(2):
        for k in range(2):
            moved[k, :, y * BX : (y + 1) * BX] = speed[k, y, FRONT + 2 : FRONT + 2 + count, :]

    def answer(o, _):
        for j in range(per):
            b = (ids[o, j] + 2) * REPLY
            back[o, 4 * j : 4 * j + 4, :] = out8[pl.ds(b, 4), :]
        return 0

    lax.fori_loop(0, n, answer, 0)


def ice_step(ids, recv, begin, fixed, below, above):
    n, per = ids.shape[0], ids.shape[1] // 3
    count = n * per
    height = (count + 4 + 7) // 8 * 8
    tall = height + 2 * FRONT
    scratch = [
        (height * STEP + 8, BX), (height, BX), (height, BX),
        (2, 3, tall, BX), (3, 3, tall, BX), (4, 3, height, BX), (height * REPLY + 8, BX), (5, 3, height, BX),
    ]
    return pl.pallas_call(
        functools.partial(ice_kernel, n, per, count),
        out_shape=[f32(n, 4 * per, BX), f32(2, count, 2 * BX), f32(n, 2 * per, BX)],
        in_specs=[pl.BlockSpec(memory_space=pl.ANY)] + [VMEM] * 5,
        out_specs=[VMEM] * 3,
        scratch_shapes=[pltpu.VMEM(s, jnp.float32) for s in scratch]
        + [pltpu.SMEM(ids.shape, jnp.int32), pltpu.SemaphoreType.DMA],
        compiler_params=params(16),
        name="ice_step",
    )(ids, recv, begin, fixed, below, above)


def cover_kernel(n, per, ids, conc, covered, land, out, spot):
    count = n * per
    cover = column(covered[...])
    for y in range(2):
        cells = slice(y * BX, (y + 1) * BX)
        act = cover * (1 - land[:, cells]).astype(jnp.float32)
        spot[pl.ds(y, count, stride=2), :] = conc[:, cells] * act

    def tile(o, _):
        for j in range(per):
            out[o, 2 * j : 2 * j + 2, :] = spot[pl.ds(2 * ids[o, j], 2), :]
        return 0

    lax.fori_loop(0, n, tile, 0)


def slot_cover(ids, conc, covered, land):
    n, per = ids.shape[0], ids.shape[1] // 3
    count = n * per
    return pl.pallas_call(
        functools.partial(cover_kernel, n, per),
        out_shape=f32(n, 2 * per, BX),
        in_specs=[SMEM] + [VMEM] * 3,
        out_specs=VMEM,
        scratch_shapes=[pltpu.VMEM((2 * count, BX), jnp.float32)],
        compiler_params=params(8),
        name="slot_cover",
    )(ids, conc, covered, land)


def final_kernel(n, per, got, cover, opened, moved, out):
    is_ocean = lax.axis_index("comp") == 0

    @pl.when(is_ocean)
    def _():
        def tile(t, _):
            for y in range(2):
                cells = slice(y * BX, (y + 1) * BX)
                u, v = [got[t, pl.ds(2 * k + y, per, stride=4), :] for k in range(2)]
                part = cover[t, pl.ds(y, per, stride=2), :]
                dx, dy = u - opened[t, 4 + 2 * y], v - opened[t, 5 + 2 * y]
                factor = (CW * part) * jnp.sqrt(dx * dx + dy * dy + DRAG_FLOOR)
                rest = 1.0 - part
                out[0, t, :, cells] = factor * dx + rest * opened[t, 2 * y]
                out[1, t, :, cells] = factor * dy + rest * opened[t, 2 * y + 1]
            return 0

        steps(0, n, tile)

    @pl.when(jnp.logical_not(is_ocean))
    def _():
        out[...] = moved[...]


def final(got, cover, opened, moved):
    n, _, per, _ = opened.shape
    return pl.pallas_call(
        functools.partial(final_kernel, n, per),
        out_shape=f32(2, n, per, 2 * BX),
        in_specs=[VMEM] * 4,
        out_specs=VMEM,
        compiler_params=params(12),
        name="final",
    )(got, cover, opened, moved)


def per_device(fields, block_owner, ice_covered, land_mask):
    nlat, nlon = lax.axis_size("lat"), lax.axis_size("lon")
    n = nlat * nlon
    count = block_owner.shape[0]
    per = count // n
    side = lax.axis_index("comp")
    fields = fields[0]
    split = fields.reshape(7, n, per, 2 * BX)
    owner = block_owner.reshape(1, count)
    other = lax.ppermute(split, "comp", [(0, 1), (1, 0)])
    opened = open_stress(split)
    def everyone(x):
        return lax.all_to_all(x, ("lat", "lon"), split_axis=0, concat_axis=0, tiled=True)

    height = (count + 4 + 7) // 8 * 8

    def ice_side(other, fields, covered, land, owner):
        recv = everyone(pack(other, owner, nlat, nlon))
        active, ends = ice_ends(fields, covered, land)
        ring = [(i, (i + 1) % nlon) for i in range(nlon)]
        west = lax.ppermute(ends, "lon", ring)
        east = lax.ppermute(ends, "lon", [(j, i) for i, j in ring])
        sides, north, south = ice_rows(fields, active, west, east)
        line = [(i, i + 1) for i in range(nlat - 1)]
        below = lax.ppermute(north, "lat", line)
        above = lax.ppermute(south, "lat", [(j, i) for i, j in line])
        begin, fixed, mine = prep(fields, active, sides, (n, 2 * per, BX))
        return recv, jnp.zeros((n, 3 * per), jnp.int32), below, above, begin, fixed, mine

    def ocean_side(other, fields, covered, land, owner):
        row = jnp.zeros((34, BX), jnp.float32)
        blank = jnp.zeros((5, 3, height, BX), jnp.float32)
        owned = everyone(table(owner, nlat, nlon))
        mine = slot_cover(owned, other.reshape(7, count, 2 * BX)[3], covered, land)
        return jnp.zeros((n, 13 * per + 40, BX), jnp.float32), owned, row, row, blank, blank[:4], mine

    recv, owned, below, above, begin, fixed, mine = lax.cond(
        side == 1, ice_side, ocean_side, other, fields, ice_covered.reshape(1, count), land_mask, owner
    )
    swap = lax.ppermute(owned, "comp", [(0, 1), (1, 0)])
    recv, below, above = fetch(recv, below, above)

    def ice_work(ids, recv, begin, fixed, below, above, mine):
        return ice_step(ids, recv, begin, fixed, below, above)

    def ocean_work(ids, recv, begin, fixed, below, above, mine):
        return jnp.zeros((n, 4 * per, BX), jnp.float32), jnp.zeros((2, count, 2 * BX), jnp.float32), everyone(mine)

    back, moved, cover = lax.cond(
        side == 1, ice_work, ocean_work, swap, recv, begin, fixed, below, above, mine
    )
    back = lax.cond(side == 1, everyone, lambda x: x, back)
    got = lax.ppermute(back, "comp", [(0, 1), (1, 0)])
    out = final(got, cover, opened, moved.reshape(2, n, per, 2 * BX))
    return out.reshape(1, 2, count, 2 * BX)


def solution(mesh):
    placed = (
        P("comp", None, ("lat", "lon"), None),
        P(("lat", "lon")),
        P(("lat", "lon")),
        P(("lat", "lon"), None),
    )
    return jax.shard_map(
        per_device,
        mesh=mesh,
        in_specs=placed,
        out_specs=P("comp", None, ("lat", "lon"), None),
        check_vma=False,
    )
```

```python
import functools

import jax
import jax.numpy as jnp
from jax import lax
from jax.experimental import pallas as pl
from jax.experimental.pallas import tpu as pltpu
from jax.sharding import PartitionSpec as P

BX = 128
NSUB = 4
FRONT = 8
STEP = 13
REPLY = 5

CD_ICE = 0.1
CW = 1.5
CSTAR = 2.0
CORIO = 0.3
DRAG_FLOOR = 0.1

VMEM = pl.BlockSpec(memory_space=pltpu.VMEM)
SMEM = pl.BlockSpec(memory_space=pltpu.SMEM)


def params(mib):
    return pltpu.CompilerParams(vmem_limit_bytes=mib * 1024 * 1024)


def f32(*shape):
    return jax.ShapeDtypeStruct(shape, jnp.float32)


def lanes(rows):
    return lax.broadcasted_iota(jnp.int32, (rows, BX), 1)


def roll(x, by):
    return pltpu.roll(x, by % BX, 1)


def at_end(q, west, east):
    return jnp.where(q, west, east)


def column(row):
    parts = []
    for lo in range(0, row.shape[1], BX):
        diag = lax.broadcasted_iota(jnp.int32, (BX, BX), 0) == lanes(BX)
        parts.append(jnp.sum(jnp.where(diag, row[:, lo : lo + BX].astype(jnp.float32), 0.0), axis=1, keepdims=True))
    return jnp.concatenate(parts, 0) if len(parts) > 1 else parts[0]


def steps(lo, hi, body):
    if hi - lo <= 32:
        for k in range(lo, hi):
            body(k, 0)
    else:
        lax.fori_loop(lo, hi, body, 0)


def pack_kernel(nlat, nlon, per, raw, owner_in, out, pay, edge, rim, owner, sems, ready):
    n = nlat * nlon
    count = n * per
    cut = 12 * per if (12 * per) % 8 == 0 else 0

    def send(d, k):
        at = pl.ds(0, cut) if k == 0 else pl.ds(cut, 13 * per + 40 - cut)
        return pltpu.make_async_copy(pay.at[d, at], out.at[d, at], sems.at[k, d])

    fetched = pltpu.make_async_copy(owner_in, owner, ready)
    fetched.start()
    lane = lanes(per)
    group = lane // 8
    slot = lax.broadcasted_iota(jnp.int32, (per, BX), 0)
    lat_base = 13 * per

    def tile(t, _):
        def half(ch, y):
            return raw[ch, t, :, y * BX : (y + 1) * BX]

        planes = [None] * 12
        for y in range(2):
            wx, wy, rho = half(0, y), half(1, y), half(6, y)
            scale = rho * CD_ICE * jnp.sqrt(wx * wx + wy * wy + 1.0)
            planes[y] = scale * wx
            planes[2 + y] = scale * wy
            for ch in range(2, 6):
                planes[2 * ch + y] = half(ch, y)
        ends = jnp.zeros((per, BX), jnp.float32)
        for p in range(12):
            pay[t, pl.ds(p, per, stride=12), :] = planes[p]
            ends = jnp.where(group == p, roll(planes[p], 8 * p + 4), ends)
        edge[t] = ends
        if cut:
            send(t, 0).start()
        return 0

    def rims(t, _):
        planes = [pay[t, pl.ds(p, per, stride=12), :] for p in range(12)]
        ends = edge[t]
        ids = jnp.zeros((per, BX), jnp.int32)
        for j in range(per):
            ids = jnp.where(slot == j, owner[0, t * per + j] - t * count, ids)

        edges = (0, 1, count - 1, count - 2)
        if per == 8:
            where = [jnp.sum(jnp.where(ids == b, slot + 1, 0), axis=0, keepdims=True) for b in edges]
            spot = jnp.zeros((per, BX), jnp.int32)
            for k, x in enumerate(where):
                spot = jnp.where(slot == k, x, spot)
            held, spot = spot > 0, jnp.maximum(spot - 1, 0)
            for p, x in enumerate(planes + [ends]):
                rim[t, 8 * p : 8 * p + 8, :] = jnp.where(held, jnp.take_along_axis(x, spot, axis=0), 0.0)
        else:
            for p, x in enumerate(planes + [ends]):
                for k, b in enumerate(edges):
                    row = jnp.sum(jnp.where(ids == b, x, 0.0), axis=0, keepdims=True)
                    rim[t, 8 * p + k : 8 * p + k + 1, :] = row
        return 0

    steps(0, n, tile)
    fetched.wait()
    steps(0, n, rims)

    def dest(d, _):
        i, j = d // nlon, d % nlon
        jw, je = (j + nlon - 1) % nlon, (j + 1) % nlon
        q8 = (lane % 8) < 4
        pay[d, 12 * per : 13 * per, :] = at_end(q8, edge[i * nlon + jw], edge[i * nlon + je])
        q2 = (lanes(2) % 8) < 4
        for ii, ok, k, lo, c in (
            (jnp.minimum(i + 1, nlat - 1), i + 1 < nlat, 0, 0, 36),
            (jnp.maximum(i - 1, 0), i > 0, 2, 18, 38),
        ):
            scale = jnp.where(ok, 1.0, 0.0)
            near = ii * nlon + j
            both = rim[near, pl.ds(k, 12, stride=8), :] * scale
            single = rim[near, pl.ds(k + 1 + 4 * k, 6, stride=16), :] * scale
            pay[d, lat_base + lo : lat_base + lo + 12, :] = both
            pay[d, lat_base + lo + 12 : lat_base + lo + 18, :] = single
            corner = at_end(q2, rim[ii * nlon + jw, 96 + k : 98 + k, :], rim[ii * nlon + je, 96 + k : 98 + k, :])
            pay[d, lat_base + c : lat_base + c + 2, :] = corner * scale
        send(d, 1).start()
        return 0

    def finish(d, _):
        if cut:
            send(d, 0).wait()
        send(d, 1).wait()
        return 0

    steps(0, n, dest)
    steps(0, n, finish)


def ends_kernel(ice, covered, land, active, ends):
    count = covered.shape[1]
    lane = lanes(count)
    group = lane // 8
    total = jnp.zeros((count, BX), jnp.float32)
    cover = column(covered[...])
    for y in range(2):
        cells = slice(y * BX, (y + 1) * BX)
        act = cover * (1 - land[:, cells]).astype(jnp.float32)
        active[:, cells] = act
        for ch in range(8):
            x = act if ch == 7 else ice[ch, :, cells]
            p = 2 * ch + y
            total = jnp.where(group == p, roll(x, 8 * p + 4), total)
    ends[...] = total


def pack(raw, owner, nlat, nlon):
    _, n, per, _ = raw.shape
    rows = 13 * per + 40
    return pl.pallas_call(
        functools.partial(pack_kernel, nlat, nlon, per),
        out_shape=f32(n, rows, BX),
        in_specs=[VMEM, pl.BlockSpec(memory_space=pl.ANY)],
        out_specs=pl.BlockSpec(memory_space=pl.ANY),
        scratch_shapes=[
            pltpu.VMEM((n, rows, BX), jnp.float32),
            pltpu.VMEM((n, per, BX), jnp.float32),
            pltpu.VMEM((n, 104, BX), jnp.float32),
            pltpu.SMEM(owner.shape, jnp.int32),
            pltpu.SemaphoreType.DMA((2, n)),
            pltpu.SemaphoreType.DMA,
        ],
        compiler_params=params(24),
        name="pack",
    )(raw, owner)


def open_kernel(n, per, raw, opened):
    @pl.when(lax.axis_index("comp") == 0)
    def _():
        def tile(t, _):
            for y in range(2):
                wx, wy, cx, cy, rho = [raw[ch, t, :, y * BX : (y + 1) * BX] for ch in (0, 1, 2, 3, 6)]
                rx, ry = wx - cx, wy - cy
                speed = jnp.sqrt(rx * rx + ry * ry + 1.0)
                rate = rho * (0.1 + 0.05 * speed) * speed
                opened[t, 2 * y] = rate * rx
                opened[t, 2 * y + 1] = rate * ry
                opened[t, 4 + 2 * y] = cx
                opened[t, 5 + 2 * y] = cy
            return 0

        steps(0, n, tile)


def open_stress(raw):
    _, n, per, _ = raw.shape
    return pl.pallas_call(
        functools.partial(open_kernel, n, per),
        out_shape=f32(n, 8, per, BX),
        in_specs=[VMEM],
        out_specs=VMEM,
        compiler_params=params(24),
        name="open_stress",
    )(raw)


def ice_ends(ice, covered, land):
    count = land.shape[0]
    return pl.pallas_call(
        ends_kernel,
        out_shape=[f32(count, 2 * BX), f32(count, BX)],
        in_specs=[VMEM] * 3,
        out_specs=[VMEM] * 2,
        compiler_params=params(8),
        name="ice_ends",
    )(ice, covered, land)


def table_kernel(nlat, nlon, per, owner, ids):
    def tile(t, _):
        i, j = t // nlon, t % nlon
        near = [t, i * nlon + (j + nlon - 1) % nlon, i * nlon + (j + 1) % nlon]
        for k, other in enumerate(near):
            for slot in range(per):
                ids[t, k * per + slot] = owner[0, other * per + slot] - other * (nlat * nlon * per)
        return 0

    steps(0, nlat * nlon, tile)


def table(owner, nlat, nlon):
    n = nlat * nlon
    per = owner.shape[1] // n
    return pl.pallas_call(
        functools.partial(table_kernel, nlat, nlon, per),
        out_shape=jax.ShapeDtypeStruct((n, 3 * per), jnp.int32),
        in_specs=[SMEM],
        out_specs=SMEM,
        compiler_params=params(4),
        name="table",
    )(owner)


def rows_kernel(ice, active, west, east, sides, north, south):
    count = active.shape[0]
    q = (lanes(count) % 8) < 4
    sides[...] = jnp.where(q, west[...], east[...])
    for out, lo in ((north, count - 2), (south, 0)):
        for y in range(2):
            cells = slice(y * BX, (y + 1) * BX)
            for ch in range(8):
                p = 2 * ch + y
                x = active[lo : lo + 2, cells] if ch == 7 else ice[ch, lo : lo + 2, cells]
                out[2 * p : 2 * p + 2, :] = x
        out[32:34, :] = sides[lo : lo + 2, :]


def ice_rows(ice, active, west, east):
    count = active.shape[0]
    return pl.pallas_call(
        rows_kernel,
        out_shape=[f32(count, BX), f32(34, BX), f32(34, BX)],
        in_specs=[VMEM] * 4,
        out_specs=[VMEM] * 3,
        compiler_params=params(8),
        name="ice_rows",
    )(ice, active, west, east)


def middle(rows):
    lane = lanes(rows)
    return (lane >= BX // 4) & (lane < 3 * BX // 4)


def side_plane(ends, ch, mid):
    odd = roll(ends, BX // 2 - (8 * (2 * ch + 1) + 4))
    return jnp.where(mid, odd, roll(ends, -(16 * ch + 4)))


def statics(mass, conc, act):
    return mass * jnp.exp(CSTAR * (conc - 1.0)) * act * (1.0 / 6.0), 2.0 * mass, act, conc


def prep_kernel(count, height, ice, active, sides, begin, still, unused, grid):
    mid = middle(count)
    for ch in range(8):
        for y in range(2):
            cells = slice(y * BX, (y + 1) * BX)
            grid[ch, y, 2 : 2 + count, :] = active[:, cells] if ch == 7 else ice[ch, :, cells]
        grid[ch, 2, 2 : 2 + count, :] = side_plane(sides[...], ch, mid)
        for z in range(3):
            grid[ch, z, 0:2, :] = jnp.zeros((2, BX), jnp.float32)
            grid[ch, z, count + 2 :, :] = jnp.zeros((height - count - 2, BX), jnp.float32)

    for r in range(height // 8):
        at = slice(8 * r, 8 * r + 8)
        for z in range(3):
            u, v, mass, conc, s1, s2, s12, act = [grid[ch, z, at, :] for ch in range(8)]
            for k, x in enumerate((u, v, 0.5 * s1, 0.5 * s2, s12)):
                begin[k, z, at, :] = x
            for k, x in enumerate(statics(mass, conc, act)):
                still[k, z, at, :] = x


def prep(ice, active, sides, spare):
    count = active.shape[0]
    height = (count + 4 + 7) // 8 * 8
    return pl.pallas_call(
        functools.partial(prep_kernel, count, height),
        out_shape=[f32(5, 3, height, BX), f32(4, 3, height, BX), f32(*spare)],
        in_specs=[VMEM] * 3,
        out_specs=[VMEM] * 3,
        scratch_shapes=[pltpu.VMEM((8, 3, height, BX), jnp.float32)],
        compiler_params=params(12),
        name="prep",
    )(ice, active, sides)


def fetch_kernel(*refs):
    k = len(refs) // 2
    big, parts = refs[0].shape[0], 4
    pieces = [(0, pl.ds(c * big // parts, big // parts)) for c in range(parts)] if big % parts == 0 else [(0, pl.ds(0, big))]
    pieces += [(i, pl.ds(0, refs[i].shape[0])) for i in range(1, k)]
    copies = [
        pltpu.make_async_copy(refs[i].at[at], refs[k + i].at[at], refs[-1].at[c]) for c, (i, at) in enumerate(pieces)
    ]
    for copy in copies:
        copy.start()
    for copy in copies:
        copy.wait()


def fetch(*arrays):
    return pl.pallas_call(
        fetch_kernel,
        out_shape=[f32(*x.shape) for x in arrays],
        in_specs=[pl.BlockSpec(memory_space=pl.ANY)] * len(arrays),
        out_specs=[VMEM] * len(arrays),
        scratch_shapes=[pltpu.SemaphoreType.DMA((len(arrays) + 3,))],
        compiler_params=params(4),
        name="fetch",
    )(*arrays)


def east_of(even, odd, side, at127, at63):
    e, o, s = roll(even, -1), roll(odd, -1), roll(side, -1)
    wide = jnp.where(at127, e, jnp.where(at63, roll(odd, 63), s))
    return jnp.where(at127, s, e), jnp.where(at127, roll(side, 63), o), wide


def west_of(even, odd, side, at0, at64):
    e, o, s = roll(even, 1), roll(odd, 1), roll(side, 1)
    wide = jnp.where(at0, e, jnp.where(at64, roll(odd, 65), s))
    return jnp.where(at0, s, e), jnp.where(at0, roll(side, -63), o), wide


def ice_kernel(n, per, count, ids_in, recv, begin, fixed, below, above, back, moved, unused,
               spot, hw, he, speed, state, forced, out8, still, ids, ready):
    tiles = (count + 4 + 7) // 8
    height = tiles * 8
    fetched = pltpu.make_async_copy(ids_in, ids, ready)
    fetched.start()
    blank = jnp.zeros((8, BX), jnp.float32)
    for k in (0, 8):
        spot[k : k + 8, :] = blank
    for k in range((count + 3) * STEP, height * STEP, 8):
        spot[k : k + 8, :] = blank
    for k in (0, height - 8):
        hw[k : k + 8, :] = blank
        he[k : k + 8, :] = blank

    q, mid, mid2 = (lanes(8) % 8) < 4, middle(8), middle(2)
    for r in range(tiles):
        at = slice(8 * r, 8 * r + 8)
        to = slice(FRONT + 8 * r, FRONT + 8 * r + 8)
        for z in range(3):
            for k in range(2):
                speed[k, z, to, :] = begin[k, z, at, :]
            for k in range(3):
                state[k, z, to, :] = begin[2 + k, z, at, :]
            hard, m2, act, conc = [fixed[k, z, at, :] for k in range(4)]
            for k, x in enumerate((hard, m2, CW * conc * act, act, conc)):
                still[k, z, at, :] = x
    for lo, msg in ((0, below), (count + 2, above)):
        at, to = slice(lo, lo + 2), slice(FRONT + lo, FRONT + lo + 2)
        for z in range(3):
            if z < 2:
                raw = [msg[4 * ch + 2 * z : 4 * ch + 2 * z + 2, :] for ch in range(8)]
            else:
                raw = [side_plane(msg[32:34, :], ch, mid2) for ch in range(8)]
            u, v, mass, conc, s1, s2, s12, act = raw
            speed[0, z, to, :] = u
            speed[1, z, to, :] = v
            state[0, z, to, :] = 0.5 * s1
            state[1, z, to, :] = 0.5 * s2
            state[2, z, to, :] = s12
            hard, m2, act, conc = statics(mass, conc, act)
            for k, x in enumerate((hard, m2, CW * conc * act, act, conc)):
                still[k, z, at, :] = x

    fetched.wait()

    def place(o, acc):
        for j in range(per):
            b = (ids[o, j] + 2) * STEP
            spot[pl.ds(b, 12), :] = recv[o, 12 * j : 12 * j + 12, :]
            row = recv[o, 12 * per + j : 12 * per + j + 1, :]
            hw[pl.ds(ids[o, per + j] + 2, 1), :] = row
            he[pl.ds(ids[o, 2 * per + j] + 2, 1), :] = row
        return acc + recv[o, 13 * per : 13 * per + 40, :]

    rim = jnp.zeros((40, BX), jnp.float32)
    if n <= 32:
        for o in range(n):
            rim = place(o, rim)
    else:
        rim = lax.fori_loop(0, n, place, rim)
    up, down = (count + 2) * STEP, STEP
    spot[up : up + 12, :] = rim[0:12]
    spot[down : down + 12, :] = rim[18:30]
    for ch in range(6):
        k = up + STEP + 2 * ch
        spot[k : k + 1, :] = rim[12 + ch : 13 + ch]
        k = 2 * ch + 1
        spot[k : k + 1, :] = rim[30 + ch : 31 + ch]
    for ref in (hw, he):
        ref[count + 2 : count + 4, :] = rim[36:38]
        ref[1:2, :] = rim[38:39]
        ref[0:1, :] = rim[39:40]

    for r in range(tiles):
        at = slice(8 * r, 8 * r + 8)
        ends = jnp.where(q, hw[at, :], he[at, :])
        for z in range(3):
            if z < 2:
                f = [spot[pl.ds(8 * r * STEP + 2 * ch + z, 8, stride=STEP), :] for ch in range(6)]
            else:
                f = [side_plane(ends, ch, mid) for ch in range(6)]
            mass, act, conc = [still[k, z, at, :] for k in (1, 3, 4)]
            mass = 0.5 * mass
            forced[0, z, at, :] = act * (conc * f[0] - mass * f[4])
            forced[1, z, at, :] = act * (conc * f[1] - mass * f[5])
            forced[2, z, at, :] = f[2]
            forced[3, z, at, :] = f[3]

    tail = FRONT + height
    for z in range(3):
        for k in range(2):
            speed[k, z, tail : tail + 8, :] = blank
        for k in range(3):
            state[k, z, 0:8, :] = blank

    lane = lanes(8)
    ends_at = [lane == k for k in (BX - 1, BX // 2 - 1, 0, BX // 2)]
    at127, at63, at0, at64 = ends_at

    def rows_of(r):
        row = 8 * r
        return pl.ds(row, 8), pl.ds(row + FRONT, 8), pl.ds(row + FRONT + 1, 8), pl.ds(row + FRONT - 1, 8)

    def stresses(r):
        at, to, up1, _ = rows_of(r)
        u = [speed[0, z, to, :] for z in range(3)]
        v = [speed[1, z, to, :] for z in range(3)]

        def north(k, x):
            return x[1], speed[k, 0, up1, :], roll(jnp.where(mid, x[2], speed[k, 2, up1, :]), BX // 2)

        un, vn = north(0, u), north(1, v)
        ue = east_of(*u, at127, at63)
        ve = east_of(*v, at127, at63)
        for z in range(3):
            sxx = ue[z] - u[z]
            syy = vn[z] - v[z]
            shear = (un[z] - u[z]) + (ve[z] - v[z])
            div, ten = sxx + syy, sxx - syy
            twice = div + div
            inv = lax.rsqrt(twice * twice + (ten * ten + shear * shear) + 1.0)
            hard = still[0, z, at, :]
            kr = hard * inv
            half = 0.5 * kr
            state[0, z, to, :] = (state[0, z, to, :] * (2.0 / 3.0) - hard) + kr * twice
            state[1, z, to, :] = state[1, z, to, :] * (2.0 / 3.0) + half * ten
            state[2, z, to, :] = state[2, z, to, :] * (2.0 / 3.0) + half * shear

    def speeds(r):
        at, to, _, down1 = rows_of(r)
        s1, s2, s12 = [[state[k, z, to, :] for z in range(3)] for k in range(3)]
        a = [x + y for x, y in zip(s1, s2)]
        c = [x - y for x, y in zip(s1, s2)]
        aw = west_of(*a, at0, at64)
        sw = west_of(*s12, at0, at64)

        def south(x, lower):
            return lower(1), x[0], roll(jnp.where(mid, lower(2), x[2]), BX // 2)

        ss = south(s12, lambda z: state[2, z, down1, :])
        cs = south(c, lambda z: state[0, z, down1, :] - state[1, z, down1, :])
        for z in range(3):
            u, v = speed[0, z, to, :], speed[1, z, to, :]
            fx = (a[z] - aw[z]) + (s12[z] - ss[z])
            fy = (s12[z] - sw[z]) + (c[z] - cs[z])
            m2, base = still[1, z, at, :], still[2, z, at, :]
            cx, cy = forced[2, z, at, :], forced[3, z, at, :]
            dx, dy = cx - u, cy - v
            y2 = dx * dx + dy * dy + DRAG_FLOOR
            drag = base * (y2 * lax.rsqrt(y2))
            part = still[3, z, at, :] * (1.0 / (jnp.maximum(m2, 1.0) + drag))
            mc = (0.5 * CORIO) * m2
            speed[0, z, to, :] = part * (m2 * u + fx + forced[0, z, at, :] + drag * cx + mc * v)
            speed[1, z, to, :] = part * (m2 * v + fy + forced[1, z, at, :] + drag * cy - mc * u)

    def subcycle():
        for r in range(tiles):
            stresses(r)
        for r in range(tiles):
            speeds(r)

    for _ in range(NSUB):
        subcycle()

    for r in range(tiles):
        to = slice(FRONT + 8 * r, FRONT + 8 * r + 8)
        for y in range(2):
            for k in range(2):
                out8[pl.ds(8 * r * REPLY + 2 * k + y, 8, stride=REPLY), :] = speed[k, y, to, :]
    for y in range(2):
        for k in range(2):
            moved[k, :, y * BX : (y + 1) * BX] = speed[k, y, FRONT + 2 : FRONT + 2 + count, :]

    def answer(o, _):
        for j in range(per):
            b = (ids[o, j] + 2) * REPLY
            back[o, 4 * j : 4 * j + 4, :] = out8[pl.ds(b, 4), :]
        return 0

    steps(0, n, answer)


def ice_step(ids, recv, begin, fixed, below, above):
    n, per = ids.shape[0], ids.shape[1] // 3
    count = n * per
    height = (count + 4 + 7) // 8 * 8
    tall = height + 2 * FRONT
    scratch = [
        (height * STEP + 8, BX), (height, BX), (height, BX),
        (2, 3, tall, BX), (3, 3, tall, BX), (4, 3, height, BX), (height * REPLY + 8, BX), (5, 3, height, BX),
    ]
    return pl.pallas_call(
        functools.partial(ice_kernel, n, per, count),
        out_shape=[f32(n, 4 * per, BX), f32(2, count, 2 * BX), f32(n, 2 * per, BX)],
        in_specs=[pl.BlockSpec(memory_space=pl.ANY)] + [VMEM] * 5,
        out_specs=[VMEM] * 3,
        scratch_shapes=[pltpu.VMEM(s, jnp.float32) for s in scratch]
        + [pltpu.SMEM(ids.shape, jnp.int32), pltpu.SemaphoreType.DMA],
        compiler_params=params(16),
        name="ice_step",
    )(ids, recv, begin, fixed, below, above)


def cover_kernel(n, per, ids, conc, covered, land, out, spot):
    count = n * per
    cover = column(covered[...])
    for y in range(2):
        cells = slice(y * BX, (y + 1) * BX)
        act = cover * (1 - land[:, cells]).astype(jnp.float32)
        spot[pl.ds(y, count, stride=2), :] = conc[:, cells] * act

    def tile(o, _):
        for j in range(per):
            out[o, 2 * j : 2 * j + 2, :] = spot[pl.ds(2 * ids[o, j], 2), :]
        return 0

    lax.fori_loop(0, n, tile, 0)


def slot_cover(ids, conc, covered, land):
    n, per = ids.shape[0], ids.shape[1] // 3
    count = n * per
    return pl.pallas_call(
        functools.partial(cover_kernel, n, per),
        out_shape=f32(n, 2 * per, BX),
        in_specs=[SMEM] + [VMEM] * 3,
        out_specs=VMEM,
        scratch_shapes=[pltpu.VMEM((2 * count, BX), jnp.float32)],
        compiler_params=params(8),
        name="slot_cover",
    )(ids, conc, covered, land)


def final_kernel(n, per, got, cover, opened, moved, out):
    is_ocean = lax.axis_index("comp") == 0

    @pl.when(is_ocean)
    def _():
        def tile(t, _):
            for y in range(2):
                cells = slice(y * BX, (y + 1) * BX)
                u, v = [got[t, pl.ds(2 * k + y, per, stride=4), :] for k in range(2)]
                part = cover[t, pl.ds(y, per, stride=2), :]
                dx, dy = u - opened[t, 4 + 2 * y], v - opened[t, 5 + 2 * y]
                factor = (CW * part) * jnp.sqrt(dx * dx + dy * dy + DRAG_FLOOR)
                rest = 1.0 - part
                out[0, t, :, cells] = factor * dx + rest * opened[t, 2 * y]
                out[1, t, :, cells] = factor * dy + rest * opened[t, 2 * y + 1]
            return 0

        steps(0, n, tile)

    @pl.when(jnp.logical_not(is_ocean))
    def _():
        out[...] = moved[...]


def final(got, cover, opened, moved):
    n, _, per, _ = opened.shape
    return pl.pallas_call(
        functools.partial(final_kernel, n, per),
        out_shape=f32(2, n, per, 2 * BX),
        in_specs=[VMEM] * 4,
        out_specs=VMEM,
        compiler_params=params(12),
        name="final",
    )(got, cover, opened, moved)


def per_device(fields, block_owner, ice_covered, land_mask):
    nlat, nlon = lax.axis_size("lat"), lax.axis_size("lon")
    n = nlat * nlon
    count = block_owner.shape[0]
    per = count // n
    side = lax.axis_index("comp")
    fields = fields[0]
    split = fields.reshape(7, n, per, 2 * BX)
    owner = block_owner.reshape(1, count)
    other = lax.ppermute(split, "comp", [(0, 1), (1, 0)])
    opened = open_stress(split)
    def everyone(x):
        return lax.all_to_all(x, ("lat", "lon"), split_axis=0, concat_axis=0, tiled=True)

    height = (count + 4 + 7) // 8 * 8

    def ice_side(other, fields, covered, land, owner):
        recv = everyone(pack(other, owner, nlat, nlon))
        active, ends = ice_ends(fields, covered, land)
        ring = [(i, (i + 1) % nlon) for i in range(nlon)]
        west = lax.ppermute(ends, "lon", ring)
        east = lax.ppermute(ends, "lon", [(j, i) for i, j in ring])
        sides, north, south = ice_rows(fields, active, west, east)
        line = [(i, i + 1) for i in range(nlat - 1)]
        below = lax.ppermute(north, "lat", line)
        above = lax.ppermute(south, "lat", [(j, i) for i, j in line])
        begin, fixed, mine = prep(fields, active, sides, (n, 2 * per, BX))
        return recv, jnp.zeros((n, 3 * per), jnp.int32), below, above, begin, fixed, mine

    def ocean_side(other, fields, covered, land, owner):
        row = jnp.zeros((34, BX), jnp.float32)
        blank = jnp.zeros((5, 3, height, BX), jnp.float32)
        owned = everyone(table(owner, nlat, nlon))
        mine = slot_cover(owned, other.reshape(7, count, 2 * BX)[3], covered, land)
        return jnp.zeros((n, 13 * per + 40, BX), jnp.float32), owned, row, row, blank, blank[:4], mine

    recv, owned, below, above, begin, fixed, mine = lax.cond(
        side == 1, ice_side, ocean_side, other, fields, ice_covered.reshape(1, count), land_mask, owner
    )
    swap = lax.ppermute(owned, "comp", [(0, 1), (1, 0)])
    recv, below, above = fetch(recv, below, above)

    def ice_work(ids, recv, begin, fixed, below, above, mine):
        return ice_step(ids, recv, begin, fixed, below, above)

    def ocean_work(ids, recv, begin, fixed, below, above, mine):
        return jnp.zeros((n, 4 * per, BX), jnp.float32), jnp.zeros((2, count, 2 * BX), jnp.float32), everyone(mine)

    back, moved, cover = lax.cond(
        side == 1, ice_work, ocean_work, swap, recv, begin, fixed, below, above, mine
    )
    back = lax.cond(side == 1, everyone, lambda x: x, back)
    got = lax.ppermute(back, "comp", [(0, 1), (1, 0)])
    out = final(got, cover, opened, moved.reshape(2, n, per, 2 * BX))
    return out.reshape(1, 2, count, 2 * BX)


def solution(mesh):
    placed = (
        P("comp", None, ("lat", "lon"), None),
        P(("lat", "lon")),
        P(("lat", "lon")),
        P(("lat", "lon"), None),
    )
    return jax.shard_map(
        per_device,
        mesh=mesh,
        in_specs=placed,
        out_specs=P("comp", None, ("lat", "lon"), None),
        check_vma=False,
    )
```

```python
import functools

import jax
import jax.numpy as jnp
from jax import lax
from jax.experimental import pallas as pl
from jax.experimental.pallas import tpu as pltpu
from jax.sharding import PartitionSpec as P

BX = 128
NSUB = 4
FRONT = 8
STEP = 13
REPLY = 5

CD_ICE = 0.1
CW = 1.5
CSTAR = 2.0
CORIO = 0.3
DRAG_FLOOR = 0.1

VMEM = pl.BlockSpec(memory_space=pltpu.VMEM)
SMEM = pl.BlockSpec(memory_space=pltpu.SMEM)


def params(mib):
    return pltpu.CompilerParams(vmem_limit_bytes=mib * 1024 * 1024)


def f32(*shape):
    return jax.ShapeDtypeStruct(shape, jnp.float32)


def lanes(rows):
    return lax.broadcasted_iota(jnp.int32, (rows, BX), 1)


def roll(x, by):
    return pltpu.roll(x, by % BX, 1)


def at_end(q, west, east):
    return jnp.where(q, west, east)


def column(row):
    parts = []
    for lo in range(0, row.shape[1], BX):
        diag = lax.broadcasted_iota(jnp.int32, (BX, BX), 0) == lanes(BX)
        parts.append(jnp.sum(jnp.where(diag, row[:, lo : lo + BX].astype(jnp.float32), 0.0), axis=1, keepdims=True))
    return jnp.concatenate(parts, 0) if len(parts) > 1 else parts[0]


def steps(lo, hi, body):
    if hi - lo <= 32:
        for k in range(lo, hi):
            body(k, 0)
    else:
        lax.fori_loop(lo, hi, body, 0)


def pack_kernel(nlat, nlon, per, raw, spread, out, pay, edge, rim, sems):
    n = nlat * nlon
    count = n * per
    cut = 12 * per if (12 * per) % 8 == 0 else 0

    def send(d, k):
        at = pl.ds(0, cut) if k == 0 else pl.ds(cut, 13 * per + 40 - cut)
        return pltpu.make_async_copy(pay.at[d, at], out.at[d, at], sems.at[k, d])

    lane = lanes(per)
    group = lane // 8
    slot = lax.broadcasted_iota(jnp.int32, (per, BX), 0)
    lat_base = 13 * per

    def tile(t, _):
        def half(ch, y):
            return raw[ch, t, :, y * BX : (y + 1) * BX]

        planes = [None] * 12
        for y in range(2):
            wx, wy, rho = half(0, y), half(1, y), half(6, y)
            scale = rho * CD_ICE * jnp.sqrt(wx * wx + wy * wy + 1.0)
            planes[y] = scale * wx
            planes[2 + y] = scale * wy
            for ch in range(2, 6):
                planes[2 * ch + y] = half(ch, y)
        ends = jnp.zeros((per, BX), jnp.float32)
        for p in range(12):
            pay[t, pl.ds(p, per, stride=12), :] = planes[p]
            ends = jnp.where(group == p, roll(planes[p], 8 * p + 4), ends)
        edge[t] = ends
        if cut:
            send(t, 0).start()
        return 0

    def rims(t, _):
        planes = [pay[t, pl.ds(p, per, stride=12), :] for p in range(12)]
        ends = edge[t]
        ids = spread[t]
        edges = (0, 1, count - 1, count - 2)
        if per == 8:
            where = [jnp.sum(jnp.where(ids == b, slot + 1, 0), axis=0, keepdims=True) for b in edges]
            spot = jnp.zeros((per, BX), jnp.int32)
            for k, x in enumerate(where):
                spot = jnp.where(slot == k, x, spot)
            held, spot = spot > 0, jnp.maximum(spot - 1, 0)
            for p, x in enumerate(planes + [ends]):
                rim[t, 8 * p : 8 * p + 8, :] = jnp.where(held, jnp.take_along_axis(x, spot, axis=0), 0.0)
        else:
            for p, x in enumerate(planes + [ends]):
                for k, b in enumerate(edges):
                    row = jnp.sum(jnp.where(ids == b, x, 0.0), axis=0, keepdims=True)
                    rim[t, 8 * p + k : 8 * p + k + 1, :] = row
        return 0

    steps(0, n, tile)
    steps(0, n, rims)

    def dest(d, _):
        i, j = d // nlon, d % nlon
        jw, je = (j + nlon - 1) % nlon, (j + 1) % nlon
        q8 = (lane % 8) < 4
        pay[d, 12 * per : 13 * per, :] = at_end(q8, edge[i * nlon + jw], edge[i * nlon + je])
        q2 = (lanes(2) % 8) < 4
        for ii, ok, k, lo, c in (
            (jnp.minimum(i + 1, nlat - 1), i + 1 < nlat, 0, 0, 36),
            (jnp.maximum(i - 1, 0), i > 0, 2, 18, 38),
        ):
            scale = jnp.where(ok, 1.0, 0.0)
            near = ii * nlon + j
            both = rim[near, pl.ds(k, 12, stride=8), :] * scale
            single = rim[near, pl.ds(k + 1 + 4 * k, 6, stride=16), :] * scale
            pay[d, lat_base + lo : lat_base + lo + 12, :] = both
            pay[d, lat_base + lo + 12 : lat_base + lo + 18, :] = single
            corner = at_end(q2, rim[ii * nlon + jw, 96 + k : 98 + k, :], rim[ii * nlon + je, 96 + k : 98 + k, :])
            pay[d, lat_base + c : lat_base + c + 2, :] = corner * scale
        send(d, 1).start()
        return 0

    def finish(d, _):
        if cut:
            send(d, 0).wait()
        send(d, 1).wait()
        return 0

    steps(0, n, dest)
    steps(0, n, finish)


def ends_kernel(ice, covered, land, active, ends):
    count = covered.shape[1]
    lane = lanes(count)
    group = lane // 8
    total = jnp.zeros((count, BX), jnp.float32)
    cover = column(covered[...])
    for y in range(2):
        cells = slice(y * BX, (y + 1) * BX)
        act = cover * (1 - land[:, cells]).astype(jnp.float32)
        active[:, cells] = act
        for ch in range(8):
            x = act if ch == 7 else ice[ch, :, cells]
            p = 2 * ch + y
            total = jnp.where(group == p, roll(x, 8 * p + 4), total)
    ends[...] = total


def pack(raw, spread, nlat, nlon):
    _, n, per, _ = raw.shape
    rows = 13 * per + 40
    return pl.pallas_call(
        functools.partial(pack_kernel, nlat, nlon, per),
        out_shape=f32(n, rows, BX),
        in_specs=[VMEM, VMEM],
        out_specs=pl.BlockSpec(memory_space=pl.ANY),
        scratch_shapes=[
            pltpu.VMEM((n, rows, BX), jnp.float32),
            pltpu.VMEM((n, per, BX), jnp.float32),
            pltpu.VMEM((n, 104, BX), jnp.float32),
            pltpu.SemaphoreType.DMA((2, n)),
        ],
        compiler_params=params(24),
        name="pack",
    )(raw, spread)


def spread_kernel(n, per, owner, out):
    slot = lax.broadcasted_iota(jnp.int32, (per, BX), 0)

    def tile(t, _):
        ids = jnp.zeros((per, BX), jnp.int32)
        for j in range(per):
            ids = jnp.where(slot == j, owner[0, t * per + j] - t * (n * per), ids)
        out[t] = ids
        return 0

    steps(0, n, tile)


def spread_ids(owner, n):
    per = owner.shape[1] // n
    return pl.pallas_call(
        functools.partial(spread_kernel, n, per),
        out_shape=jax.ShapeDtypeStruct((n, per, BX), jnp.int32),
        in_specs=[SMEM],
        out_specs=VMEM,
        compiler_params=params(4),
        name="spread",
    )(owner)


def open_kernel(n, per, raw, opened):
    @pl.when(lax.axis_index("comp") == 0)
    def _():
        def tile(t, _):
            for y in range(2):
                wx, wy, cx, cy, rho = [raw[ch, t, :, y * BX : (y + 1) * BX] for ch in (0, 1, 2, 3, 6)]
                rx, ry = wx - cx, wy - cy
                speed = jnp.sqrt(rx * rx + ry * ry + 1.0)
                rate = rho * (0.1 + 0.05 * speed) * speed
                opened[t, 2 * y] = rate * rx
                opened[t, 2 * y + 1] = rate * ry
                opened[t, 4 + 2 * y] = cx
                opened[t, 5 + 2 * y] = cy
            return 0

        steps(0, n, tile)


def open_stress(raw):
    _, n, per, _ = raw.shape
    return pl.pallas_call(
        functools.partial(open_kernel, n, per),
        out_shape=f32(n, 8, per, BX),
        in_specs=[VMEM],
        out_specs=VMEM,
        compiler_params=params(24),
        name="open_stress",
    )(raw)


def ice_ends(ice, covered, land):
    count = land.shape[0]
    return pl.pallas_call(
        ends_kernel,
        out_shape=[f32(count, 2 * BX), f32(count, BX)],
        in_specs=[VMEM] * 3,
        out_specs=[VMEM] * 2,
        compiler_params=params(8),
        name="ice_ends",
    )(ice, covered, land)


def table_kernel(nlat, nlon, per, owner, ids):
    def tile(t, _):
        i, j = t // nlon, t % nlon
        near = [t, i * nlon + (j + nlon - 1) % nlon, i * nlon + (j + 1) % nlon]
        for k, other in enumerate(near):
            for slot in range(per):
                ids[t, k * per + slot] = owner[0, other * per + slot] - other * (nlat * nlon * per)
        return 0

    steps(0, nlat * nlon, tile)


def table(owner, nlat, nlon):
    n = nlat * nlon
    per = owner.shape[1] // n
    return pl.pallas_call(
        functools.partial(table_kernel, nlat, nlon, per),
        out_shape=jax.ShapeDtypeStruct((n, 3 * per), jnp.int32),
        in_specs=[SMEM],
        out_specs=SMEM,
        compiler_params=params(4),
        name="table",
    )(owner)


def rows_kernel(ice, active, west, east, sides, north, south):
    count = active.shape[0]
    q = (lanes(count) % 8) < 4
    sides[...] = jnp.where(q, west[...], east[...])
    for out, lo in ((north, count - 2), (south, 0)):
        for y in range(2):
            cells = slice(y * BX, (y + 1) * BX)
            for ch in range(8):
                p = 2 * ch + y
                x = active[lo : lo + 2, cells] if ch == 7 else ice[ch, lo : lo + 2, cells]
                out[2 * p : 2 * p + 2, :] = x
        out[32:34, :] = sides[lo : lo + 2, :]


def ice_rows(ice, active, west, east):
    count = active.shape[0]
    return pl.pallas_call(
        rows_kernel,
        out_shape=[f32(count, BX), f32(34, BX), f32(34, BX)],
        in_specs=[VMEM] * 4,
        out_specs=[VMEM] * 3,
        compiler_params=params(8),
        name="ice_rows",
    )(ice, active, west, east)


def middle(rows):
    lane = lanes(rows)
    return (lane >= BX // 4) & (lane < 3 * BX // 4)


def side_plane(ends, ch, mid):
    odd = roll(ends, BX // 2 - (8 * (2 * ch + 1) + 4))
    return jnp.where(mid, odd, roll(ends, -(16 * ch + 4)))


def statics(mass, conc, act):
    return mass * jnp.exp(CSTAR * (conc - 1.0)) * act * (1.0 / 6.0), 2.0 * mass, act, conc


def prep_kernel(count, height, ice, active, sides, begin, still, unused, grid):
    mid = middle(count)
    for ch in range(8):
        for y in range(2):
            cells = slice(y * BX, (y + 1) * BX)
            grid[ch, y, 2 : 2 + count, :] = active[:, cells] if ch == 7 else ice[ch, :, cells]
        grid[ch, 2, 2 : 2 + count, :] = side_plane(sides[...], ch, mid)
        for z in range(3):
            grid[ch, z, 0:2, :] = jnp.zeros((2, BX), jnp.float32)
            grid[ch, z, count + 2 :, :] = jnp.zeros((height - count - 2, BX), jnp.float32)

    for r in range(height // 8):
        at = slice(8 * r, 8 * r + 8)
        for z in range(3):
            u, v, mass, conc, s1, s2, s12, act = [grid[ch, z, at, :] for ch in range(8)]
            for k, x in enumerate((u, v, 0.5 * s1, 0.5 * s2, s12)):
                begin[k, z, at, :] = x
            for k, x in enumerate(statics(mass, conc, act)):
                still[k, z, at, :] = x


def prep(ice, active, sides, spare):
    count = active.shape[0]
    height = (count + 4 + 7) // 8 * 8
    return pl.pallas_call(
        functools.partial(prep_kernel, count, height),
        out_shape=[f32(5, 3, height, BX), f32(4, 3, height, BX), f32(*spare)],
        in_specs=[VMEM] * 3,
        out_specs=[VMEM] * 3,
        scratch_shapes=[pltpu.VMEM((8, 3, height, BX), jnp.float32)],
        compiler_params=params(12),
        name="prep",
    )(ice, active, sides)


def fetch_kernel(*refs):
    k = len(refs) // 2
    big, parts = refs[0].shape[0], 4
    pieces = [(0, pl.ds(c * big // parts, big // parts)) for c in range(parts)] if big % parts == 0 else [(0, pl.ds(0, big))]
    pieces += [(i, pl.ds(0, refs[i].shape[0])) for i in range(1, k)]
    copies = [
        pltpu.make_async_copy(refs[i].at[at], refs[k + i].at[at], refs[-1].at[c]) for c, (i, at) in enumerate(pieces)
    ]
    for copy in copies:
        copy.start()
    for copy in copies:
        copy.wait()


def fetch(*arrays):
    return pl.pallas_call(
        fetch_kernel,
        out_shape=[f32(*x.shape) for x in arrays],
        in_specs=[pl.BlockSpec(memory_space=pl.ANY)] * len(arrays),
        out_specs=[VMEM] * len(arrays),
        scratch_shapes=[pltpu.SemaphoreType.DMA((len(arrays) + 3,))],
        compiler_params=params(4),
        name="fetch",
    )(*arrays)


def east_of(even, odd, side, at127, at63):
    e, o, s = roll(even, -1), roll(odd, -1), roll(side, -1)
    wide = jnp.where(at127, e, jnp.where(at63, roll(odd, 63), s))
    return jnp.where(at127, s, e), jnp.where(at127, roll(side, 63), o), wide


def west_of(even, odd, side, at0, at64):
    e, o, s = roll(even, 1), roll(odd, 1), roll(side, 1)
    wide = jnp.where(at0, e, jnp.where(at64, roll(odd, 65), s))
    return jnp.where(at0, s, e), jnp.where(at0, roll(side, -63), o), wide


def ice_kernel(n, per, count, ids_in, recv, begin, fixed, below, above, back, moved, unused,
               spot, hw, he, speed, state, forced, out8, still, ids, ready):
    tiles = (count + 4 + 7) // 8
    height = tiles * 8
    fetched = pltpu.make_async_copy(ids_in, ids, ready)
    fetched.start()
    blank = jnp.zeros((8, BX), jnp.float32)
    for k in (0, 8):
        spot[k : k + 8, :] = blank
    for k in range((count + 3) * STEP, height * STEP, 8):
        spot[k : k + 8, :] = blank
    for k in (0, height - 8):
        hw[k : k + 8, :] = blank
        he[k : k + 8, :] = blank

    q, mid, mid2 = (lanes(8) % 8) < 4, middle(8), middle(2)
    for r in range(tiles):
        at = slice(8 * r, 8 * r + 8)
        to = slice(FRONT + 8 * r, FRONT + 8 * r + 8)
        for z in range(3):
            for k in range(2):
                speed[k, z, to, :] = begin[k, z, at, :]
            for k in range(3):
                state[k, z, to, :] = begin[2 + k, z, at, :]
            hard, m2, act, conc = [fixed[k, z, at, :] for k in range(4)]
            for k, x in enumerate((hard, m2, CW * conc * act, act, conc)):
                still[k, z, at, :] = x
    for lo, msg in ((0, below), (count + 2, above)):
        at, to = slice(lo, lo + 2), slice(FRONT + lo, FRONT + lo + 2)
        for z in range(3):
            if z < 2:
                raw = [msg[4 * ch + 2 * z : 4 * ch + 2 * z + 2, :] for ch in range(8)]
            else:
                raw = [side_plane(msg[32:34, :], ch, mid2) for ch in range(8)]
            u, v, mass, conc, s1, s2, s12, act = raw
            speed[0, z, to, :] = u
            speed[1, z, to, :] = v
            state[0, z, to, :] = 0.5 * s1
            state[1, z, to, :] = 0.5 * s2
            state[2, z, to, :] = s12
            hard, m2, act, conc = statics(mass, conc, act)
            for k, x in enumerate((hard, m2, CW * conc * act, act, conc)):
                still[k, z, at, :] = x

    fetched.wait()

    def place(o, acc):
        for j in range(per):
            b = (ids[o, j] + 2) * STEP
            spot[pl.ds(b, 12), :] = recv[o, 12 * j : 12 * j + 12, :]
            row = recv[o, 12 * per + j : 12 * per + j + 1, :]
            hw[pl.ds(ids[o, per + j] + 2, 1), :] = row
            he[pl.ds(ids[o, 2 * per + j] + 2, 1), :] = row
        return acc + recv[o, 13 * per : 13 * per + 40, :]

    rim = jnp.zeros((40, BX), jnp.float32)
    if n <= 32:
        for o in range(n):
            rim = place(o, rim)
    else:
        rim = lax.fori_loop(0, n, place, rim)
    up, down = (count + 2) * STEP, STEP
    spot[up : up + 12, :] = rim[0:12]
    spot[down : down + 12, :] = rim[18:30]
    for ch in range(6):
        k = up + STEP + 2 * ch
        spot[k : k + 1, :] = rim[12 + ch : 13 + ch]
        k = 2 * ch + 1
        spot[k : k + 1, :] = rim[30 + ch : 31 + ch]
    for ref in (hw, he):
        ref[count + 2 : count + 4, :] = rim[36:38]
        ref[1:2, :] = rim[38:39]
        ref[0:1, :] = rim[39:40]

    for r in range(tiles):
        at = slice(8 * r, 8 * r + 8)
        ends = jnp.where(q, hw[at, :], he[at, :])
        for z in range(3):
            if z < 2:
                f = [spot[pl.ds(8 * r * STEP + 2 * ch + z, 8, stride=STEP), :] for ch in range(6)]
            else:
                f = [side_plane(ends, ch, mid) for ch in range(6)]
            mass, act, conc = [still[k, z, at, :] for k in (1, 3, 4)]
            mass = 0.5 * mass
            forced[0, z, at, :] = act * (conc * f[0] - mass * f[4])
            forced[1, z, at, :] = act * (conc * f[1] - mass * f[5])
            forced[2, z, at, :] = f[2]
            forced[3, z, at, :] = f[3]

    tail = FRONT + height
    for z in range(3):
        for k in range(2):
            speed[k, z, tail : tail + 8, :] = blank
        for k in range(3):
            state[k, z, 0:8, :] = blank

    lane = lanes(8)
    ends_at = [lane == k for k in (BX - 1, BX // 2 - 1, 0, BX // 2)]
    at127, at63, at0, at64 = ends_at

    def rows_of(r):
        row = 8 * r
        return pl.ds(row, 8), pl.ds(row + FRONT, 8), pl.ds(row + FRONT + 1, 8), pl.ds(row + FRONT - 1, 8)

    def stresses(r):
        at, to, up1, _ = rows_of(r)
        u = [speed[0, z, to, :] for z in range(3)]
        v = [speed[1, z, to, :] for z in range(3)]

        def north(k, x):
            return x[1], speed[k, 0, up1, :], roll(jnp.where(mid, x[2], speed[k, 2, up1, :]), BX // 2)

        un, vn = north(0, u), north(1, v)
        ue = east_of(*u, at127, at63)
        ve = east_of(*v, at127, at63)
        for z in range(3):
            sxx = ue[z] - u[z]
            syy = vn[z] - v[z]
            shear = (un[z] - u[z]) + (ve[z] - v[z])
            div, ten = sxx + syy, sxx - syy
            twice = div + div
            inv = lax.rsqrt(twice * twice + (ten * ten + shear * shear) + 1.0)
            hard = still[0, z, at, :]
            kr = hard * inv
            half = 0.5 * kr
            state[0, z, to, :] = (state[0, z, to, :] * (2.0 / 3.0) - hard) + kr * twice
            state[1, z, to, :] = state[1, z, to, :] * (2.0 / 3.0) + half * ten
            state[2, z, to, :] = state[2, z, to, :] * (2.0 / 3.0) + half * shear

    def speeds(r):
        at, to, _, down1 = rows_of(r)
        s1, s2, s12 = [[state[k, z, to, :] for z in range(3)] for k in range(3)]
        a = [x + y for x, y in zip(s1, s2)]
        c = [x - y for x, y in zip(s1, s2)]
        aw = west_of(*a, at0, at64)
        sw = west_of(*s12, at0, at64)

        def south(x, lower):
            return lower(1), x[0], roll(jnp.where(mid, lower(2), x[2]), BX // 2)

        ss = south(s12, lambda z: state[2, z, down1, :])
        cs = south(c, lambda z: state[0, z, down1, :] - state[1, z, down1, :])
        for z in range(3):
            u, v = speed[0, z, to, :], speed[1, z, to, :]
            fx = (a[z] - aw[z]) + (s12[z] - ss[z])
            fy = (s12[z] - sw[z]) + (c[z] - cs[z])
            m2, base = still[1, z, at, :], still[2, z, at, :]
            cx, cy = forced[2, z, at, :], forced[3, z, at, :]
            dx, dy = cx - u, cy - v
            y2 = dx * dx + dy * dy + DRAG_FLOOR
            drag = base * (y2 * lax.rsqrt(y2))
            part = still[3, z, at, :] * (1.0 / (jnp.maximum(m2, 1.0) + drag))
            mc = (0.5 * CORIO) * m2
            speed[0, z, to, :] = part * (m2 * u + fx + forced[0, z, at, :] + drag * cx + mc * v)
            speed[1, z, to, :] = part * (m2 * v + fy + forced[1, z, at, :] + drag * cy - mc * u)

    def subcycle():
        for r in range(tiles):
            stresses(r)
        for r in range(tiles):
            speeds(r)

    for _ in range(NSUB):
        subcycle()

    for r in range(tiles):
        to = slice(FRONT + 8 * r, FRONT + 8 * r + 8)
        for y in range(2):
            for k in range(2):
                out8[pl.ds(8 * r * REPLY + 2 * k + y, 8, stride=REPLY), :] = speed[k, y, to, :]
    for y in range(2):
        for k in range(2):
            moved[k, :, y * BX : (y + 1) * BX] = speed[k, y, FRONT + 2 : FRONT + 2 + count, :]

    def answer(o, _):
        for j in range(per):
            b = (ids[o, j] + 2) * REPLY
            back[o, 4 * j : 4 * j + 4, :] = out8[pl.ds(b, 4), :]
        return 0

    steps(0, n, answer)


def ice_step(ids, recv, begin, fixed, below, above):
    n, per = ids.shape[0], ids.shape[1] // 3
    count = n * per
    height = (count + 4 + 7) // 8 * 8
    tall = height + 2 * FRONT
    scratch = [
        (height * STEP + 8, BX), (height, BX), (height, BX),
        (2, 3, tall, BX), (3, 3, tall, BX), (4, 3, height, BX), (height * REPLY + 8, BX), (5, 3, height, BX),
    ]
    return pl.pallas_call(
        functools.partial(ice_kernel, n, per, count),
        out_shape=[f32(n, 4 * per, BX), f32(2, count, 2 * BX), f32(n, 2 * per, BX)],
        in_specs=[pl.BlockSpec(memory_space=pl.ANY)] + [VMEM] * 5,
        out_specs=[VMEM] * 3,
        scratch_shapes=[pltpu.VMEM(s, jnp.float32) for s in scratch]
        + [pltpu.SMEM(ids.shape, jnp.int32), pltpu.SemaphoreType.DMA],
        compiler_params=params(16),
        name="ice_step",
    )(ids, recv, begin, fixed, below, above)


def cover_kernel(n, per, ids, conc, covered, land, out, spot):
    count = n * per
    cover = column(covered[...])
    for y in range(2):
        cells = slice(y * BX, (y + 1) * BX)
        act = cover * (1 - land[:, cells]).astype(jnp.float32)
        spot[pl.ds(y, count, stride=2), :] = conc[:, cells] * act

    def tile(o, _):
        for j in range(per):
            out[o, 2 * j : 2 * j + 2, :] = spot[pl.ds(2 * ids[o, j], 2), :]
        return 0

    lax.fori_loop(0, n, tile, 0)


def slot_cover(ids, conc, covered, land):
    n, per = ids.shape[0], ids.shape[1] // 3
    count = n * per
    return pl.pallas_call(
        functools.partial(cover_kernel, n, per),
        out_shape=f32(n, 2 * per, BX),
        in_specs=[SMEM] + [VMEM] * 3,
        out_specs=VMEM,
        scratch_shapes=[pltpu.VMEM((2 * count, BX), jnp.float32)],
        compiler_params=params(8),
        name="slot_cover",
    )(ids, conc, covered, land)


def final_kernel(n, per, got, cover, opened, moved, out):
    is_ocean = lax.axis_index("comp") == 0

    @pl.when(is_ocean)
    def _():
        def tile(t, _):
            for y in range(2):
                cells = slice(y * BX, (y + 1) * BX)
                u, v = [got[t, pl.ds(2 * k + y, per, stride=4), :] for k in range(2)]
                part = cover[t, pl.ds(y, per, stride=2), :]
                dx, dy = u - opened[t, 4 + 2 * y], v - opened[t, 5 + 2 * y]
                factor = (CW * part) * jnp.sqrt(dx * dx + dy * dy + DRAG_FLOOR)
                rest = 1.0 - part
                out[0, t, :, cells] = factor * dx + rest * opened[t, 2 * y]
                out[1, t, :, cells] = factor * dy + rest * opened[t, 2 * y + 1]
            return 0

        steps(0, n, tile)

    @pl.when(jnp.logical_not(is_ocean))
    def _():
        out[...] = moved[...]


def final(got, cover, opened, moved):
    n, _, per, _ = opened.shape
    return pl.pallas_call(
        functools.partial(final_kernel, n, per),
        out_shape=f32(2, n, per, 2 * BX),
        in_specs=[VMEM] * 4,
        out_specs=VMEM,
        compiler_params=params(12),
        name="final",
    )(got, cover, opened, moved)


def per_device(fields, block_owner, ice_covered, land_mask):
    nlat, nlon = lax.axis_size("lat"), lax.axis_size("lon")
    n = nlat * nlon
    count = block_owner.shape[0]
    per = count // n
    side = lax.axis_index("comp")
    fields = fields[0]
    split = fields.reshape(7, n, per, 2 * BX)
    owner = block_owner.reshape(1, count)
    other = lax.ppermute(split, "comp", [(0, 1), (1, 0)])
    opened = open_stress(split)
    def everyone(x):
        return lax.all_to_all(x, ("lat", "lon"), split_axis=0, concat_axis=0, tiled=True)

    height = (count + 4 + 7) // 8 * 8

    def ice_side(other, fields, covered, land, owner, spread):
        recv = everyone(pack(other, spread, nlat, nlon))
        active, ends = ice_ends(fields, covered, land)
        ring = [(i, (i + 1) % nlon) for i in range(nlon)]
        west = lax.ppermute(ends, "lon", ring)
        east = lax.ppermute(ends, "lon", [(j, i) for i, j in ring])
        sides, north, south = ice_rows(fields, active, west, east)
        line = [(i, i + 1) for i in range(nlat - 1)]
        below = lax.ppermute(north, "lat", line)
        above = lax.ppermute(south, "lat", [(j, i) for i, j in line])
        begin, fixed, mine = prep(fields, active, sides, (n, 2 * per, BX))
        return recv, jnp.zeros((n, 3 * per), jnp.int32), below, above, begin, fixed, mine

    def ocean_side(other, fields, covered, land, owner, spread):
        row = jnp.zeros((34, BX), jnp.float32)
        blank = jnp.zeros((5, 3, height, BX), jnp.float32)
        owned = everyone(table(owner, nlat, nlon))
        mine = slot_cover(owned, other.reshape(7, count, 2 * BX)[3], covered, land)
        return jnp.zeros((n, 13 * per + 40, BX), jnp.float32), owned, row, row, blank, blank[:4], mine

    recv, owned, below, above, begin, fixed, mine = lax.cond(
        side == 1, ice_side, ocean_side, other, fields, ice_covered.reshape(1, count), land_mask, owner, spread_ids(owner, n)
    )
    swap = lax.ppermute(owned, "comp", [(0, 1), (1, 0)])
    recv, below, above = fetch(recv, below, above)

    def ice_work(ids, recv, begin, fixed, below, above, mine):
        return ice_step(ids, recv, begin, fixed, below, above)

    def ocean_work(ids, recv, begin, fixed, below, above, mine):
        return jnp.zeros((n, 4 * per, BX), jnp.float32), jnp.zeros((2, count, 2 * BX), jnp.float32), everyone(mine)

    back, moved, cover = lax.cond(
        side == 1, ice_work, ocean_work, swap, recv, begin, fixed, below, above, mine
    )
    back = lax.cond(side == 1, everyone, lambda x: x, back)
    got = lax.ppermute(back, "comp", [(0, 1), (1, 0)])
    out = final(got, cover, opened, moved.reshape(2, n, per, 2 * BX))
    return out.reshape(1, 2, count, 2 * BX)


def solution(mesh):
    placed = (
        P("comp", None, ("lat", "lon"), None),
        P(("lat", "lon")),
        P(("lat", "lon")),
        P(("lat", "lon"), None),
    )
    return jax.shard_map(
        per_device,
        mesh=mesh,
        in_specs=placed,
        out_specs=P("comp", None, ("lat", "lon"), None),
        check_vma=False,
    )
```

```python
import functools

import jax
import jax.numpy as jnp
from jax import lax
from jax.experimental import pallas as pl
from jax.experimental.pallas import tpu as pltpu
from jax.sharding import PartitionSpec as P

BX = 128
NSUB = 4
FRONT = 8
STEP = 13
REPLY = 5

CD_ICE = 0.1
CW = 1.5
CSTAR = 2.0
CORIO = 0.3
DRAG_FLOOR = 0.1

VMEM = pl.BlockSpec(memory_space=pltpu.VMEM)
SMEM = pl.BlockSpec(memory_space=pltpu.SMEM)


def params(mib):
    return pltpu.CompilerParams(vmem_limit_bytes=mib * 1024 * 1024)


def f32(*shape):
    return jax.ShapeDtypeStruct(shape, jnp.float32)


def lanes(rows):
    return lax.broadcasted_iota(jnp.int32, (rows, BX), 1)


def root(x):
    return x * lax.rsqrt(x)


def roll(x, by):
    return pltpu.roll(x, by % BX, 1)


def at_end(q, west, east):
    return jnp.where(q, west, east)


def column(row):
    parts = []
    for lo in range(0, row.shape[1], BX):
        diag = lax.broadcasted_iota(jnp.int32, (BX, BX), 0) == lanes(BX)
        parts.append(jnp.sum(jnp.where(diag, row[:, lo : lo + BX].astype(jnp.float32), 0.0), axis=1, keepdims=True))
    return jnp.concatenate(parts, 0) if len(parts) > 1 else parts[0]


def steps(lo, hi, body):
    if hi - lo <= 32:
        for k in range(lo, hi):
            body(k, 0)
    else:
        lax.fori_loop(lo, hi, body, 0)


def pack_kernel(nlat, nlon, per, raw, spread, out, pay, edge, rim, sems):
    n = nlat * nlon
    count = n * per
    cut = 12 * per if (12 * per) % 8 == 0 else 0

    def send(d, k):
        at = pl.ds(0, cut) if k == 0 else pl.ds(cut, 13 * per + 40 - cut)
        return pltpu.make_async_copy(pay.at[d, at], out.at[d, at], sems.at[k, d])

    lane = lanes(per)
    group = lane // 8
    slot = lax.broadcasted_iota(jnp.int32, (per, BX), 0)
    lat_base = 13 * per

    def tile(t, _):
        def half(ch, y):
            return raw[ch, t, :, y * BX : (y + 1) * BX]

        planes = [None] * 12
        for y in range(2):
            wx, wy, rho = half(0, y), half(1, y), half(6, y)
            scale = rho * CD_ICE * root(wx * wx + wy * wy + 1.0)
            planes[y] = scale * wx
            planes[2 + y] = scale * wy
            for ch in range(2, 6):
                planes[2 * ch + y] = half(ch, y)
        ends = jnp.zeros((per, BX), jnp.float32)
        for p in range(12):
            pay[t, pl.ds(p, per, stride=12), :] = planes[p]
            ends = jnp.where(group == p, roll(planes[p], 8 * p + 4), ends)
        edge[t] = ends
        if cut:
            send(t, 0).start()
        return 0

    def rims(t, _):
        planes = [pay[t, pl.ds(p, per, stride=12), :] for p in range(12)]
        ends = edge[t]
        ids = spread[t]
        edges = (0, 1, count - 1, count - 2)
        if per == 8:
            where = [jnp.sum(jnp.where(ids == b, slot + 1, 0), axis=0, keepdims=True) for b in edges]
            spot = jnp.zeros((per, BX), jnp.int32)
            for k, x in enumerate(where):
                spot = jnp.where(slot == k, x, spot)
            held, spot = spot > 0, jnp.maximum(spot - 1, 0)
            for p, x in enumerate(planes + [ends]):
                rim[t, 8 * p : 8 * p + 8, :] = jnp.where(held, jnp.take_along_axis(x, spot, axis=0), 0.0)
        else:
            for p, x in enumerate(planes + [ends]):
                for k, b in enumerate(edges):
                    row = jnp.sum(jnp.where(ids == b, x, 0.0), axis=0, keepdims=True)
                    rim[t, 8 * p + k : 8 * p + k + 1, :] = row
        return 0

    steps(0, n, tile)
    steps(0, n, rims)

    def dest(d, _):
        i, j = d // nlon, d % nlon
        jw, je = (j + nlon - 1) % nlon, (j + 1) % nlon
        q8 = (lane % 8) < 4
        pay[d, 12 * per : 13 * per, :] = at_end(q8, edge[i * nlon + jw], edge[i * nlon + je])
        q2 = (lanes(2) % 8) < 4
        for ii, ok, k, lo, c in (
            (jnp.minimum(i + 1, nlat - 1), i + 1 < nlat, 0, 0, 36),
            (jnp.maximum(i - 1, 0), i > 0, 2, 18, 38),
        ):
            scale = jnp.where(ok, 1.0, 0.0)
            near = ii * nlon + j
            both = rim[near, pl.ds(k, 12, stride=8), :] * scale
            single = rim[near, pl.ds(k + 1 + 4 * k, 6, stride=16), :] * scale
            pay[d, lat_base + lo : lat_base + lo + 12, :] = both
            pay[d, lat_base + lo + 12 : lat_base + lo + 18, :] = single
            corner = at_end(q2, rim[ii * nlon + jw, 96 + k : 98 + k, :], rim[ii * nlon + je, 96 + k : 98 + k, :])
            pay[d, lat_base + c : lat_base + c + 2, :] = corner * scale
        send(d, 1).start()
        return 0

    def finish(d, _):
        if cut:
            send(d, 0).wait()
        send(d, 1).wait()
        return 0

    steps(0, n, dest)
    steps(0, n, finish)


def ends_kernel(ice, covered, land, active, ends):
    count = covered.shape[1]
    lane = lanes(count)
    group = lane // 8
    total = jnp.zeros((count, BX), jnp.float32)
    cover = column(covered[...])
    for y in range(2):
        cells = slice(y * BX, (y + 1) * BX)
        act = cover * (1 - land[:, cells]).astype(jnp.float32)
        active[:, cells] = act
        for ch in range(8):
            x = act if ch == 7 else ice[ch, :, cells]
            p = 2 * ch + y
            total = jnp.where(group == p, roll(x, 8 * p + 4), total)
    ends[...] = total


def pack(raw, spread, nlat, nlon):
    _, n, per, _ = raw.shape
    rows = 13 * per + 40
    return pl.pallas_call(
        functools.partial(pack_kernel, nlat, nlon, per),
        out_shape=f32(n, rows, BX),
        in_specs=[VMEM, VMEM],
        out_specs=pl.BlockSpec(memory_space=pl.ANY),
        scratch_shapes=[
            pltpu.VMEM((n, rows, BX), jnp.float32),
            pltpu.VMEM((n, per, BX), jnp.float32),
            pltpu.VMEM((n, 104, BX), jnp.float32),
            pltpu.SemaphoreType.DMA((2, n)),
        ],
        compiler_params=params(24),
        name="pack",
    )(raw, spread)


def spread_kernel(n, per, owner, out):
    slot = lax.broadcasted_iota(jnp.int32, (per, BX), 0)

    def tile(t, _):
        ids = jnp.zeros((per, BX), jnp.int32)
        for j in range(per):
            ids = jnp.where(slot == j, owner[0, t * per + j] - t * (n * per), ids)
        out[t] = ids
        return 0

    steps(0, n, tile)


def spread_ids(owner, n):
    per = owner.shape[1] // n
    return pl.pallas_call(
        functools.partial(spread_kernel, n, per),
        out_shape=jax.ShapeDtypeStruct((n, per, BX), jnp.int32),
        in_specs=[SMEM],
        out_specs=VMEM,
        compiler_params=params(4),
        name="spread",
    )(owner)


def open_kernel(n, per, raw, opened):
    @pl.when(lax.axis_index("comp") == 0)
    def _():
        def tile(t, _):
            for y in range(2):
                wx, wy, cx, cy, rho = [raw[ch, t, :, y * BX : (y + 1) * BX] for ch in (0, 1, 2, 3, 6)]
                rx, ry = wx - cx, wy - cy
                speed = root(rx * rx + ry * ry + 1.0)
                rate = rho * (0.1 + 0.05 * speed) * speed
                opened[t, 2 * y] = rate * rx
                opened[t, 2 * y + 1] = rate * ry
                opened[t, 4 + 2 * y] = cx
                opened[t, 5 + 2 * y] = cy
            return 0

        steps(0, n, tile)


def open_stress(raw):
    _, n, per, _ = raw.shape
    return pl.pallas_call(
        functools.partial(open_kernel, n, per),
        out_shape=f32(n, 8, per, BX),
        in_specs=[VMEM],
        out_specs=VMEM,
        compiler_params=params(24),
        name="open_stress",
    )(raw)


def ice_ends(ice, covered, land):
    count = land.shape[0]
    return pl.pallas_call(
        ends_kernel,
        out_shape=[f32(count, 2 * BX), f32(count, BX)],
        in_specs=[VMEM] * 3,
        out_specs=[VMEM] * 2,
        compiler_params=params(8),
        name="ice_ends",
    )(ice, covered, land)


def table_kernel(nlat, nlon, per, owner, ids):
    def tile(t, _):
        i, j = t // nlon, t % nlon
        near = [t, i * nlon + (j + nlon - 1) % nlon, i * nlon + (j + 1) % nlon]
        for k, other in enumerate(near):
            for slot in range(per):
                ids[t, k * per + slot] = owner[0, other * per + slot] - other * (nlat * nlon * per)
        return 0

    steps(0, nlat * nlon, tile)


def table(owner, nlat, nlon):
    n = nlat * nlon
    per = owner.shape[1] // n
    return pl.pallas_call(
        functools.partial(table_kernel, nlat, nlon, per),
        out_shape=jax.ShapeDtypeStruct((n, 3 * per), jnp.int32),
        in_specs=[SMEM],
        out_specs=SMEM,
        compiler_params=params(4),
        name="table",
    )(owner)


def rows_kernel(ice, active, west, east, sides, north, south):
    count = active.shape[0]
    q = (lanes(count) % 8) < 4
    sides[...] = jnp.where(q, west[...], east[...])
    for out, lo in ((north, count - 2), (south, 0)):
        for y in range(2):
            cells = slice(y * BX, (y + 1) * BX)
            for ch in range(8):
                p = 2 * ch + y
                x = active[lo : lo + 2, cells] if ch == 7 else ice[ch, lo : lo + 2, cells]
                out[2 * p : 2 * p + 2, :] = x
        out[32:34, :] = sides[lo : lo + 2, :]


def ice_rows(ice, active, west, east):
    count = active.shape[0]
    return pl.pallas_call(
        rows_kernel,
        out_shape=[f32(count, BX), f32(34, BX), f32(34, BX)],
        in_specs=[VMEM] * 4,
        out_specs=[VMEM] * 3,
        compiler_params=params(8),
        name="ice_rows",
    )(ice, active, west, east)


def middle(rows):
    lane = lanes(rows)
    return (lane >= BX // 4) & (lane < 3 * BX // 4)


def side_plane(ends, ch, mid):
    odd = roll(ends, BX // 2 - (8 * (2 * ch + 1) + 4))
    return jnp.where(mid, odd, roll(ends, -(16 * ch + 4)))


def statics(mass, conc, act):
    return mass * jnp.exp(CSTAR * (conc - 1.0)) * act * (1.0 / 6.0), 2.0 * mass, act, conc


def prep_kernel(count, height, ice, active, sides, begin, still, unused, grid):
    mid = middle(count)
    for ch in range(8):
        for y in range(2):
            cells = slice(y * BX, (y + 1) * BX)
            grid[ch, y, 2 : 2 + count, :] = active[:, cells] if ch == 7 else ice[ch, :, cells]
        grid[ch, 2, 2 : 2 + count, :] = side_plane(sides[...], ch, mid)
        for z in range(3):
            grid[ch, z, 0:2, :] = jnp.zeros((2, BX), jnp.float32)
            grid[ch, z, count + 2 :, :] = jnp.zeros((height - count - 2, BX), jnp.float32)

    for r in range(height // 8):
        at = slice(8 * r, 8 * r + 8)
        for z in range(3):
            u, v, mass, conc, s1, s2, s12, act = [grid[ch, z, at, :] for ch in range(8)]
            for k, x in enumerate((u, v, 0.5 * s1, 0.5 * s2, s12)):
                begin[k, z, at, :] = x
            for k, x in enumerate(statics(mass, conc, act)):
                still[k, z, at, :] = x


def prep(ice, active, sides, spare):
    count = active.shape[0]
    height = (count + 4 + 7) // 8 * 8
    return pl.pallas_call(
        functools.partial(prep_kernel, count, height),
        out_shape=[f32(5, 3, height, BX), f32(4, 3, height, BX), f32(*spare)],
        in_specs=[VMEM] * 3,
        out_specs=[VMEM] * 3,
        scratch_shapes=[pltpu.VMEM((8, 3, height, BX), jnp.float32)],
        compiler_params=params(12),
        name="prep",
    )(ice, active, sides)


def fetch_kernel(*refs):
    k = len(refs) // 2
    big, parts = refs[0].shape[0], 4
    pieces = [(0, pl.ds(c * big // parts, big // parts)) for c in range(parts)] if big % parts == 0 else [(0, pl.ds(0, big))]
    pieces += [(i, pl.ds(0, refs[i].shape[0])) for i in range(1, k)]
    copies = [
        pltpu.make_async_copy(refs[i].at[at], refs[k + i].at[at], refs[-1].at[c]) for c, (i, at) in enumerate(pieces)
    ]
    for copy in copies:
        copy.start()
    for copy in copies:
        copy.wait()


def fetch(*arrays):
    return pl.pallas_call(
        fetch_kernel,
        out_shape=[f32(*x.shape) for x in arrays],
        in_specs=[pl.BlockSpec(memory_space=pl.ANY)] * len(arrays),
        out_specs=[VMEM] * len(arrays),
        scratch_shapes=[pltpu.SemaphoreType.DMA((len(arrays) + 3,))],
        compiler_params=params(4),
        name="fetch",
    )(*arrays)


def east_of(even, odd, side, at127, at63):
    e, o, s = roll(even, -1), roll(odd, -1), roll(side, -1)
    wide = jnp.where(at127, e, jnp.where(at63, roll(odd, 63), s))
    return jnp.where(at127, s, e), jnp.where(at127, roll(side, 63), o), wide


def west_of(even, odd, side, at0, at64):
    e, o, s = roll(even, 1), roll(odd, 1), roll(side, 1)
    wide = jnp.where(at0, e, jnp.where(at64, roll(odd, 65), s))
    return jnp.where(at0, s, e), jnp.where(at0, roll(side, -63), o), wide


def ice_kernel(n, per, count, ids_in, recv, begin, fixed, below, above, back, moved, unused,
               spot, hw, he, speed, state, forced, out8, still, ids, ready):
    tiles = (count + 4 + 7) // 8
    height = tiles * 8
    fetched = pltpu.make_async_copy(ids_in, ids, ready)
    fetched.start()
    blank = jnp.zeros((8, BX), jnp.float32)
    for k in (0, 8):
        spot[k : k + 8, :] = blank
    for k in range((count + 3) * STEP, height * STEP, 8):
        spot[k : k + 8, :] = blank
    for k in (0, height - 8):
        hw[k : k + 8, :] = blank
        he[k : k + 8, :] = blank

    q, mid, mid2 = (lanes(8) % 8) < 4, middle(8), middle(2)
    for r in range(tiles):
        at = slice(8 * r, 8 * r + 8)
        to = slice(FRONT + 8 * r, FRONT + 8 * r + 8)
        for z in range(3):
            for k in range(2):
                speed[k, z, to, :] = begin[k, z, at, :]
            for k in range(3):
                state[k, z, to, :] = begin[2 + k, z, at, :]
            hard, m2, act, conc = [fixed[k, z, at, :] for k in range(4)]
            for k, x in enumerate((hard, m2, CW * conc * act, act, conc)):
                still[k, z, at, :] = x
    for lo, msg in ((0, below), (count + 2, above)):
        at, to = slice(lo, lo + 2), slice(FRONT + lo, FRONT + lo + 2)
        for z in range(3):
            if z < 2:
                raw = [msg[4 * ch + 2 * z : 4 * ch + 2 * z + 2, :] for ch in range(8)]
            else:
                raw = [side_plane(msg[32:34, :], ch, mid2) for ch in range(8)]
            u, v, mass, conc, s1, s2, s12, act = raw
            speed[0, z, to, :] = u
            speed[1, z, to, :] = v
            state[0, z, to, :] = 0.5 * s1
            state[1, z, to, :] = 0.5 * s2
            state[2, z, to, :] = s12
            hard, m2, act, conc = statics(mass, conc, act)
            for k, x in enumerate((hard, m2, CW * conc * act, act, conc)):
                still[k, z, at, :] = x

    fetched.wait()

    def place(o, acc):
        for j in range(per):
            b = (ids[o, j] + 2) * STEP
            spot[pl.ds(b, 12), :] = recv[o, 12 * j : 12 * j + 12, :]
            row = recv[o, 12 * per + j : 12 * per + j + 1, :]
            hw[pl.ds(ids[o, per + j] + 2, 1), :] = row
            he[pl.ds(ids[o, 2 * per + j] + 2, 1), :] = row
        return acc + recv[o, 13 * per : 13 * per + 40, :]

    rim = jnp.zeros((40, BX), jnp.float32)
    if n <= 32:
        for o in range(n):
            rim = place(o, rim)
    else:
        rim = lax.fori_loop(0, n, place, rim)
    up, down = (count + 2) * STEP, STEP
    spot[up : up + 12, :] = rim[0:12]
    spot[down : down + 12, :] = rim[18:30]
    for ch in range(6):
        k = up + STEP + 2 * ch
        spot[k : k + 1, :] = rim[12 + ch : 13 + ch]
        k = 2 * ch + 1
        spot[k : k + 1, :] = rim[30 + ch : 31 + ch]
    for ref in (hw, he):
        ref[count + 2 : count + 4, :] = rim[36:38]
        ref[1:2, :] = rim[38:39]
        ref[0:1, :] = rim[39:40]

    for r in range(tiles):
        at = slice(8 * r, 8 * r + 8)
        ends = jnp.where(q, hw[at, :], he[at, :])
        for z in range(3):
            if z < 2:
                f = [spot[pl.ds(8 * r * STEP + 2 * ch + z, 8, stride=STEP), :] for ch in range(6)]
            else:
                f = [side_plane(ends, ch, mid) for ch in range(6)]
            mass, act, conc = [still[k, z, at, :] for k in (1, 3, 4)]
            mass = 0.5 * mass
            forced[0, z, at, :] = act * (conc * f[0] - mass * f[4])
            forced[1, z, at, :] = act * (conc * f[1] - mass * f[5])
            forced[2, z, at, :] = f[2]
            forced[3, z, at, :] = f[3]

    tail = FRONT + height
    for z in range(3):
        for k in range(2):
            speed[k, z, tail : tail + 8, :] = blank
        for k in range(3):
            state[k, z, 0:8, :] = blank

    lane = lanes(8)
    ends_at = [lane == k for k in (BX - 1, BX // 2 - 1, 0, BX // 2)]
    at127, at63, at0, at64 = ends_at

    def rows_of(r):
        row = 8 * r
        return pl.ds(row, 8), pl.ds(row + FRONT, 8), pl.ds(row + FRONT + 1, 8), pl.ds(row + FRONT - 1, 8)

    def stresses(r):
        at, to, up1, _ = rows_of(r)
        u = [speed[0, z, to, :] for z in range(3)]
        v = [speed[1, z, to, :] for z in range(3)]

        def north(k, x):
            return x[1], speed[k, 0, up1, :], roll(jnp.where(mid, x[2], speed[k, 2, up1, :]), BX // 2)

        un, vn = north(0, u), north(1, v)
        ue = east_of(*u, at127, at63)
        ve = east_of(*v, at127, at63)
        for z in range(3):
            sxx = ue[z] - u[z]
            syy = vn[z] - v[z]
            shear = (un[z] - u[z]) + (ve[z] - v[z])
            div, ten = sxx + syy, sxx - syy
            twice = div + div
            inv = lax.rsqrt(twice * twice + (ten * ten + shear * shear) + 1.0)
            hard = still[0, z, at, :]
            kr = hard * inv
            half = 0.5 * kr
            state[0, z, to, :] = (state[0, z, to, :] * (2.0 / 3.0) - hard) + kr * twice
            state[1, z, to, :] = state[1, z, to, :] * (2.0 / 3.0) + half * ten
            state[2, z, to, :] = state[2, z, to, :] * (2.0 / 3.0) + half * shear

    def speeds(r):
        at, to, _, down1 = rows_of(r)
        s1, s2, s12 = [[state[k, z, to, :] for z in range(3)] for k in range(3)]
        a = [x + y for x, y in zip(s1, s2)]
        c = [x - y for x, y in zip(s1, s2)]
        aw = west_of(*a, at0, at64)
        sw = west_of(*s12, at0, at64)

        def south(x, lower):
            return lower(1), x[0], roll(jnp.where(mid, lower(2), x[2]), BX // 2)

        ss = south(s12, lambda z: state[2, z, down1, :])
        cs = south(c, lambda z: state[0, z, down1, :] - state[1, z, down1, :])
        for z in range(3):
            u, v = speed[0, z, to, :], speed[1, z, to, :]
            fx = (a[z] - aw[z]) + (s12[z] - ss[z])
            fy = (s12[z] - sw[z]) + (c[z] - cs[z])
            m2, base = still[1, z, at, :], still[2, z, at, :]
            cx, cy = forced[2, z, at, :], forced[3, z, at, :]
            dx, dy = cx - u, cy - v
            y2 = dx * dx + dy * dy + DRAG_FLOOR
            drag = base * (y2 * lax.rsqrt(y2))
            part = still[3, z, at, :] * (1.0 / (jnp.maximum(m2, 1.0) + drag))
            mc = (0.5 * CORIO) * m2
            speed[0, z, to, :] = part * (m2 * u + fx + forced[0, z, at, :] + drag * cx + mc * v)
            speed[1, z, to, :] = part * (m2 * v + fy + forced[1, z, at, :] + drag * cy - mc * u)

    def subcycle():
        for r in range(tiles):
            stresses(r)
        for r in range(tiles):
            speeds(r)

    for _ in range(NSUB):
        subcycle()

    for r in range(tiles):
        to = slice(FRONT + 8 * r, FRONT + 8 * r + 8)
        for y in range(2):
            for k in range(2):
                out8[pl.ds(8 * r * REPLY + 2 * k + y, 8, stride=REPLY), :] = speed[k, y, to, :]
    for y in range(2):
        for k in range(2):
            moved[k, :, y * BX : (y + 1) * BX] = speed[k, y, FRONT + 2 : FRONT + 2 + count, :]

    def answer(o, _):
        for j in range(per):
            b = (ids[o, j] + 2) * REPLY
            back[o, 4 * j : 4 * j + 4, :] = out8[pl.ds(b, 4), :]
        return 0

    steps(0, n, answer)


def ice_step(ids, recv, begin, fixed, below, above):
    n, per = ids.shape[0], ids.shape[1] // 3
    count = n * per
    height = (count + 4 + 7) // 8 * 8
    tall = height + 2 * FRONT
    scratch = [
        (height * STEP + 8, BX), (height, BX), (height, BX),
        (2, 3, tall, BX), (3, 3, tall, BX), (4, 3, height, BX), (height * REPLY + 8, BX), (5, 3, height, BX),
    ]
    return pl.pallas_call(
        functools.partial(ice_kernel, n, per, count),
        out_shape=[f32(n, 4 * per, BX), f32(2, count, 2 * BX), f32(n, 2 * per, BX)],
        in_specs=[pl.BlockSpec(memory_space=pl.ANY)] + [VMEM] * 5,
        out_specs=[VMEM] * 3,
        scratch_shapes=[pltpu.VMEM(s, jnp.float32) for s in scratch]
        + [pltpu.SMEM(ids.shape, jnp.int32), pltpu.SemaphoreType.DMA],
        compiler_params=params(16),
        name="ice_step",
    )(ids, recv, begin, fixed, below, above)


def cover_kernel(n, per, ids, conc, covered, land, out, spot):
    count = n * per
    cover = column(covered[...])
    for y in range(2):
        cells = slice(y * BX, (y + 1) * BX)
        act = cover * (1 - land[:, cells]).astype(jnp.float32)
        spot[pl.ds(y, count, stride=2), :] = conc[:, cells] * act

    def tile(o, _):
        for j in range(per):
            out[o, 2 * j : 2 * j + 2, :] = spot[pl.ds(2 * ids[o, j], 2), :]
        return 0

    lax.fori_loop(0, n, tile, 0)


def slot_cover(ids, conc, covered, land):
    n, per = ids.shape[0], ids.shape[1] // 3
    count = n * per
    return pl.pallas_call(
        functools.partial(cover_kernel, n, per),
        out_shape=f32(n, 2 * per, BX),
        in_specs=[SMEM] + [VMEM] * 3,
        out_specs=VMEM,
        scratch_shapes=[pltpu.VMEM((2 * count, BX), jnp.float32)],
        compiler_params=params(8),
        name="slot_cover",
    )(ids, conc, covered, land)


def final_kernel(n, per, got, cover, opened, moved, out):
    is_ocean = lax.axis_index("comp") == 0

    @pl.when(is_ocean)
    def _():
        def tile(t, _):
            for y in range(2):
                cells = slice(y * BX, (y + 1) * BX)
                u, v = [got[t, pl.ds(2 * k + y, per, stride=4), :] for k in range(2)]
                part = cover[t, pl.ds(y, per, stride=2), :]
                dx, dy = u - opened[t, 4 + 2 * y], v - opened[t, 5 + 2 * y]
                factor = (CW * part) * root(dx * dx + dy * dy + DRAG_FLOOR)
                rest = 1.0 - part
                out[0, t, :, cells] = factor * dx + rest * opened[t, 2 * y]
                out[1, t, :, cells] = factor * dy + rest * opened[t, 2 * y + 1]
            return 0

        steps(0, n, tile)

    @pl.when(jnp.logical_not(is_ocean))
    def _():
        out[...] = moved[...]


def final(got, cover, opened, moved):
    n, _, per, _ = opened.shape
    return pl.pallas_call(
        functools.partial(final_kernel, n, per),
        out_shape=f32(2, n, per, 2 * BX),
        in_specs=[VMEM] * 4,
        out_specs=VMEM,
        compiler_params=params(12),
        name="final",
    )(got, cover, opened, moved)


def per_device(fields, block_owner, ice_covered, land_mask):
    nlat, nlon = lax.axis_size("lat"), lax.axis_size("lon")
    n = nlat * nlon
    count = block_owner.shape[0]
    per = count // n
    side = lax.axis_index("comp")
    fields = fields[0]
    split = fields.reshape(7, n, per, 2 * BX)
    owner = block_owner.reshape(1, count)
    other = lax.ppermute(split, "comp", [(0, 1), (1, 0)])
    opened = open_stress(split)
    def everyone(x):
        return lax.all_to_all(x, ("lat", "lon"), split_axis=0, concat_axis=0, tiled=True)

    height = (count + 4 + 7) // 8 * 8

    def ice_side(other, fields, covered, land, owner, spread):
        recv = everyone(pack(other, spread, nlat, nlon))
        active, ends = ice_ends(fields, covered, land)
        ring = [(i, (i + 1) % nlon) for i in range(nlon)]
        west = lax.ppermute(ends, "lon", ring)
        east = lax.ppermute(ends, "lon", [(j, i) for i, j in ring])
        sides, north, south = ice_rows(fields, active, west, east)
        line = [(i, i + 1) for i in range(nlat - 1)]
        below = lax.ppermute(north, "lat", line)
        above = lax.ppermute(south, "lat", [(j, i) for i, j in line])
        begin, fixed, mine = prep(fields, active, sides, (n, 2 * per, BX))
        return recv, jnp.zeros((n, 3 * per), jnp.int32), below, above, begin, fixed, mine

    def ocean_side(other, fields, covered, land, owner, spread):
        row = jnp.zeros((34, BX), jnp.float32)
        blank = jnp.zeros((5, 3, height, BX), jnp.float32)
        owned = everyone(table(owner, nlat, nlon))
        mine = slot_cover(owned, other.reshape(7, count, 2 * BX)[3], covered, land)
        return jnp.zeros((n, 13 * per + 40, BX), jnp.float32), owned, row, row, blank, blank[:4], mine

    recv, owned, below, above, begin, fixed, mine = lax.cond(
        side == 1, ice_side, ocean_side, other, fields, ice_covered.reshape(1, count), land_mask, owner, spread_ids(owner, n)
    )
    swap = lax.ppermute(owned, "comp", [(0, 1), (1, 0)])
    recv, below, above = fetch(recv, below, above)

    def ice_work(ids, recv, begin, fixed, below, above, mine):
        return ice_step(ids, recv, begin, fixed, below, above)

    def ocean_work(ids, recv, begin, fixed, below, above, mine):
        return jnp.zeros((n, 4 * per, BX), jnp.float32), jnp.zeros((2, count, 2 * BX), jnp.float32), everyone(mine)

    back, moved, cover = lax.cond(
        side == 1, ice_work, ocean_work, swap, recv, begin, fixed, below, above, mine
    )
    back = lax.cond(side == 1, everyone, lambda x: x, back)
    got = lax.ppermute(back, "comp", [(0, 1), (1, 0)])
    out = final(got, cover, opened, moved.reshape(2, n, per, 2 * BX))
    return out.reshape(1, 2, count, 2 * BX)


def solution(mesh):
    placed = (
        P("comp", None, ("lat", "lon"), None),
        P(("lat", "lon")),
        P(("lat", "lon")),
        P(("lat", "lon"), None),
    )
    return jax.shard_map(
        per_device,
        mesh=mesh,
        in_specs=placed,
        out_specs=P("comp", None, ("lat", "lon"), None),
        check_vma=False,
    )
```
